128 devices in a mesh: front: 2 (over core), row: 8 (over y, z_lo), col: 8 (over x, z_hi).
Axes of the slice: x: 4, y: 4, z: 4 (z_hi: 2, z_lo: 2; z = z_hi * 2 + z_lo), core: 2. Of those that a mesh axis runs over, the one named last changes fastest.
Arguments:
- orig_front: float32 [2, 12, 8, 128, 12, 8, 128], P('front', None, 'row', None, None, 'col'), may hold values from -100 to 300, as said below
- child_updates: bfloat16 [2, 2, 8, 8, 128, 8, 8, 128], P('front', None, None, 'row', None, None, 'col'), may hold values from -2 to 2, as said below
- index_maps: int32 [2, 2, 64], replicated, may hold values from 0 to 95, as said below
Outputs:
- factored: float32 [2, 12, 8, 128, 12, 8, 128], P('front', None, 'row', None, None, 'col')
The draws below stay inside these ranges and needn't reach their ends.
Inputs may be any that keep to these rules, and one draw needn't show every extreme that they name: `index_maps`: within one child, distinct blocks go to distinct parent blocks. Call b mod 8 the grid row of parent block b. Of the 8 child blocks q * 8 + r with one r, at most 2 go to any one grid row and exactly 2 to some; each grid row receives exactly 8 blocks of each child. `orig_front`: each front plus its placed child updates is symmetric, with a positive definite leading block of order 2 * 128. `child_updates`: each child update is symmetric.
All inputs are finite; a program needn't handle non-finite values.
Results may differ from the reference program's by a relative error of at most 0.0003.
Values may be sent and summed in bfloat16 or wider, within the bound.
A program may use at most 128 MiB of HBM per device.

```python
import jax
import jax.numpy as jnp
from jax import lax

BLK = 128
LB = 12
QB = 8
PANELS = 2
N_ROW = 8
N_COL = 8


def symmetric_draw(key, order, spread):
    first = jax.random.fold_in(key, 0)
    noise = jnp.clip(jax.random.normal(first, (order, order), jnp.float32), -3.0, 3.0) * spread
    both = (noise + noise.T) * 0.7071
    return both


def coupled_front(key, order, leading):
    inner_width = 2 * leading
    noise_key, load_key = jax.random.split(key, 2)
    matrix = symmetric_draw(noise_key, order, 1.0)
    loadings = jnp.clip(jax.random.normal(load_key, (order, inner_width), jnp.float32), -3.0, 3.0)
    weight = 64.0 / inner_width
    coupling = jnp.dot(loadings, loadings[:leading].T, precision=lax.Precision.HIGHEST) * weight
    matrix = matrix.at[:, :leading].set(coupling)
    matrix = matrix.at[:leading, :].set(coupling.T)
    corner = 0.5 * (coupling[:leading] + coupling[:leading].T)
    matrix = matrix.at[:leading, :leading].set(corner)
    positions = jnp.arange(order)
    diagonal = 35.0 + weight * jnp.sum(loadings * loadings, axis=1)
    matrix = matrix.at[positions, positions].set(diagonal)
    return matrix


def draw_orig_front(key, part):
    order = LB * N_ROW * BLK
    leading = PANELS * BLK
    fronts = []
    for parent in range(2):
        base = jax.random.fold_in(key, 11 + parent)
        matrix = coupled_front(base, order, leading)
        fronts.append(matrix.reshape(LB, N_ROW, BLK, LB, N_COL, BLK))
    return jnp.stack(fronts).astype(jnp.float32)


def draw_child_updates(key, part):
    order = QB * N_ROW * BLK
    rows = []
    for child in range(2):
        pair = []
        for parent in range(2):
            base = jax.random.fold_in(key, 101 + 2 * child + parent)
            pair.append(symmetric_draw(base, order, 0.25).reshape(QB, N_ROW, BLK, QB, N_COL, BLK))
        rows.append(jnp.stack(pair))
    return jnp.stack(rows).astype(jnp.bfloat16)


def one_map(key):
    first, second = jax.random.split(key)
    shuffled = jax.random.permutation(first, N_ROW)
    local_ids = jnp.arange(QB, dtype=jnp.int32)
    shifts = shuffled[local_ids % N_ROW]
    if QB <= N_ROW:
        shifts = shifts.at[QB - 1].set(shifts[0])
    slot_table = jax.vmap(lambda single: jax.random.permutation(single, LB))(jax.random.split(second, N_ROW))[:, :QB]
    grid_ids = jnp.arange(N_ROW, dtype=jnp.int32)
    target = (grid_ids[None, :] + shifts[:, None]) % N_ROW
    landing = slot_table[target, local_ids[:, None]]
    return (landing * N_ROW + target).reshape(-1).astype(jnp.int32)


def draw_index_maps(key, part):
    rows = []
    for parent in range(2):
        pair = []
        for child in range(2):
            pair.append(one_map(jax.random.fold_in(key, 501 + 2 * parent + child)))
        rows.append(jnp.stack(pair))
    return jnp.stack(rows).astype(jnp.int32)


def setup_inputs(seed: int = 0) -> dict:
    seeds = jax.random.split(jax.random.key(seed), 4)
    orig_front = draw_orig_front(jax.random.fold_in(seeds[3], 71), 0)
    child_updates = draw_child_updates(jax.random.fold_in(seeds[3], 71), 0)
    index_maps = draw_index_maps(jax.random.fold_in(seeds[3], 71), 0)
    return {"orig_front": orig_front, "child_updates": child_updates, "index_maps": index_maps}


def panel_step(matrix, step):
    order = matrix.shape[0]
    start = step * BLK
    lower = jnp.linalg.cholesky(matrix[start:start + BLK, start:start + BLK])
    column = matrix[:, start:start + BLK]
    solved = lax.linalg.triangular_solve(lower, column, left_side=False, lower=True, transpose_a=True)
    block_ids = (jnp.arange(order) // BLK).astype(jnp.int32)
    solved = jnp.where((block_ids < step)[:, None], jnp.float32(0.0), solved)
    solved = solved.at[start:start + BLK].set(lower)
    matrix = matrix - jnp.dot(solved, solved.T, precision=lax.Precision.HIGHEST)
    matrix = matrix.at[:, start:start + BLK].set(solved)
    matrix = matrix.at[start:start + BLK, start + BLK:].set(jnp.float32(0.0))
    return matrix

def reference(orig_front, child_updates, index_maps):
    order = LB * N_ROW * BLK
    child_order = QB * N_ROW * BLK
    results = []
    for parent in range(2):
        matrix = orig_front[parent].reshape(order, order)
        for child in range(2):
            update = child_updates[child, parent].reshape(child_order, child_order).astype(jnp.float32)
            places = (index_maps[parent, child][:, None] * BLK + jnp.arange(BLK).astype(jnp.int32)[None, :]).reshape(-1).astype(jnp.int32)
            matrix = matrix.at[places[:, None], places[None, :]].add(update)
        for step in range(PANELS):
            matrix = panel_step(matrix, step)
        results.append(matrix.reshape(LB, N_ROW, BLK, LB, N_COL, BLK))
    return jnp.stack(results)
```

```python
import functools

import jax
import jax.numpy as jnp
from jax import lax
from jax.experimental import pallas as pl
from jax.experimental.pallas import tpu as pltpu
from jax.sharding import PartitionSpec as P

F32 = jnp.float32
BF16 = jnp.bfloat16
I32 = jnp.int32
MESH = pl.DeviceIdType.MESH
HIGHEST = lax.Precision.HIGHEST
HBM = pltpu.MemorySpace.HBM
VMEM = pltpu.MemorySpace.VMEM
SMEM = pltpu.MemorySpace.SMEM


def tables(maps, front, row, col, grid, parent_blocks):
    blocks = maps.shape[-1] // grid
    by_source = maps.reshape(2, 2, blocks, grid)
    target = by_source % grid
    place = by_source // grid
    ids = jnp.arange(blocks, dtype=I32)
    before = ids[None, :] < ids[:, None]
    same = target[:, :, :, None, :] == target[:, :, None, :, :]
    order = jnp.sum((same & before[None, None, :, :, None]).astype(I32), axis=3)
    send_slot = target * 2 + order
    recv_slot = jnp.arange(grid, dtype=I32) * 2 + order
    mine = lax.dynamic_index_in_dim(by_source, front, 1, keepdims=False)
    row_send = lax.dynamic_index_in_dim(
        lax.dynamic_index_in_dim(send_slot, front, 1, keepdims=False), row, 2, keepdims=False
    )
    held_rows = lax.dynamic_index_in_dim(mine, row, 2, keepdims=False)
    held_cols = lax.dynamic_index_in_dim(mine, col, 2, keepdims=False)
    lead = jnp.arange(2, dtype=I32)
    lead_row = jnp.sum(
        (held_rows[:, None, :] == lead[None, :, None]).astype(I32) * (ids + 1), axis=-1
    ) - 1
    lead_col = jnp.sum(
        (held_cols[:, None, :] == lead[None, :, None]).astype(I32) * (ids + 1), axis=-1
    ) - 1
    own = lambda value: lax.dynamic_index_in_dim(value, front, 0, keepdims=False)
    own_target, own_place, own_recv = own(target), own(place), own(recv_slot)
    col_send = lax.dynamic_index_in_dim(own(send_slot), col, 2, keepdims=False)
    flat = lambda value: value.reshape(2, blocks * grid)
    row_hit = flat(own_target == row).astype(I32)
    col_hit = flat(own_target == col).astype(I32)
    count = jnp.arange(blocks * grid, dtype=I32)
    rank = jnp.sum(row_hit[:, None, :] * (count[None, :] < count[:, None]).astype(I32), axis=-1)
    row_slot = jnp.sum(
        row_hit[:, None, :] * (rank[:, None, :] == ids[None, :, None]).astype(I32) * flat(own_recv)[:, None, :],
        axis=-1,
    )
    spots = jnp.arange(parent_blocks, dtype=I32)
    at = (flat(own_place)[:, None, :] == spots[None, :, None]).astype(I32)
    row_pos = jnp.sum(row_hit[:, None, :] * at * (rank + 1)[:, None, :], axis=-1) - 1
    col_pos = jnp.sum(col_hit[:, None, :] * at * (flat(own_recv) + 1)[:, None, :], axis=-1) - 1
    return row_send, lead_row, lead_col, row_slot, col_send, row_pos, col_pos


def pack_rows_kernel(slot_ref, lrow_ref, lcol_ref, where_ref, child_ref, corner_ref, out_ref, lead_ref, wide):
    p, q = pl.program_id(0), pl.program_id(1)
    size, blocks = child_ref.shape[2], child_ref.shape[3]
    wide[...] = child_ref[0, 0].astype(F32).reshape(size * blocks, size)

    @pl.when(q == 0)
    def _():
        for a in range(2):
            for b in range(2):
                hit = (where_ref[0] == p) & (where_ref[1] == a) & (where_ref[2] == b)
                lead_ref[0, a, b] = jnp.where(hit, corner_ref[...], 0.0)

    for j in range(blocks):
        out_ref[0, 0, j] = wide[pl.ds(j, size, stride=blocks), :].astype(BF16)

    for a in range(2):
        for b in range(2):

            @pl.when((lrow_ref[2 * p + a] == q) & (lcol_ref[2 * p + b] >= 0))
            def _():
                j = jnp.maximum(lcol_ref[2 * p + b], 0)
                lead_ref[0, a, b] = lead_ref[0, a, b] + out_ref[0, 0, j].astype(F32)


def pack_rows(child, corner, slots, lead_row, lead_col, where, grid):
    _, blocks, size, _, _ = child.shape
    return pl.pallas_call(
        pack_rows_kernel,
        grid_spec=pltpu.PrefetchScalarGridSpec(
            num_scalar_prefetch=4,
            grid=(2, blocks),
            in_specs=[
                pl.BlockSpec((1, 1, size, blocks, size), lambda p, q, *_: (p, q, 0, 0, 0)),
                pl.BlockSpec((size, size), lambda p, q, *_: (0, 0)),
            ],
            out_specs=[
                pl.BlockSpec((1, 1, blocks, size, size), lambda p, q, s, *_: (p, s[p * blocks + q], 0, 0, 0)),
                pl.BlockSpec((1, 2, 2, size, size), lambda p, q, *_: (p, 0, 0, 0, 0)),
            ],
            scratch_shapes=[pltpu.VMEM((size * blocks, size), F32)],
        ),
        out_shape=[
            jax.ShapeDtypeStruct((2, grid * 2, blocks, size, size), BF16),
            jax.ShapeDtypeStruct((2, 2, 2, size, size), F32),
        ],
        compiler_params=pltpu.CompilerParams(dimension_semantics=("arbitrary", "arbitrary")),
        cost_estimate=pl.CostEstimate(flops=2_000_000, bytes_accessed=4 * child.size, transcendentals=0),
        name="pack_rows",
    )(slots.reshape(-1), lead_row.reshape(-1), lead_col.reshape(-1), where, child, corner)


def pack_cols_kernel(row_ref, slot_ref, in_ref, out_ref):
    k = pl.program_id(0)
    blocks = in_ref.shape[2]
    for j in range(blocks):
        out_ref[0, 0, slot_ref[k * blocks + j]] = in_ref[0, 0, j]


def pack_cols(received, row_slot, col_send, grid):
    _, _, blocks, size, _ = received.shape
    return pl.pallas_call(
        pack_cols_kernel,
        grid_spec=pltpu.PrefetchScalarGridSpec(
            num_scalar_prefetch=2,
            grid=(2, blocks),
            in_specs=[
                pl.BlockSpec((1, 1, blocks, size, size), lambda k, j, r, *_: (k, r[k * blocks + j], 0, 0, 0))
            ],
            out_specs=pl.BlockSpec((1, 1, grid * 2, size, size), lambda k, j, *_: (k, j, 0, 0, 0)),
        ),
        out_shape=jax.ShapeDtypeStruct((2, blocks, grid * 2, size, size), BF16),
        compiler_params=pltpu.CompilerParams(dimension_semantics=("arbitrary", "arbitrary")),
        cost_estimate=pl.CostEstimate(flops=2_000_000, bytes_accessed=4 * received.size, transcendentals=0),
        name="pack_cols",
    )(row_slot.reshape(-1), col_send.reshape(-1), received)


def meet(peers):
    barrier = pltpu.get_barrier_semaphore()
    for peer in peers:
        pl.semaphore_signal(barrier, inc=1, device_id=peer, device_id_type=MESH)
    pl.semaphore_wait(barrier, len(peers))


def hop_order(grid):
    return [d for pair in zip(range(1, grid), range(grid - 1, 0, -1)) for d in pair][: grid - 1]


def row_exchange_kernel(grid, send_ref, recv_ref, send_sem, recv_sem, local_sem):
    f, r, c = lax.axis_index("front"), lax.axis_index("row"), lax.axis_index("col")
    others = [(p, d) for d in hop_order(grid) for p in range(2)] + [(1, 0)]
    peers = [(lax.rem(f + p, 2), lax.rem(r + d, grid), c) for p, d in others]
    local = pltpu.make_async_copy(send_ref.at[f, pl.ds(2 * r, 2)], recv_ref.at[f, pl.ds(2 * r, 2)], local_sem)
    local.start()
    meet(peers)
    copies = []
    for n, (p, d) in enumerate(others):
        peer = peers[n]
        copy = pltpu.make_async_remote_copy(
            src_ref=send_ref.at[peer[0], pl.ds(2 * peer[1], 2)],
            dst_ref=recv_ref.at[f, pl.ds(2 * r, 2)],
            send_sem=send_sem.at[n],
            recv_sem=recv_sem.at[p, d],
            device_id=peer,
            device_id_type=MESH,
        )
        copy.start()
        copies.append(copy)
    local.wait()
    for copy in copies:
        copy.wait_send()
    for copy in copies:
        copy.wait_recv()


def row_exchange(packed, grid):
    n = 2 * grid
    return pl.pallas_call(
        functools.partial(row_exchange_kernel, grid),
        out_shape=jax.ShapeDtypeStruct(packed.shape, BF16),
        in_specs=[pl.BlockSpec(memory_space=HBM)],
        out_specs=pl.BlockSpec(memory_space=HBM),
        scratch_shapes=[
            pltpu.SemaphoreType.DMA((n,)),
            pltpu.SemaphoreType.DMA((2, grid)),
            pltpu.SemaphoreType.DMA,
        ],
        compiler_params=pltpu.CompilerParams(collective_id=1, has_side_effects=True),
        cost_estimate=pl.CostEstimate(flops=100_000_000, bytes_accessed=4 * packed.size, transcendentals=0),
        name="row_exchange",
    )(packed)


def factor_block(work, size):
    lanes = lax.broadcasted_iota(I32, (size, size), 1)
    rows = lax.broadcasted_iota(I32, (size, 1), 0)

    def step(j, carry):
        pivot_row = work[pl.ds(j, 1), :]
        left = work[:, :size]
        column = jnp.sum(jnp.where(lanes == j, left, 0.0), axis=1, keepdims=True)
        pivot = jnp.sum(jnp.where(lanes[:1] == j, pivot_row[:, :size], 0.0), axis=1, keepdims=True)
        scale = jnp.where(rows > j, column / pivot, 0.0)
        work[...] = work[...] - scale * pivot_row
        return carry

    lax.fori_loop(0, size, step, 0)


def triangular(work, size):
    eye = lax.broadcasted_iota(I32, (size, size), 0) == lax.broadcasted_iota(I32, (size, size), 1)
    upper = lax.broadcasted_iota(I32, (size, size), 0) <= lax.broadcasted_iota(I32, (size, size), 1)
    u = work[:, :size]
    root = lax.rsqrt(jnp.sum(jnp.where(eye, u, 0.0), axis=1, keepdims=True))
    lower = jnp.where(upper, u * root, 0.0).T
    inverse = work[:, size:] * root
    return lower, inverse


def mm(a, b):
    return jnp.dot(a, b, precision=HIGHEST, preferred_element_type=F32)


def mm_t(a, b):
    return lax.dot_general(a, b, (((1,), (1,)), ((), ())), precision=HIGHEST, preferred_element_type=F32)


def factor_lead(lead_ref, low_ref, inv_ref, work, size):
    eye = (
        lax.broadcasted_iota(I32, (size, size), 0) == lax.broadcasted_iota(I32, (size, size), 1)
    ).astype(F32)
    work[:, :size] = lead_ref[0, 0]
    work[:, size:] = eye
    factor_block(work, size)
    l0, i0 = triangular(work, size)
    l10 = mm_t(lead_ref[1, 0], i0)
    work[:, :size] = lead_ref[1, 1] - mm_t(l10, l10)
    work[:, size:] = eye
    factor_block(work, size)
    l1, i1 = triangular(work, size)
    low_ref[0] = jnp.concatenate([l0, jnp.zeros_like(l0)], axis=1)
    low_ref[1] = jnp.concatenate([l10, l1], axis=1)
    inv_ref[:size, :size] = i0
    inv_ref[:size, size:] = jnp.zeros_like(i0)
    inv_ref[size:, :size] = -mm(i1, mm(l10, i0))
    inv_ref[size:, size:] = i1


def col_exchange_kernel(grid, size, send_ref, lead_ref, recv_ref, low_ref, inv_ref, work, send_sem, recv_sem, local_sem):
    f, r, c = lax.axis_index("front"), lax.axis_index("row"), lax.axis_index("col")
    others = hop_order(grid)
    peers = [(f, r, lax.rem(c + d, grid)) for d in others]
    local = pltpu.make_async_copy(send_ref.at[:, :, pl.ds(2 * c, 2)], recv_ref.at[c], local_sem)
    local.start()
    meet(peers)
    copies = []
    for n, d in enumerate(others):
        copy = pltpu.make_async_remote_copy(
            src_ref=send_ref.at[:, :, pl.ds(2 * peers[n][2], 2)],
            dst_ref=recv_ref.at[c],
            send_sem=send_sem.at[n],
            recv_sem=recv_sem.at[d],
            device_id=peers[n],
            device_id_type=MESH,
        )
        copy.start()
        copies.append(copy)
    factor_lead(lead_ref, low_ref, inv_ref, work, size)
    local.wait()
    for copy in copies:
        copy.wait_send()
    for copy in copies:
        copy.wait_recv()


def col_exchange(packed, lead, grid):
    _, blocks, _, size, _ = packed.shape
    return pl.pallas_call(
        functools.partial(col_exchange_kernel, grid, size),
        out_shape=[
            jax.ShapeDtypeStruct((grid, 2, blocks, 2, size, size), BF16),
            jax.ShapeDtypeStruct((2, size, 2 * size), F32),
            jax.ShapeDtypeStruct((2 * size, 2 * size), F32),
        ],
        in_specs=[pl.BlockSpec(memory_space=HBM), pl.BlockSpec(memory_space=VMEM)],
        out_specs=[
            pl.BlockSpec(memory_space=HBM),
            pl.BlockSpec(memory_space=VMEM),
            pl.BlockSpec(memory_space=VMEM),
        ],
        scratch_shapes=[
            pltpu.VMEM((size, 2 * size), F32),
            pltpu.SemaphoreType.DMA((grid,)),
            pltpu.SemaphoreType.DMA((grid,)),
            pltpu.SemaphoreType.DMA,
        ],
        compiler_params=pltpu.CompilerParams(collective_id=2, has_side_effects=True),
        cost_estimate=pl.CostEstimate(flops=100_000_000, bytes_accessed=4 * packed.size, transcendentals=0),
        name="col_exchange",
    )(packed, lead)


def added(base, parts):
    for ref, index, valid in parts:
        base = base + jnp.where(valid, ref(jnp.maximum(index, 0)).astype(F32), 0.0)
    return base


def panel_kernel(spots, row_ref, col_ref, fcol_ref, frow_ref, c0, c1, r0, r1, rows_out, cols_out):
    size = fcol_ref.shape[-1]
    cols = (c0, c1)
    rows = (r0, r1)
    for l in range(spots):
        parts = []
        for k in range(2):
            index = row_ref[k * spots + l]
            valid = (index >= 0) & (col_ref[k * spots] >= 0)
            parts.append((lambda i, k=k: cols[k][0, 0, i, 0], index, valid))
        rows_out[l] = added(fcol_ref[l], parts)
        parts = []
        for k in range(2):
            index = col_ref[k * spots + l]
            valid = (index >= 0) & (row_ref[k * spots] >= 0)
            parts.append((lambda i, k=k: rows[k][i // 2, 0, 0, i % 2], index, valid))
        cols_out[l] = added(frow_ref[pl.ds(l, size, stride=spots), :], parts).T


def panels(received, fcol, flat, row_pos, col_pos):
    grid, _, blocks, _, size, _ = received.shape
    spots = fcol.shape[0]

    def by_col(k):
        def index(_, row, col):
            i = jnp.maximum(col[k * spots], 0)
            return (i // 2, k, 0, i % 2, 0, 0)

        return pl.BlockSpec((1, 1, blocks, 1, size, size), index)

    def by_row(k):
        return pl.BlockSpec(
            (grid, 1, 1, 2, size, size),
            lambda _, row, col: (0, k, jnp.maximum(row[k * spots], 0), 0, 0, 0),
        )

    shape = jax.ShapeDtypeStruct((spots, size, size), F32)
    whole = pl.BlockSpec((spots, size, size), lambda *_: (0, 0, 0))
    return pl.pallas_call(
        functools.partial(panel_kernel, spots),
        grid_spec=pltpu.PrefetchScalarGridSpec(
            num_scalar_prefetch=2,
            grid=(1,),
            in_specs=[
                whole,
                pl.BlockSpec((size * spots, size), lambda *_: (0, 0)),
                by_col(0),
                by_col(1),
                by_row(0),
                by_row(1),
            ],
            out_specs=[whole, whole],
        ),
        out_shape=[shape, shape],
        cost_estimate=pl.CostEstimate(flops=2_000_000, bytes_accessed=6_000_000, transcendentals=0),
        name="panels",
    )(row_pos.reshape(-1), col_pos.reshape(-1), fcol, flat, received, received, received, received)


def spread_kernel(grid, spots, rows_ref, cols_ref, rows_out, cols_out, one_send, one_recv, two_send, two_recv):
    f, r, c = lax.axis_index("front"), lax.axis_index("row"), lax.axis_index("col")
    half = grid // 2
    part = spots // half
    row_peer = lambda i: (f, r, i)
    col_peer = lambda i: (f, i, c)
    groups = ((rows_ref, rows_out, c, row_peer), (cols_ref, cols_out, r, col_peer))
    meet([peer(lax.rem(me + d, grid)) for _, _, me, peer in groups for d in range(1, grid)])

    def first(g, s, n):
        source, out, me, peer = groups[g]
        to = lax.rem(s + n, grid)
        piece = pl.ds((to // 2) * part, part)
        return pltpu.make_async_remote_copy(
            src_ref=source.at[piece],
            dst_ref=out.at[s, piece],
            send_sem=one_send.at[g, n],
            recv_sem=one_recv.at[g, s],
            device_id=peer(to),
            device_id_type=MESH,
        )

    def second(g, s, n, source):
        _, out, me, peer = groups[g]
        piece = pl.ds((me // 2) * part, part)
        return pltpu.make_async_remote_copy(
            src_ref=source.at[piece],
            dst_ref=out.at[s, piece],
            send_sem=two_send.at[g, s, n],
            recv_sem=two_recv.at[g, s, n],
            device_id=peer(lax.rem(me + 2 * n, grid)),
            device_id_type=MESH,
        )

    for g in range(2):
        for s in range(2):

            @pl.when(groups[g][2] == s)
            def _():
                for n in hop_order(grid):
                    first(g, s, n).start()

    for g in range(2):
        source, out, me, _ = groups[g]
        for s in range(2):

            @pl.when(me == s)
            def _():
                out[s, pl.ds(0, part)] = source[pl.ds(0, part)]
                for n in range(1, half):
                    second(g, s, n, source).start()

    for g in range(2):
        _, out, me, _ = groups[g]
        for s in range(2):

            @pl.when(me != s)
            def _():
                piece = pl.ds((me // 2) * part, part)
                pltpu.make_async_remote_copy(
                    src_ref=out.at[s, piece],
                    dst_ref=out.at[s, piece],
                    send_sem=one_send.at[g, 0],
                    recv_sem=one_recv.at[g, s],
                    device_id=groups[g][3](s),
                    device_id_type=MESH,
                ).wait_recv()
                for n in range(1, half):
                    second(g, s, n, out.at[s]).start()

    for g in range(2):
        source, out, me, _ = groups[g]
        for s in range(2):

            @pl.when(me == s)
            def _():
                for n in hop_order(grid):
                    first(g, s, n).wait_send()

            for n in range(1, half):
                second(g, s, n, out.at[s]).wait_send()
                piece = pl.ds(lax.rem(me // 2 + half - n, half) * part, part)
                pltpu.make_async_remote_copy(
                    src_ref=out.at[s, piece],
                    dst_ref=out.at[s, piece],
                    send_sem=two_send.at[g, s, n],
                    recv_sem=two_recv.at[g, s, n],
                    device_id=groups[g][3](lax.rem(me + 2 * n, grid)),
                    device_id_type=MESH,
                ).wait_recv()


def spread(rows, cols, grid):
    spots, size, _ = rows.shape
    half = grid // 2
    shape = jax.ShapeDtypeStruct((2, spots, size, size), F32)
    return pl.pallas_call(
        functools.partial(spread_kernel, grid, spots),
        out_shape=[shape, shape],
        in_specs=[pl.BlockSpec(memory_space=VMEM)] * 2,
        out_specs=[pl.BlockSpec(memory_space=VMEM)] * 2,
        scratch_shapes=[
            pltpu.SemaphoreType.DMA((2, grid)),
            pltpu.SemaphoreType.DMA((2, 2)),
            pltpu.SemaphoreType.DMA((2, 2, half)),
            pltpu.SemaphoreType.DMA((2, 2, half)),
        ],
        compiler_params=pltpu.CompilerParams(collective_id=3, has_side_effects=True),
        cost_estimate=pl.CostEstimate(flops=40_000_000, bytes_accessed=8 * rows.size, transcendentals=0),
        name="spread",
    )(rows, cols)


def split(value):
    high = value.astype(BF16)
    return high, (value - high.astype(F32)).astype(BF16)


def update_kernel(
    spots, row_ref, col_ref, where_ref, front_ref, r0, r1, rows_ref, cols_ref, low_ref, inv_ref, out_ref,
    v_rows, rows_high, rows_low, cols_high, cols_low,
):
    l = pl.program_id(0)
    size = front_ref.shape[-1]
    my_row, my_col = where_ref[1], where_ref[2]
    received = (r0, r1)

    @pl.when(l == 0)
    def _():
        for i in range(spots):
            here = pl.ds(i * size, size)
            v = mm_t(jnp.concatenate([rows_ref[0, i], rows_ref[1, i]], axis=1), inv_ref[...])
            if i == 0:
                low = jnp.where(my_row == 0, low_ref[0], low_ref[1])
                v = jnp.where(my_row < 2, low, v)
            v_rows[here, :] = v
            rows_high[here, :], rows_low[here, :] = split(v)
            w = mm_t(jnp.concatenate([cols_ref[0, i], cols_ref[1, i]], axis=1), inv_ref[...])
            cols_high[here, :], cols_low[here, :] = split(w)

    here = pl.ds(pl.multiple_of(l * size, size), size)
    high, low = rows_high[here, :], rows_low[here, :]
    top = (l == 0) & (my_row < 2)
    for j in range(spots):
        there = pl.ds(j * size, size)

        def dot(a, b):
            return lax.dot_general(a, b, (((1,), (1,)), ((), ())), preferred_element_type=F32)

        ch, cl = cols_high[there, :], cols_low[there, :]
        product = dot(high, ch) + (dot(high, cl) + dot(low, ch))
        parts = []
        for k in range(2):
            index = col_ref[k * spots + j]
            valid = (index >= 0) & (row_ref[k * spots + l] >= 0)
            parts.append((lambda i, k=k: received[k][i // 2, 0, 0, i % 2], index, valid))
        value = added(front_ref[pl.ds(j, size, stride=spots), :], parts) - product
        value = jnp.where(top, 0.0, value)
        if j == 0:
            v = v_rows[here, :]
            value = jnp.where(my_col == 0, v[:, :size], jnp.where(my_col == 1, v[:, size:], value))
        out_ref[pl.ds(j, size, stride=spots), :] = value


def update(flat, received, rows, cols, low, inverse, row_pos, col_pos, where):
    grid, _, blocks, _, size, _ = received.shape
    spots = rows.shape[1]

    def by_row(k):
        return pl.BlockSpec(
            (grid, 1, 1, 2, size, size),
            lambda l, row, *_: (0, k, jnp.maximum(row[k * spots + l], 0), 0, 0, 0),
        )

    def whole(value):
        zeros = (0,) * value.ndim
        return pl.BlockSpec(value.shape, lambda *_: zeros, pipeline_mode=pl.Buffered(1))

    line = pl.BlockSpec((size * spots, size), lambda l, *_: (l, 0))
    order = spots * size
    return pl.pallas_call(
        functools.partial(update_kernel, spots),
        grid_spec=pltpu.PrefetchScalarGridSpec(
            num_scalar_prefetch=3,
            grid=(spots,),
            in_specs=[line, by_row(0), by_row(1), whole(rows), whole(cols), whole(low), whole(inverse)],
            out_specs=line,
            scratch_shapes=[pltpu.VMEM((order, 2 * size), F32)] + [pltpu.VMEM((order, 2 * size), BF16)] * 4,
        ),
        out_shape=jax.ShapeDtypeStruct(flat.shape, F32),
        compiler_params=pltpu.CompilerParams(dimension_semantics=("arbitrary",)),
        cost_estimate=pl.CostEstimate(flops=4_000_000_000, bytes_accessed=12 * flat.size, transcendentals=0),
        name="update",
    )(row_pos.reshape(-1), col_pos.reshape(-1), where, flat, received, received, rows, cols, low, inverse)


def per_device(grid, orig_front, child_updates, index_maps):
    front, row, col = (lax.axis_index(name) for name in ("front", "row", "col"))
    local = orig_front[0, :, 0, :, :, 0, :]
    spots, size, _, _ = local.shape
    flat = local.reshape(spots * size * spots, size)
    child = child_updates[0, :, :, 0, :, :, 0, :]
    row_send, lead_row, lead_col, row_slot, col_send, row_pos, col_pos = tables(
        index_maps, front, row, col, grid, spots
    )
    where = jnp.stack([front, row, col]).astype(I32)
    fcol = local[:, :, 0, :]
    packed, lead = pack_rows(child, fcol[0], row_send, lead_row, lead_col, where, grid)
    lead = lax.psum(lead, ("front", "row", "col"))
    arrived = row_exchange(packed, grid)
    packed = pack_cols(arrived, row_slot, col_send, grid)
    lead = lax.dynamic_index_in_dim(lead, front, 0, keepdims=False)
    received, low, inverse = col_exchange(packed, lead, grid)
    rows, cols = panels(received, fcol, flat, row_pos, col_pos)
    rows, cols = spread(rows, cols, grid)
    out = update(flat, received, rows, cols, low, inverse, row_pos, col_pos, where)
    return out.reshape(1, spots, 1, size, spots, 1, size)


def solution(mesh):
    placed = (
        P("front", None, "row", None, None, "col", None),
        P("front", None, None, "row", None, None, "col", None),
        P(),
    )
    return jax.shard_map(
        functools.partial(per_device, mesh.shape["row"]),
        mesh=mesh,
        in_specs=placed,
        out_specs=P("front", None, "row", None, None, "col", None),
        check_vma=False,
    )
```

```python
import functools

import jax
import jax.numpy as jnp
from jax import lax
from jax.experimental import pallas as pl
from jax.experimental.pallas import tpu as pltpu
from jax.sharding import PartitionSpec as P

F32 = jnp.float32
BF16 = jnp.bfloat16
I32 = jnp.int32
MESH = pl.DeviceIdType.MESH
HIGHEST = lax.Precision.HIGHEST
HBM = pltpu.MemorySpace.HBM
VMEM = pltpu.MemorySpace.VMEM
SMEM = pltpu.MemorySpace.SMEM


def tables(maps, front, row, col, grid, parent_blocks):
    blocks = maps.shape[-1] // grid
    by_source = maps.reshape(2, 2, blocks, grid)
    target = by_source % grid
    place = by_source // grid
    ids = jnp.arange(blocks, dtype=I32)
    before = ids[None, :] < ids[:, None]
    same = target[:, :, :, None, :] == target[:, :, None, :, :]
    order = jnp.sum((same & before[None, None, :, :, None]).astype(I32), axis=3)
    send_slot = target * 2 + order
    recv_slot = jnp.arange(grid, dtype=I32) * 2 + order
    mine = lax.dynamic_index_in_dim(by_source, front, 1, keepdims=False)
    row_send = lax.dynamic_index_in_dim(
        lax.dynamic_index_in_dim(send_slot, front, 1, keepdims=False), row, 2, keepdims=False
    )
    held_rows = lax.dynamic_index_in_dim(mine, row, 2, keepdims=False)
    held_cols = lax.dynamic_index_in_dim(mine, col, 2, keepdims=False)
    lead = jnp.arange(2, dtype=I32)
    lead_row = jnp.sum(
        (held_rows[:, None, :] == lead[None, :, None]).astype(I32) * (ids + 1), axis=-1
    ) - 1
    lead_col = jnp.sum(
        (held_cols[:, None, :] == lead[None, :, None]).astype(I32) * (ids + 1), axis=-1
    ) - 1
    own = lambda value: lax.dynamic_index_in_dim(value, front, 0, keepdims=False)
    own_target, own_place, own_recv = own(target), own(place), own(recv_slot)
    col_send = lax.dynamic_index_in_dim(own(send_slot), col, 2, keepdims=False)
    flat = lambda value: value.reshape(2, blocks * grid)
    row_hit = flat(own_target == row).astype(I32)
    col_hit = flat(own_target == col).astype(I32)
    count = jnp.arange(blocks * grid, dtype=I32)
    rank = jnp.sum(row_hit[:, None, :] * (count[None, :] < count[:, None]).astype(I32), axis=-1)
    row_slot = jnp.sum(
        row_hit[:, None, :] * (rank[:, None, :] == ids[None, :, None]).astype(I32) * flat(own_recv)[:, None, :],
        axis=-1,
    )
    spots = jnp.arange(parent_blocks, dtype=I32)
    at = (flat(own_place)[:, None, :] == spots[None, :, None]).astype(I32)
    row_pos = jnp.sum(row_hit[:, None, :] * at * (rank + 1)[:, None, :], axis=-1) - 1
    col_pos = jnp.sum(col_hit[:, None, :] * at * (flat(own_recv) + 1)[:, None, :], axis=-1) - 1
    slots = jnp.arange(2 * grid, dtype=I32)
    inverse = lambda sent: jnp.sum((sent[:, None, :] == slots[None, :, None]).astype(I32) * ids, axis=-1)
    return inverse(row_send), lead_row, lead_col, row_slot, inverse(col_send), row_pos, col_pos


def meet(peers):
    barrier = pltpu.get_barrier_semaphore()
    for peer in peers:
        pl.semaphore_signal(barrier, inc=1, device_id=peer, device_id_type=MESH)
    pl.semaphore_wait(barrier, len(peers))


def hop_order(grid):
    return [d for pair in zip(range(1, grid), range(grid - 1, 0, -1)) for d in pair][: grid - 1]


def factor_block(work, size):
    lanes = lax.broadcasted_iota(I32, (size, size), 1)
    rows = lax.broadcasted_iota(I32, (size, 1), 0)

    def step(j, carry):
        pivot_row = work[pl.ds(j, 1), :]
        left = work[:, :size]
        column = jnp.sum(jnp.where(lanes == j, left, 0.0), axis=1, keepdims=True)
        pivot = jnp.sum(jnp.where(lanes[:1] == j, pivot_row[:, :size], 0.0), axis=1, keepdims=True)
        scale = jnp.where(rows > j, column / pivot, 0.0)
        work[...] = work[...] - scale * pivot_row
        return carry

    lax.fori_loop(0, size, step, 0)


def triangular(work, size):
    eye = lax.broadcasted_iota(I32, (size, size), 0) == lax.broadcasted_iota(I32, (size, size), 1)
    upper = lax.broadcasted_iota(I32, (size, size), 0) <= lax.broadcasted_iota(I32, (size, size), 1)
    u = work[:, :size]
    root = lax.rsqrt(jnp.sum(jnp.where(eye, u, 0.0), axis=1, keepdims=True))
    lower = jnp.where(upper, u * root, 0.0).T
    inverse = work[:, size:] * root
    return lower, inverse


def mm(a, b):
    return jnp.dot(a, b, precision=HIGHEST, preferred_element_type=F32)


def mm_t(a, b):
    return lax.dot_general(a, b, (((1,), (1,)), ((), ())), precision=HIGHEST, preferred_element_type=F32)


def factor_lead(lead_ref, low_ref, inv_ref, work, size):
    eye = (
        lax.broadcasted_iota(I32, (size, size), 0) == lax.broadcasted_iota(I32, (size, size), 1)
    ).astype(F32)
    work[:, :size] = lead_ref[:size]
    work[:, size:] = eye
    factor_block(work, size)
    l0, i0 = triangular(work, size)
    l10 = mm_t(lead_ref[size : 2 * size], i0)
    work[:, :size] = lead_ref[2 * size :] - mm_t(l10, l10)
    work[:, size:] = eye
    factor_block(work, size)
    l1, i1 = triangular(work, size)
    low_ref[0] = jnp.concatenate([l0, jnp.zeros_like(l0)], axis=1)
    low_ref[1] = jnp.concatenate([l10, l1], axis=1)
    inv_ref[:size, :size] = i0
    inv_ref[:size, size:] = jnp.zeros_like(i0)
    inv_ref[size:, :size] = -mm(i1, mm(l10, i0))
    inv_ref[size:, size:] = i1


LEAD = ((0, 0), (1, 0), (1, 1))


def exchange_kernel(
    grid, size, blocks, spots,
    rows_inv, row_slot, cols_inv, lead_row, lead_col, child_hbm, flat_hbm,
    recv_two, low_ref, inv_ref, fcol_ref,
    child, send_one, recv_one, turned, send_two, wide, chunk, part, sum_one, sum_two, got_one, got_two, lead, work,
    child_sem, chunk_sem, local_sem, one_send, one_recv, two_send, two_recv,
    la_send, la_recv, lb_send, lb_recv, lc_send, lc_recv,
):
    f, r, c = lax.axis_index("front"), lax.axis_index("row"), lax.axis_index("col")
    other = 1 - f
    piece = len(LEAD) * size // grid
    steps = hop_order(grid)
    row_peers = [(0, d) for d in steps] + [(1, 0)] + [(1, d) for d in steps]
    row_at = lambda p, d: (lax.rem(f + p, 2), lax.rem(r + d, grid), c)
    col_at = lambda d: (f, r, lax.rem(c + d, grid))

    def remote(src, dst, send_sem, recv_sem, peer):
        return pltpu.make_async_remote_copy(
            src_ref=src, dst_ref=dst, send_sem=send_sem, recv_sem=recv_sem, device_id=peer, device_id_type=MESH
        )

    def line(n, slot):
        rows = pl.ds(n * size * spots, size * spots)
        return pltpu.make_async_copy(flat_hbm.at[rows], chunk.at[slot], chunk_sem.at[slot])

    loads = [pltpu.make_async_copy(child_hbm.at[p], child.at[p], child_sem.at[p]) for p in range(2)]
    for load in loads:
        load.start()
    line(0, 0).start()
    meet([row_at(p, d) for p, d in row_peers] + [col_at(d) for d in steps])
    for load in loads:
        load.wait()
    line(0, 0).wait()

    corner = chunk[0, pl.ds(0, size, stride=spots), :]
    lane = lax.broadcasted_iota(I32, (size, blocks, size), 1)
    for p in range(2):
        for n, (a, b) in enumerate(LEAD):
            qa, qb = lead_row[2 * p + a], lead_col[2 * p + b]
            block = child[p, jnp.maximum(qa, 0)].astype(F32)
            block = jnp.sum(jnp.where(lane == qb, block, 0.0), axis=1)
            block = jnp.where((qa >= 0) & (qb >= 0), block, 0.0)
            mine = (f == p) & (r == a) & (c == b)
            part[p, pl.ds(n * size, size)] = block + jnp.where(mine, corner, 0.0)
    round_a = []
    for n, (p, d) in enumerate(row_peers):
        peer = row_at(p, d)
        copy = remote(
            part.at[peer[0], pl.ds(peer[1] * piece, piece)],
            got_one.at[f, r], la_send.at[n], la_recv.at[p, d], peer,
        )
        copy.start()
        round_a.append(copy)

    round_one = []
    for p in range(2):
        for n, (q, d) in enumerate(row_peers):
            if q != p:
                continue
            peer = row_at(p, d)
            for s in range(2):
                slot = 2 * peer[1] + s
                send_one[peer[0], slot] = child[peer[0], rows_inv[peer[0] * 2 * grid + slot]]
            copy = remote(
                send_one.at[peer[0], pl.ds(2 * peer[1], 2)],
                recv_one.at[f, pl.ds(2 * r, 2)], one_send.at[n], one_recv.at[p, d], peer,
            )
            copy.start()
            round_one.append(copy)

    def turn(source, k, slot):
        wide[...] = source.astype(F32).reshape(size * blocks, size)
        for j in range(blocks):
            turned[k, slot, j] = wide[pl.ds(j, size, stride=blocks), :].astype(BF16)

    def turn_own(s, carry):
        slot = 2 * r + s
        turn(child[f, rows_inv[f * 2 * grid + slot]], f, slot)
        return carry

    lax.fori_loop(0, 2, turn_own, 0)

    for copy in round_a:
        copy.wait_recv()
    got_one[f, r] = part[f, pl.ds(pl.multiple_of(r * piece, 8), piece)]
    total = got_one[0, 0]
    for k in range(2):
        for n in range(grid):
            if k + n > 0:
                total = total + got_one[k, n]
    sum_one[...] = total
    got_two[c] = total
    round_b = []
    for n, d in enumerate(steps):
        copy = remote(sum_one, got_two.at[c], lb_send.at[n], lb_recv.at[d], col_at(d))
        copy.start()
        round_b.append(copy)

    def finish_child(p):
        k = f if p == 0 else other
        for n, (q, d) in enumerate(row_peers):
            if q != p:
                continue
            round_one[n].wait_recv()
            source = lax.rem(r + grid - d, grid)

            def turn_one(s, carry):
                turn(recv_one[k, 2 * source + s], k, 2 * source + s)
                return carry

            lax.fori_loop(0, 2, turn_one, 0)

        def gather(j, carry):
            row = row_slot[k * blocks + j]
            for slot in range(2 * grid):
                send_two[k, slot // 2, j, slot % 2] = turned[k, row, cols_inv[k * 2 * grid + slot]]
            return carry

        lax.fori_loop(0, blocks, gather, 0)
        sent = []
        for n, d in enumerate(steps):
            peer = col_at(d)
            copy = remote(
                send_two.at[k, peer[2]], recv_two.at[c, k], two_send.at[p, n], two_recv.at[k, d], peer
            )
            copy.start()
            sent.append(copy)
        local = pltpu.make_async_copy(send_two.at[k, c], recv_two.at[c, k], local_sem.at[p])
        local.start()
        return sent, local

    sent_a, local_a = finish_child(0)

    for copy in round_b:
        copy.wait_recv()
    total = got_two[0]
    for n in range(1, grid):
        total = total + got_two[n]
    sum_two[...] = total
    lead[pl.ds(pl.multiple_of(r * piece, 8), piece)] = total
    round_c = []
    for n, d in enumerate(steps):
        copy = remote(
            sum_two, lead.at[pl.ds(pl.multiple_of(r * piece, 8), piece)], lc_send.at[n], lc_recv.at[d], row_at(0, d)
        )
        copy.start()
        round_c.append(copy)

    sent_b, local_b = finish_child(1)

    for n in range(spots):
        line(n, n % 2).start()
        if n > 0:
            line(n - 1, (n - 1) % 2).wait()
            fcol_ref[n - 1] = chunk[(n - 1) % 2, pl.ds(0, size, stride=spots), :]
    line(spots - 1, (spots - 1) % 2).wait()
    fcol_ref[spots - 1] = chunk[(spots - 1) % 2, pl.ds(0, size, stride=spots), :]

    for n, d in enumerate(steps):
        source = pl.ds(pl.multiple_of(lax.rem(r + grid - d, grid) * piece, 8), piece)
        remote(sum_two, lead.at[source], lc_send.at[n], lc_recv.at[d], row_at(0, d)).wait_recv()
    factor_lead(lead, low_ref, inv_ref, work, size)

    for copy in round_a + round_b + round_c + round_one:
        copy.wait_send()
    for sent, local, k in ((sent_a, local_a, f), (sent_b, local_b, other)):
        local.wait()
        for n, d in enumerate(steps):
            sent[n].wait_send()
            sent[n].wait_recv()


def exchange(child, flat, rows_inv, row_slot, cols_inv, lead_row, lead_col, grid, spots):
    _, blocks, size, _, _ = child.shape
    piece = len(LEAD) * size // grid
    dma = pltpu.SemaphoreType.DMA
    smem = pl.BlockSpec(memory_space=SMEM)
    hbm = pl.BlockSpec(memory_space=HBM)
    vmem = pl.BlockSpec(memory_space=VMEM)
    return pl.pallas_call(
        functools.partial(exchange_kernel, grid, size, blocks, spots),
        out_shape=[
            jax.ShapeDtypeStruct((grid, 2, blocks, 2, size, size), BF16),
            jax.ShapeDtypeStruct((2, size, 2 * size), F32),
            jax.ShapeDtypeStruct((2 * size, 2 * size), F32),
            jax.ShapeDtypeStruct((spots, size, size), F32),
        ],
        in_specs=[smem] * 5 + [hbm] * 2,
        out_specs=[hbm, vmem, vmem, vmem],
        scratch_shapes=[
            pltpu.VMEM(child.shape, BF16),
            pltpu.VMEM((2, 2 * grid, size, blocks, size), BF16),
            pltpu.VMEM((2, 2 * grid, size, blocks, size), BF16),
            pltpu.VMEM((2, 2 * grid, blocks, size, size), BF16),
            pltpu.VMEM((2, grid, blocks, 2, size, size), BF16),
            pltpu.VMEM((size * blocks, size), F32),
            pltpu.VMEM((2, size * spots, size), F32),
            pltpu.VMEM((2, len(LEAD) * size, size), F32),
            pltpu.VMEM((piece, size), F32),
            pltpu.VMEM((piece, size), F32),
            pltpu.VMEM((2, grid, piece, size), F32),
            pltpu.VMEM((grid, piece, size), F32),
            pltpu.VMEM((len(LEAD) * size, size), F32),
            pltpu.VMEM((size, 2 * size), F32),
            dma((2,)),
            dma((2,)),
            dma((2,)),
            dma((2 * grid,)),
            dma((2, grid)),
            dma((2, grid)),
            dma((2, grid)),
            dma((2 * grid,)),
            dma((2, grid)),
            dma((grid,)),
            dma((grid,)),
            dma((grid,)),
            dma((grid,)),
        ],
        compiler_params=pltpu.CompilerParams(
            collective_id=1, has_side_effects=True, vmem_limit_bytes=60 * 2**20
        ),
        cost_estimate=pl.CostEstimate(flops=400_000_000, bytes_accessed=8 * child.size, transcendentals=0),
        name="exchange",
    )(rows_inv.reshape(-1), row_slot.reshape(-1), cols_inv.reshape(-1), lead_row.reshape(-1), lead_col.reshape(-1), child, flat)


def added(base, parts):
    for ref, index, valid in parts:
        base = base + jnp.where(valid, ref(jnp.maximum(index, 0)).astype(F32), 0.0)
    return base


def panel_kernel(spots, row_ref, col_ref, fcol_ref, frow_ref, c0, c1, r0, r1, rows_out, cols_out):
    size = fcol_ref.shape[-1]
    cols = (c0, c1)
    rows = (r0, r1)
    for l in range(spots):
        parts = []
        for k in range(2):
            index = row_ref[k * spots + l]
            valid = (index >= 0) & (col_ref[k * spots] >= 0)
            parts.append((lambda i, k=k: cols[k][0, 0, i, 0], index, valid))
        rows_out[l] = added(fcol_ref[l], parts)
        parts = []
        for k in range(2):
            index = col_ref[k * spots + l]
            valid = (index >= 0) & (row_ref[k * spots] >= 0)
            parts.append((lambda i, k=k: rows[k][i // 2, 0, 0, i % 2], index, valid))
        cols_out[l] = added(frow_ref[pl.ds(l, size, stride=spots), :], parts).T


def panels(received, fcol, flat, row_pos, col_pos):
    grid, _, blocks, _, size, _ = received.shape
    spots = fcol.shape[0]

    def by_col(k):
        def index(_, row, col):
            i = jnp.maximum(col[k * spots], 0)
            return (i // 2, k, 0, i % 2, 0, 0)

        return pl.BlockSpec((1, 1, blocks, 1, size, size), index)

    def by_row(k):
        return pl.BlockSpec(
            (grid, 1, 1, 2, size, size),
            lambda _, row, col: (0, k, jnp.maximum(row[k * spots], 0), 0, 0, 0),
        )

    shape = jax.ShapeDtypeStruct((spots, size, size), F32)
    whole = pl.BlockSpec((spots, size, size), lambda *_: (0, 0, 0))
    return pl.pallas_call(
        functools.partial(panel_kernel, spots),
        grid_spec=pltpu.PrefetchScalarGridSpec(
            num_scalar_prefetch=2,
            grid=(1,),
            in_specs=[
                whole,
                pl.BlockSpec((size * spots, size), lambda *_: (0, 0)),
                by_col(0),
                by_col(1),
                by_row(0),
                by_row(1),
            ],
            out_specs=[whole, whole],
        ),
        out_shape=[shape, shape],
        cost_estimate=pl.CostEstimate(flops=2_000_000, bytes_accessed=6_000_000, transcendentals=0),
        name="panels",
    )(row_pos.reshape(-1), col_pos.reshape(-1), fcol, flat, received, received, received, received)


def spread_kernel(grid, spots, rows_ref, cols_ref, rows_out, cols_out, one_send, one_recv, two_send, two_recv):
    f, r, c = lax.axis_index("front"), lax.axis_index("row"), lax.axis_index("col")
    half = grid // 2
    part = spots // half
    row_peer = lambda i: (f, r, i)
    col_peer = lambda i: (f, i, c)
    groups = ((rows_ref, rows_out, c, row_peer), (cols_ref, cols_out, r, col_peer))
    meet([peer(lax.rem(me + d, grid)) for _, _, me, peer in groups for d in range(1, grid)])

    def first(g, s, n):
        source, out, me, peer = groups[g]
        to = lax.rem(s + n, grid)
        piece = pl.ds((to // 2) * part, part)
        return pltpu.make_async_remote_copy(
            src_ref=source.at[piece],
            dst_ref=out.at[s, piece],
            send_sem=one_send.at[g, n],
            recv_sem=one_recv.at[g, s],
            device_id=peer(to),
            device_id_type=MESH,
        )

    def second(g, s, n, source):
        _, out, me, peer = groups[g]
        piece = pl.ds((me // 2) * part, part)
        return pltpu.make_async_remote_copy(
            src_ref=source.at[piece],
            dst_ref=out.at[s, piece],
            send_sem=two_send.at[g, s, n],
            recv_sem=two_recv.at[g, s, n],
            device_id=peer(lax.rem(me + 2 * n, grid)),
            device_id_type=MESH,
        )

    for g in range(2):
        for s in range(2):

            @pl.when(groups[g][2] == s)
            def _():
                for n in hop_order(grid):
                    first(g, s, n).start()

    for g in range(2):
        source, out, me, _ = groups[g]
        for s in range(2):

            @pl.when(me == s)
            def _():
                out[s, pl.ds(0, part)] = source[pl.ds(0, part)]
                for n in range(1, half):
                    second(g, s, n, source).start()

    for g in range(2):
        _, out, me, _ = groups[g]
        for s in range(2):

            @pl.when(me != s)
            def _():
                piece = pl.ds((me // 2) * part, part)
                pltpu.make_async_remote_copy(
                    src_ref=out.at[s, piece],
                    dst_ref=out.at[s, piece],
                    send_sem=one_send.at[g, 0],
                    recv_sem=one_recv.at[g, s],
                    device_id=groups[g][3](s),
                    device_id_type=MESH,
                ).wait_recv()
                for n in range(1, half):
                    second(g, s, n, out.at[s]).start()

    for g in range(2):
        source, out, me, _ = groups[g]
        for s in range(2):

            @pl.when(me == s)
            def _():
                for n in hop_order(grid):
                    first(g, s, n).wait_send()

            for n in range(1, half):
                second(g, s, n, out.at[s]).wait_send()
                piece = pl.ds(lax.rem(me // 2 + half - n, half) * part, part)
                pltpu.make_async_remote_copy(
                    src_ref=out.at[s, piece],
                    dst_ref=out.at[s, piece],
                    send_sem=two_send.at[g, s, n],
                    recv_sem=two_recv.at[g, s, n],
                    device_id=groups[g][3](lax.rem(me + 2 * n, grid)),
                    device_id_type=MESH,
                ).wait_recv()


def spread(rows, cols, grid):
    spots, size, _ = rows.shape
    half = grid // 2
    shape = jax.ShapeDtypeStruct((2, spots, size, size), F32)
    return pl.pallas_call(
        functools.partial(spread_kernel, grid, spots),
        out_shape=[shape, shape],
        in_specs=[pl.BlockSpec(memory_space=VMEM)] * 2,
        out_specs=[pl.BlockSpec(memory_space=VMEM)] * 2,
        scratch_shapes=[
            pltpu.SemaphoreType.DMA((2, grid)),
            pltpu.SemaphoreType.DMA((2, 2)),
            pltpu.SemaphoreType.DMA((2, 2, half)),
            pltpu.SemaphoreType.DMA((2, 2, half)),
        ],
        compiler_params=pltpu.CompilerParams(collective_id=3, has_side_effects=True),
        cost_estimate=pl.CostEstimate(flops=40_000_000, bytes_accessed=8 * rows.size, transcendentals=0),
        name="spread",
    )(rows, cols)


def split(value):
    high = value.astype(BF16)
    return high, (value - high.astype(F32)).astype(BF16)


def update_kernel(
    spots, row_ref, col_ref, where_ref, front_ref, r0, r1, rows_ref, cols_ref, low_ref, inv_ref, out_ref,
    v_rows, rows_high, rows_low, cols_high, cols_low,
):
    l = pl.program_id(0)
    size = front_ref.shape[-1]
    my_row, my_col = where_ref[1], where_ref[2]
    received = (r0, r1)

    @pl.when(l == 0)
    def _():
        for i in range(spots):
            here = pl.ds(i * size, size)
            v = mm_t(jnp.concatenate([rows_ref[0, i], rows_ref[1, i]], axis=1), inv_ref[...])
            if i == 0:
                low = jnp.where(my_row == 0, low_ref[0], low_ref[1])
                v = jnp.where(my_row < 2, low, v)
            v_rows[here, :] = v
            rows_high[here, :], rows_low[here, :] = split(v)
            w = mm_t(jnp.concatenate([cols_ref[0, i], cols_ref[1, i]], axis=1), inv_ref[...])
            cols_high[here, :], cols_low[here, :] = split(w)

    here = pl.ds(pl.multiple_of(l * size, size), size)
    high, low = rows_high[here, :], rows_low[here, :]
    top = (l == 0) & (my_row < 2)
    for j in range(spots):
        there = pl.ds(j * size, size)

        def dot(a, b):
            return lax.dot_general(a, b, (((1,), (1,)), ((), ())), preferred_element_type=F32)

        ch, cl = cols_high[there, :], cols_low[there, :]
        product = dot(high, ch) + (dot(high, cl) + dot(low, ch))
        parts = []
        for k in range(2):
            index = col_ref[k * spots + j]
            valid = (index >= 0) & (row_ref[k * spots + l] >= 0)
            parts.append((lambda i, k=k: received[k][i // 2, 0, 0, i % 2], index, valid))
        value = added(front_ref[pl.ds(j, size, stride=spots), :], parts) - product
        value = jnp.where(top, 0.0, value)
        if j == 0:
            v = v_rows[here, :]
            value = jnp.where(my_col == 0, v[:, :size], jnp.where(my_col == 1, v[:, size:], value))
        out_ref[pl.ds(j, size, stride=spots), :] = value


def update(flat, received, rows, cols, low, inverse, row_pos, col_pos, where):
    grid, _, blocks, _, size, _ = received.shape
    spots = rows.shape[1]

    def by_row(k):
        return pl.BlockSpec(
            (grid, 1, 1, 2, size, size),
            lambda l, row, *_: (0, k, jnp.maximum(row[k * spots + l], 0), 0, 0, 0),
        )

    def whole(value):
        zeros = (0,) * value.ndim
        return pl.BlockSpec(value.shape, lambda *_: zeros, pipeline_mode=pl.Buffered(1))

    line = pl.BlockSpec((size * spots, size), lambda l, *_: (l, 0))
    order = spots * size
    return pl.pallas_call(
        functools.partial(update_kernel, spots),
        grid_spec=pltpu.PrefetchScalarGridSpec(
            num_scalar_prefetch=3,
            grid=(spots,),
            in_specs=[line, by_row(0), by_row(1), whole(rows), whole(cols), whole(low), whole(inverse)],
            out_specs=line,
            scratch_shapes=[pltpu.VMEM((order, 2 * size), F32)] + [pltpu.VMEM((order, 2 * size), BF16)] * 4,
        ),
        out_shape=jax.ShapeDtypeStruct(flat.shape, F32),
        compiler_params=pltpu.CompilerParams(dimension_semantics=("arbitrary",)),
        cost_estimate=pl.CostEstimate(flops=4_000_000_000, bytes_accessed=12 * flat.size, transcendentals=0),
        name="update",
    )(row_pos.reshape(-1), col_pos.reshape(-1), where, flat, received, received, rows, cols, low, inverse)


def per_device(grid, orig_front, child_updates, index_maps):
    front, row, col = (lax.axis_index(name) for name in ("front", "row", "col"))
    local = orig_front[0, :, 0, :, :, 0, :]
    spots, size, _, _ = local.shape
    flat = local.reshape(spots * size * spots, size)
    child = child_updates[0, :, :, 0, :, :, 0, :]
    rows_inv, lead_row, lead_col, row_slot, cols_inv, row_pos, col_pos = tables(
        index_maps, front, row, col, grid, spots
    )
    where = jnp.stack([front, row, col]).astype(I32)
    received, low, inverse, fcol = exchange(
        child, flat, rows_inv, row_slot, cols_inv, lead_row, lead_col, grid, spots
    )
    rows, cols = panels(received, fcol, flat, row_pos, col_pos)
    rows, cols = spread(rows, cols, grid)
    out = update(flat, received, rows, cols, low, inverse, row_pos, col_pos, where)
    return out.reshape(1, spots, 1, size, spots, 1, size)


def solution(mesh):
    placed = (
        P("front", None, "row", None, None, "col", None),
        P("front", None, None, "row", None, None, "col", None),
        P(),
    )
    return jax.shard_map(
        functools.partial(per_device, mesh.shape["row"]),
        mesh=mesh,
        in_specs=placed,
        out_specs=P("front", None, "row", None, None, "col", None),
        check_vma=False,
    )
```

```python
import functools

import jax
import jax.numpy as jnp
from jax import lax
from jax.experimental import pallas as pl
from jax.experimental.pallas import tpu as pltpu
from jax.sharding import PartitionSpec as P

F32 = jnp.float32
BF16 = jnp.bfloat16
I32 = jnp.int32
MESH = pl.DeviceIdType.MESH
HIGHEST = lax.Precision.HIGHEST
HBM = pltpu.MemorySpace.HBM
VMEM = pltpu.MemorySpace.VMEM
SMEM = pltpu.MemorySpace.SMEM


def tables(maps, front, row, col, grid, parent_blocks):
    blocks = maps.shape[-1] // grid
    by_source = maps.reshape(2, 2, blocks, grid)
    target = by_source % grid
    place = by_source // grid
    ids = jnp.arange(blocks, dtype=I32)
    before = ids[None, :] < ids[:, None]
    same = target[:, :, :, None, :] == target[:, :, None, :, :]
    order = jnp.sum((same & before[None, None, :, :, None]).astype(I32), axis=3)
    send_slot = target * 2 + order
    recv_slot = jnp.arange(grid, dtype=I32) * 2 + order
    mine = lax.dynamic_index_in_dim(by_source, front, 1, keepdims=False)
    row_send = lax.dynamic_index_in_dim(
        lax.dynamic_index_in_dim(send_slot, front, 1, keepdims=False), row, 2, keepdims=False
    )
    held_rows = lax.dynamic_index_in_dim(mine, row, 2, keepdims=False)
    held_cols = lax.dynamic_index_in_dim(mine, col, 2, keepdims=False)
    lead = jnp.arange(2, dtype=I32)
    lead_row = jnp.sum(
        (held_rows[:, None, :] == lead[None, :, None]).astype(I32) * (ids + 1), axis=-1
    ) - 1
    lead_col = jnp.sum(
        (held_cols[:, None, :] == lead[None, :, None]).astype(I32) * (ids + 1), axis=-1
    ) - 1
    own = lambda value: lax.dynamic_index_in_dim(value, front, 0, keepdims=False)
    own_target, own_place, own_recv = own(target), own(place), own(recv_slot)
    col_send = lax.dynamic_index_in_dim(own(send_slot), col, 2, keepdims=False)
    flat = lambda value: value.reshape(2, blocks * grid)
    row_hit = flat(own_target == row).astype(I32)
    col_hit = flat(own_target == col).astype(I32)
    count = jnp.arange(blocks * grid, dtype=I32)
    rank = jnp.sum(row_hit[:, None, :] * (count[None, :] < count[:, None]).astype(I32), axis=-1)
    row_slot = jnp.sum(
        row_hit[:, None, :] * (rank[:, None, :] == ids[None, :, None]).astype(I32) * flat(own_recv)[:, None, :],
        axis=-1,
    )
    spots = jnp.arange(parent_blocks, dtype=I32)
    at = (flat(own_place)[:, None, :] == spots[None, :, None]).astype(I32)
    row_pos = jnp.sum(row_hit[:, None, :] * at * (rank + 1)[:, None, :], axis=-1) - 1
    col_pos = jnp.sum(col_hit[:, None, :] * at * (flat(own_recv) + 1)[:, None, :], axis=-1) - 1
    slots = jnp.arange(2 * grid, dtype=I32)
    inverse = lambda sent: jnp.sum((sent[:, None, :] == slots[None, :, None]).astype(I32) * ids, axis=-1)
    return inverse(row_send), lead_row, lead_col, row_slot, inverse(col_send), row_pos, col_pos


def meet(peers):
    barrier = pltpu.get_barrier_semaphore()
    for peer in peers:
        pl.semaphore_signal(barrier, inc=1, device_id=peer, device_id_type=MESH)
    pl.semaphore_wait(barrier, len(peers))


def hop_order(grid):
    return [d for pair in zip(range(1, grid), range(grid - 1, 0, -1)) for d in pair][: grid - 1]


def factor_block(work, size):
    lanes = lax.broadcasted_iota(I32, (size, size), 1)
    rows = lax.broadcasted_iota(I32, (size, 1), 0)

    def step(j, carry):
        pivot_row = work[pl.ds(j, 1), :]
        left = work[:, :size]
        column = jnp.sum(jnp.where(lanes == j, left, 0.0), axis=1, keepdims=True)
        pivot = jnp.sum(jnp.where(lanes[:1] == j, pivot_row[:, :size], 0.0), axis=1, keepdims=True)
        scale = jnp.where(rows > j, column / pivot, 0.0)
        work[...] = work[...] - scale * pivot_row
        return carry

    lax.fori_loop(0, size, step, 0)


def triangular(work, size):
    eye = lax.broadcasted_iota(I32, (size, size), 0) == lax.broadcasted_iota(I32, (size, size), 1)
    upper = lax.broadcasted_iota(I32, (size, size), 0) <= lax.broadcasted_iota(I32, (size, size), 1)
    u = work[:, :size]
    root = lax.rsqrt(jnp.sum(jnp.where(eye, u, 0.0), axis=1, keepdims=True))
    lower = jnp.where(upper, u * root, 0.0).T
    inverse = work[:, size:] * root
    return lower, inverse


def mm(a, b):
    return jnp.dot(a, b, precision=HIGHEST, preferred_element_type=F32)


def mm_t(a, b):
    return lax.dot_general(a, b, (((1,), (1,)), ((), ())), precision=HIGHEST, preferred_element_type=F32)


def factor_lead(lead_ref, low_ref, inv_ref, work, size):
    eye = (
        lax.broadcasted_iota(I32, (size, size), 0) == lax.broadcasted_iota(I32, (size, size), 1)
    ).astype(F32)
    work[:, :size] = lead_ref[:size]
    work[:, size:] = eye
    factor_block(work, size)
    l0, i0 = triangular(work, size)
    l10 = mm_t(lead_ref[size : 2 * size], i0)
    work[:, :size] = lead_ref[2 * size :] - mm_t(l10, l10)
    work[:, size:] = eye
    factor_block(work, size)
    l1, i1 = triangular(work, size)
    low_ref[0] = jnp.concatenate([l0, jnp.zeros_like(l0)], axis=1)
    low_ref[1] = jnp.concatenate([l10, l1], axis=1)
    inv_ref[:size, :size] = i0
    inv_ref[:size, size:] = jnp.zeros_like(i0)
    inv_ref[size:, :size] = -mm(i1, mm(l10, i0))
    inv_ref[size:, size:] = i1


LEAD = ((0, 0), (1, 0), (1, 1))


def exchange_kernel(
    grid, size, blocks, spots,
    rows_inv, row_slot, cols_inv, lead_row, lead_col, child_hbm, flat_hbm,
    recv_two, low_ref, inv_ref, fcol_ref,
    child, send_one, recv_one, turned, send_two, wide, chunk, part, sum_one, sum_two, got_one, got_two, lead, work,
    child_sem, chunk_sem, local_sem, one_send, one_recv, two_send, two_recv,
    la_send, la_recv, lb_send, lb_recv, lc_send, lc_recv,
):
    f, r, c = lax.axis_index("front"), lax.axis_index("row"), lax.axis_index("col")
    other = 1 - f
    piece = len(LEAD) * size // grid
    steps = hop_order(grid)
    row_peers = [(0, d) for d in steps] + [(1, 0)] + [(1, d) for d in steps]
    row_at = lambda p, d: (lax.rem(f + p, 2), lax.rem(r + d, grid), c)
    col_at = lambda d: (f, r, lax.rem(c + d, grid))

    def remote(src, dst, send_sem, recv_sem, peer):
        return pltpu.make_async_remote_copy(
            src_ref=src, dst_ref=dst, send_sem=send_sem, recv_sem=recv_sem, device_id=peer, device_id_type=MESH
        )

    def line(n, slot):
        rows = pl.ds(n * size * spots, size * spots)
        return pltpu.make_async_copy(flat_hbm.at[rows], chunk.at[slot], chunk_sem.at[slot])

    loads = [pltpu.make_async_copy(child_hbm.at[p], child.at[p], child_sem.at[p]) for p in range(2)]
    for load in loads:
        load.start()
    line(0, 0).start()
    meet([row_at(p, d) for p, d in row_peers] + [col_at(d) for d in steps])
    for load in loads:
        load.wait()
    line(0, 0).wait()

    corner = chunk[0, pl.ds(0, size, stride=spots), :]
    lane = lax.broadcasted_iota(I32, (size, blocks, size), 1)
    for p in range(2):
        for n, (a, b) in enumerate(LEAD):
            qa, qb = lead_row[2 * p + a], lead_col[2 * p + b]
            block = child[p, jnp.maximum(qa, 0)].astype(F32)
            block = jnp.sum(jnp.where(lane == qb, block, 0.0), axis=1)
            block = jnp.where((qa >= 0) & (qb >= 0), block, 0.0)
            mine = (f == p) & (r == a) & (c == b)
            part[p, pl.ds(n * size, size)] = block + jnp.where(mine, corner, 0.0)
    round_a = []
    for n, (p, d) in enumerate(row_peers):
        peer = row_at(p, d)
        copy = remote(
            part.at[peer[0], pl.ds(peer[1] * piece, piece)],
            got_one.at[f, r], la_send.at[n], la_recv.at[p, d], peer,
        )
        copy.start()
        round_a.append(copy)

    round_one = []
    for p in range(2):
        for n, (q, d) in enumerate(row_peers):
            if q != p:
                continue
            peer = row_at(p, d)
            for s in range(2):
                slot = 2 * peer[1] + s
                send_one[peer[0], slot] = child[peer[0], rows_inv[peer[0] * 2 * grid + slot]]
            copy = remote(
                send_one.at[peer[0], pl.ds(2 * peer[1], 2)],
                recv_one.at[f, pl.ds(2 * r, 2)], one_send.at[n], one_recv.at[p, d], peer,
            )
            copy.start()
            round_one.append(copy)

    def turn(source, k, slot):
        wide[...] = source.astype(F32).reshape(size * blocks, size)
        for j in range(blocks):
            turned[k, slot, j] = wide[pl.ds(j, size, stride=blocks), :].astype(BF16)

    def turn_own(s, carry):
        slot = 2 * r + s
        turn(child[f, rows_inv[f * 2 * grid + slot]], f, slot)
        return carry

    lax.fori_loop(0, 2, turn_own, 0)

    for copy in round_a:
        copy.wait_recv()
    got_one[f, r] = part[f, pl.ds(pl.multiple_of(r * piece, 8), piece)]
    total = got_one[0, 0]
    for k in range(2):
        for n in range(grid):
            if k + n > 0:
                total = total + got_one[k, n]
    sum_one[...] = total
    got_two[c] = total
    round_b = []
    for n, d in enumerate(steps):
        copy = remote(sum_one, got_two.at[c], lb_send.at[n], lb_recv.at[d], col_at(d))
        copy.start()
        round_b.append(copy)

    def finish_child(p):
        k = f if p == 0 else other
        for n, (q, d) in enumerate(row_peers):
            if q != p:
                continue
            round_one[n].wait_recv()
            source = lax.rem(r + grid - d, grid)

            def turn_one(s, carry):
                turn(recv_one[k, 2 * source + s], k, 2 * source + s)
                return carry

            lax.fori_loop(0, 2, turn_one, 0)

        def gather(j, carry):
            row = row_slot[k * blocks + j]
            for slot in range(2 * grid):
                send_two[k, slot // 2, j, slot % 2] = turned[k, row, cols_inv[k * 2 * grid + slot]]
            return carry

        lax.fori_loop(0, blocks, gather, 0)
        local = pltpu.make_async_copy(send_two.at[k, c], recv_two.at[c, k], local_sem.at[p])
        local.start()
        return local

    def send_child(p, which):
        k = f if p == 0 else other
        for n, d in enumerate(steps):
            if d % 2 == which:
                peer = col_at(d)
                copy = remote(
                    send_two.at[k, peer[2]], recv_two.at[c, k], two_send.at[p, n], two_recv.at[k, d], peer
                )
                copy.start()
                round_two.append(copy)

    round_two = []
    local_a = finish_child(0)
    send_child(0, 0)

    for copy in round_b:
        copy.wait_recv()
    total = got_two[0]
    for n in range(1, grid):
        total = total + got_two[n]
    sum_two[...] = total
    lead[pl.ds(pl.multiple_of(r * piece, 8), piece)] = total
    round_c = []
    for n, d in enumerate(steps):
        copy = remote(
            sum_two, lead.at[pl.ds(pl.multiple_of(r * piece, 8), piece)], lc_send.at[n], lc_recv.at[d], row_at(0, d)
        )
        copy.start()
        round_c.append(copy)

    local_b = finish_child(1)
    send_child(0, 1)
    send_child(1, 1)
    send_child(1, 0)

    for n in range(spots):
        line(n, n % 2).start()
        if n > 0:
            line(n - 1, (n - 1) % 2).wait()
            fcol_ref[n - 1] = chunk[(n - 1) % 2, pl.ds(0, size, stride=spots), :]
    line(spots - 1, (spots - 1) % 2).wait()
    fcol_ref[spots - 1] = chunk[(spots - 1) % 2, pl.ds(0, size, stride=spots), :]

    for n, d in enumerate(steps):
        source = pl.ds(pl.multiple_of(lax.rem(r + grid - d, grid) * piece, 8), piece)
        remote(sum_two, lead.at[source], lc_send.at[n], lc_recv.at[d], row_at(0, d)).wait_recv()
    factor_lead(lead, low_ref, inv_ref, work, size)

    for copy in round_a + round_b + round_c + round_one:
        copy.wait_send()
    local_a.wait()
    local_b.wait()
    for copy in round_two:
        copy.wait_send()
        copy.wait_recv()


def exchange(child, flat, rows_inv, row_slot, cols_inv, lead_row, lead_col, grid, spots):
    _, blocks, size, _, _ = child.shape
    piece = len(LEAD) * size // grid
    dma = pltpu.SemaphoreType.DMA
    smem = pl.BlockSpec(memory_space=SMEM)
    hbm = pl.BlockSpec(memory_space=HBM)
    vmem = pl.BlockSpec(memory_space=VMEM)
    return pl.pallas_call(
        functools.partial(exchange_kernel, grid, size, blocks, spots),
        out_shape=[
            jax.ShapeDtypeStruct((grid, 2, blocks, 2, size, size), BF16),
            jax.ShapeDtypeStruct((2, size, 2 * size), F32),
            jax.ShapeDtypeStruct((2 * size, 2 * size), F32),
            jax.ShapeDtypeStruct((spots, size, size), F32),
        ],
        in_specs=[smem] * 5 + [hbm] * 2,
        out_specs=[hbm, vmem, vmem, vmem],
        scratch_shapes=[
            pltpu.VMEM(child.shape, BF16),
            pltpu.VMEM((2, 2 * grid, size, blocks, size), BF16),
            pltpu.VMEM((2, 2 * grid, size, blocks, size), BF16),
            pltpu.VMEM((2, 2 * grid, blocks, size, size), BF16),
            pltpu.VMEM((2, grid, blocks, 2, size, size), BF16),
            pltpu.VMEM((size * blocks, size), F32),
            pltpu.VMEM((2, size * spots, size), F32),
            pltpu.VMEM((2, len(LEAD) * size, size), F32),
            pltpu.VMEM((piece, size), F32),
            pltpu.VMEM((piece, size), F32),
            pltpu.VMEM((2, grid, piece, size), F32),
            pltpu.VMEM((grid, piece, size), F32),
            pltpu.VMEM((len(LEAD) * size, size), F32),
            pltpu.VMEM((size, 2 * size), F32),
            dma((2,)),
            dma((2,)),
            dma((2,)),
            dma((2 * grid,)),
            dma((2, grid)),
            dma((2, grid)),
            dma((2, grid)),
            dma((2 * grid,)),
            dma((2, grid)),
            dma((grid,)),
            dma((grid,)),
            dma((grid,)),
            dma((grid,)),
        ],
        compiler_params=pltpu.CompilerParams(
            collective_id=1, has_side_effects=True, vmem_limit_bytes=60 * 2**20
        ),
        cost_estimate=pl.CostEstimate(flops=400_000_000, bytes_accessed=8 * child.size, transcendentals=0),
        name="exchange",
    )(rows_inv.reshape(-1), row_slot.reshape(-1), cols_inv.reshape(-1), lead_row.reshape(-1), lead_col.reshape(-1), child, flat)


def added(base, parts):
    for ref, index, valid in parts:
        base = base + jnp.where(valid, ref(jnp.maximum(index, 0)).astype(F32), 0.0)
    return base


def panel_kernel(spots, row_ref, col_ref, fcol_ref, frow_ref, c0, c1, r0, r1, rows_out, cols_out):
    size = fcol_ref.shape[-1]
    cols = (c0, c1)
    rows = (r0, r1)
    for l in range(spots):
        parts = []
        for k in range(2):
            index = row_ref[k * spots + l]
            valid = (index >= 0) & (col_ref[k * spots] >= 0)
            parts.append((lambda i, k=k: cols[k][0, 0, i, 0], index, valid))
        rows_out[l] = added(fcol_ref[l], parts)
        parts = []
        for k in range(2):
            index = col_ref[k * spots + l]
            valid = (index >= 0) & (row_ref[k * spots] >= 0)
            parts.append((lambda i, k=k: rows[k][i // 2, 0, 0, i % 2], index, valid))
        cols_out[l] = added(frow_ref[pl.ds(l, size, stride=spots), :], parts).T


def panels(received, fcol, flat, row_pos, col_pos):
    grid, _, blocks, _, size, _ = received.shape
    spots = fcol.shape[0]

    def by_col(k):
        def index(_, row, col):
            i = jnp.maximum(col[k * spots], 0)
            return (i // 2, k, 0, i % 2, 0, 0)

        return pl.BlockSpec((1, 1, blocks, 1, size, size), index)

    def by_row(k):
        return pl.BlockSpec(
            (grid, 1, 1, 2, size, size),
            lambda _, row, col: (0, k, jnp.maximum(row[k * spots], 0), 0, 0, 0),
        )

    shape = jax.ShapeDtypeStruct((spots, size, size), F32)
    whole = pl.BlockSpec((spots, size, size), lambda *_: (0, 0, 0))
    return pl.pallas_call(
        functools.partial(panel_kernel, spots),
        grid_spec=pltpu.PrefetchScalarGridSpec(
            num_scalar_prefetch=2,
            grid=(1,),
            in_specs=[
                whole,
                pl.BlockSpec((size * spots, size), lambda *_: (0, 0)),
                by_col(0),
                by_col(1),
                by_row(0),
                by_row(1),
            ],
            out_specs=[whole, whole],
        ),
        out_shape=[shape, shape],
        cost_estimate=pl.CostEstimate(flops=2_000_000, bytes_accessed=6_000_000, transcendentals=0),
        name="panels",
    )(row_pos.reshape(-1), col_pos.reshape(-1), fcol, flat, received, received, received, received)


def spread_kernel(grid, spots, rows_ref, cols_ref, rows_out, cols_out, one_send, one_recv, two_send, two_recv):
    f, r, c = lax.axis_index("front"), lax.axis_index("row"), lax.axis_index("col")
    half = grid // 2
    part = spots // half
    row_peer = lambda i: (f, r, i)
    col_peer = lambda i: (f, i, c)
    groups = ((rows_ref, rows_out, c, row_peer), (cols_ref, cols_out, r, col_peer))
    meet([peer(lax.rem(me + d, grid)) for _, _, me, peer in groups for d in range(1, grid)])

    def first(g, s, n):
        source, out, me, peer = groups[g]
        to = lax.rem(s + n, grid)
        piece = pl.ds((to // 2) * part, part)
        return pltpu.make_async_remote_copy(
            src_ref=source.at[piece],
            dst_ref=out.at[s, piece],
            send_sem=one_send.at[g, n],
            recv_sem=one_recv.at[g, s],
            device_id=peer(to),
            device_id_type=MESH,
        )

    def second(g, s, n, source):
        _, out, me, peer = groups[g]
        piece = pl.ds((me // 2) * part, part)
        return pltpu.make_async_remote_copy(
            src_ref=source.at[piece],
            dst_ref=out.at[s, piece],
            send_sem=two_send.at[g, s, n],
            recv_sem=two_recv.at[g, s, n],
            device_id=peer(lax.rem(me + 2 * n, grid)),
            device_id_type=MESH,
        )

    for g in range(2):
        for s in range(2):

            @pl.when(groups[g][2] == s)
            def _():
                for n in hop_order(grid):
                    first(g, s, n).start()

    for g in range(2):
        source, out, me, _ = groups[g]
        for s in range(2):

            @pl.when(me == s)
            def _():
                out[s, pl.ds(0, part)] = source[pl.ds(0, part)]
                for n in range(1, half):
                    second(g, s, n, source).start()

    for g in range(2):
        _, out, me, _ = groups[g]
        for s in range(2):

            @pl.when(me != s)
            def _():
                piece = pl.ds((me // 2) * part, part)
                pltpu.make_async_remote_copy(
                    src_ref=out.at[s, piece],
                    dst_ref=out.at[s, piece],
                    send_sem=one_send.at[g, 0],
                    recv_sem=one_recv.at[g, s],
                    device_id=groups[g][3](s),
                    device_id_type=MESH,
                ).wait_recv()
                for n in range(1, half):
                    second(g, s, n, out.at[s]).start()

    for g in range(2):
        source, out, me, _ = groups[g]
        for s in range(2):

            @pl.when(me == s)
            def _():
                for n in hop_order(grid):
                    first(g, s, n).wait_send()

            for n in range(1, half):
                second(g, s, n, out.at[s]).wait_send()
                piece = pl.ds(lax.rem(me // 2 + half - n, half) * part, part)
                pltpu.make_async_remote_copy(
                    src_ref=out.at[s, piece],
                    dst_ref=out.at[s, piece],
                    send_sem=two_send.at[g, s, n],
                    recv_sem=two_recv.at[g, s, n],
                    device_id=groups[g][3](lax.rem(me + 2 * n, grid)),
                    device_id_type=MESH,
                ).wait_recv()


def spread(rows, cols, grid):
    spots, size, _ = rows.shape
    half = grid // 2
    shape = jax.ShapeDtypeStruct((2, spots, size, size), F32)
    return pl.pallas_call(
        functools.partial(spread_kernel, grid, spots),
        out_shape=[shape, shape],
        in_specs=[pl.BlockSpec(memory_space=VMEM)] * 2,
        out_specs=[pl.BlockSpec(memory_space=VMEM)] * 2,
        scratch_shapes=[
            pltpu.SemaphoreType.DMA((2, grid)),
            pltpu.SemaphoreType.DMA((2, 2)),
            pltpu.SemaphoreType.DMA((2, 2, half)),
            pltpu.SemaphoreType.DMA((2, 2, half)),
        ],
        compiler_params=pltpu.CompilerParams(collective_id=3, has_side_effects=True),
        cost_estimate=pl.CostEstimate(flops=40_000_000, bytes_accessed=8 * rows.size, transcendentals=0),
        name="spread",
    )(rows, cols)


def split(value):
    high = value.astype(BF16)
    return high, (value - high.astype(F32)).astype(BF16)


def update_kernel(
    spots, row_ref, col_ref, where_ref, front_ref, r0, r1, rows_ref, cols_ref, low_ref, inv_ref, out_ref,
    v_rows, rows_high, rows_low, cols_high, cols_low,
):
    l = pl.program_id(0)
    size = front_ref.shape[-1]
    my_row, my_col = where_ref[1], where_ref[2]
    received = (r0, r1)

    @pl.when(l == 0)
    def _():
        for i in range(spots):
            here = pl.ds(i * size, size)
            v = mm_t(jnp.concatenate([rows_ref[0, i], rows_ref[1, i]], axis=1), inv_ref[...])
            if i == 0:
                low = jnp.where(my_row == 0, low_ref[0], low_ref[1])
                v = jnp.where(my_row < 2, low, v)
            v_rows[here, :] = v
            rows_high[here, :], rows_low[here, :] = split(v)
            w = mm_t(jnp.concatenate([cols_ref[0, i], cols_ref[1, i]], axis=1), inv_ref[...])
            cols_high[here, :], cols_low[here, :] = split(w)

    here = pl.ds(pl.multiple_of(l * size, size), size)
    high, low = rows_high[here, :], rows_low[here, :]
    top = (l == 0) & (my_row < 2)
    for j in range(spots):
        there = pl.ds(j * size, size)

        def dot(a, b):
            return lax.dot_general(a, b, (((1,), (1,)), ((), ())), preferred_element_type=F32)

        ch, cl = cols_high[there, :], cols_low[there, :]
        product = dot(high, ch) + (dot(high, cl) + dot(low, ch))
        parts = []
        for k in range(2):
            index = col_ref[k * spots + j]
            valid = (index >= 0) & (row_ref[k * spots + l] >= 0)
            parts.append((lambda i, k=k: received[k][i // 2, 0, 0, i % 2], index, valid))
        value = added(front_ref[pl.ds(j, size, stride=spots), :], parts) - product
        value = jnp.where(top, 0.0, value)
        if j == 0:
            v = v_rows[here, :]
            value = jnp.where(my_col == 0, v[:, :size], jnp.where(my_col == 1, v[:, size:], value))
        out_ref[pl.ds(j, size, stride=spots), :] = value


def update(flat, received, rows, cols, low, inverse, row_pos, col_pos, where):
    grid, _, blocks, _, size, _ = received.shape
    spots = rows.shape[1]

    def by_row(k):
        return pl.BlockSpec(
            (grid, 1, 1, 2, size, size),
            lambda l, row, *_: (0, k, jnp.maximum(row[k * spots + l], 0), 0, 0, 0),
        )

    def whole(value):
        zeros = (0,) * value.ndim
        return pl.BlockSpec(value.shape, lambda *_: zeros, pipeline_mode=pl.Buffered(1))

    line = pl.BlockSpec((size * spots, size), lambda l, *_: (l, 0))
    order = spots * size
    return pl.pallas_call(
        functools.partial(update_kernel, spots),
        grid_spec=pltpu.PrefetchScalarGridSpec(
            num_scalar_prefetch=3,
            grid=(spots,),
            in_specs=[line, by_row(0), by_row(1), whole(rows), whole(cols), whole(low), whole(inverse)],
            out_specs=line,
            scratch_shapes=[pltpu.VMEM((order, 2 * size), F32)] + [pltpu.VMEM((order, 2 * size), BF16)] * 4,
        ),
        out_shape=jax.ShapeDtypeStruct(flat.shape, F32),
        compiler_params=pltpu.CompilerParams(dimension_semantics=("arbitrary",)),
        cost_estimate=pl.CostEstimate(flops=4_000_000_000, bytes_accessed=12 * flat.size, transcendentals=0),
        name="update",
    )(row_pos.reshape(-1), col_pos.reshape(-1), where, flat, received, received, rows, cols, low, inverse)


def per_device(grid, orig_front, child_updates, index_maps):
    front, row, col = (lax.axis_index(name) for name in ("front", "row", "col"))
    local = orig_front[0, :, 0, :, :, 0, :]
    spots, size, _, _ = local.shape
    flat = local.reshape(spots * size * spots, size)
    child = child_updates[0, :, :, 0, :, :, 0, :]
    rows_inv, lead_row, lead_col, row_slot, cols_inv, row_pos, col_pos = tables(
        index_maps, front, row, col, grid, spots
    )
    where = jnp.stack([front, row, col]).astype(I32)
    received, low, inverse, fcol = exchange(
        child, flat, rows_inv, row_slot, cols_inv, lead_row, lead_col, grid, spots
    )
    rows, cols = panels(received, fcol, flat, row_pos, col_pos)
    rows, cols = spread(rows, cols, grid)
    out = update(flat, received, rows, cols, low, inverse, row_pos, col_pos, where)
    return out.reshape(1, spots, 1, size, spots, 1, size)


def solution(mesh):
    placed = (
        P("front", None, "row", None, None, "col", None),
        P("front", None, None, "row", None, None, "col", None),
        P(),
    )
    return jax.shard_map(
        functools.partial(per_device, mesh.shape["row"]),
        mesh=mesh,
        in_specs=placed,
        out_specs=P("front", None, "row", None, None, "col", None),
        check_vma=False,
    )
```

```python
import functools

import jax
import jax.numpy as jnp
from jax import lax
from jax.experimental import pallas as pl
from jax.experimental.pallas import tpu as pltpu
from jax.sharding import PartitionSpec as P

F32 = jnp.float32
BF16 = jnp.bfloat16
I32 = jnp.int32
MESH = pl.DeviceIdType.MESH
HIGHEST = lax.Precision.HIGHEST
HBM = pltpu.MemorySpace.HBM
VMEM = pltpu.MemorySpace.VMEM
SMEM = pltpu.MemorySpace.SMEM


def tables(maps, front, row, col, grid, parent_blocks):
    blocks = maps.shape[-1] // grid
    by_source = maps.reshape(2, 2, blocks, grid)
    target = by_source % grid
    place = by_source // grid
    ids = jnp.arange(blocks, dtype=I32)
    before = ids[None, :] < ids[:, None]
    same = target[:, :, :, None, :] == target[:, :, None, :, :]
    order = jnp.sum((same & before[None, None, :, :, None]).astype(I32), axis=3)
    send_slot = target * 2 + order
    recv_slot = jnp.arange(grid, dtype=I32) * 2 + order
    mine = lax.dynamic_index_in_dim(by_source, front, 1, keepdims=False)
    row_send = lax.dynamic_index_in_dim(
        lax.dynamic_index_in_dim(send_slot, front, 1, keepdims=False), row, 2, keepdims=False
    )
    held_rows = lax.dynamic_index_in_dim(mine, row, 2, keepdims=False)
    held_cols = lax.dynamic_index_in_dim(mine, col, 2, keepdims=False)
    lead = jnp.arange(2, dtype=I32)
    lead_row = jnp.sum(
        (held_rows[:, None, :] == lead[None, :, None]).astype(I32) * (ids + 1), axis=-1
    ) - 1
    lead_col = jnp.sum(
        (held_cols[:, None, :] == lead[None, :, None]).astype(I32) * (ids + 1), axis=-1
    ) - 1
    own = lambda value: lax.dynamic_index_in_dim(value, front, 0, keepdims=False)
    own_target, own_place, own_recv = own(target), own(place), own(recv_slot)
    col_send = lax.dynamic_index_in_dim(own(send_slot), col, 2, keepdims=False)
    flat = lambda value: value.reshape(2, blocks * grid)
    row_hit = flat(own_target == row).astype(I32)
    col_hit = flat(own_target == col).astype(I32)
    count = jnp.arange(blocks * grid, dtype=I32)
    rank = jnp.sum(row_hit[:, None, :] * (count[None, :] < count[:, None]).astype(I32), axis=-1)
    row_slot = jnp.sum(
        row_hit[:, None, :] * (rank[:, None, :] == ids[None, :, None]).astype(I32) * flat(own_recv)[:, None, :],
        axis=-1,
    )
    spots = jnp.arange(parent_blocks, dtype=I32)
    at = (flat(own_place)[:, None, :] == spots[None, :, None]).astype(I32)
    row_pos = jnp.sum(row_hit[:, None, :] * at * (rank + 1)[:, None, :], axis=-1) - 1
    col_pos = jnp.sum(col_hit[:, None, :] * at * (flat(own_recv) + 1)[:, None, :], axis=-1) - 1
    slots = jnp.arange(2 * grid, dtype=I32)
    inverse = lambda sent: jnp.sum((sent[:, None, :] == slots[None, :, None]).astype(I32) * ids, axis=-1)
    return inverse(row_send), lead_row, lead_col, row_slot, inverse(col_send), row_pos, col_pos


def meet(peers):
    barrier = pltpu.get_barrier_semaphore()
    for peer in peers:
        pl.semaphore_signal(barrier, inc=1, device_id=peer, device_id_type=MESH)
    pl.semaphore_wait(barrier, len(peers))


def hop_order(grid):
    return [d for pair in zip(range(1, grid), range(grid - 1, 0, -1)) for d in pair][: grid - 1]


def codes(half, flip_cost):
    pairs = [(n, flip) for n in range(half) for flip in range(2) if n + flip > 0]
    return sorted(pairs, key=lambda pair: -(min(pair[0], half - pair[0]) + flip_cost * pair[1]))


def member(me, code, half, sign=1):
    ring = lax.rem(me // 2 + (half + sign * code[0]), half)
    return 2 * ring + lax.rem(me + code[1], 2)


def factor_block(work, size):
    lanes = lax.broadcasted_iota(I32, (size, size), 1)
    rows = lax.broadcasted_iota(I32, (size, 1), 0)

    def step(j, carry):
        pivot_row = work[pl.ds(j, 1), :]
        left = work[:, :size]
        column = jnp.sum(jnp.where(lanes == j, left, 0.0), axis=1, keepdims=True)
        pivot = jnp.sum(jnp.where(lanes[:1] == j, pivot_row[:, :size], 0.0), axis=1, keepdims=True)
        scale = jnp.where(rows > j, column / pivot, 0.0)
        work[...] = work[...] - scale * pivot_row
        return carry

    lax.fori_loop(0, size, step, 0)


def triangular(work, size):
    eye = lax.broadcasted_iota(I32, (size, size), 0) == lax.broadcasted_iota(I32, (size, size), 1)
    upper = lax.broadcasted_iota(I32, (size, size), 0) <= lax.broadcasted_iota(I32, (size, size), 1)
    u = work[:, :size]
    root = lax.rsqrt(jnp.sum(jnp.where(eye, u, 0.0), axis=1, keepdims=True))
    lower = jnp.where(upper, u * root, 0.0).T
    inverse = work[:, size:] * root
    return lower, inverse


def mm(a, b):
    return jnp.dot(a, b, precision=HIGHEST, preferred_element_type=F32)


def mm_t(a, b):
    return lax.dot_general(a, b, (((1,), (1,)), ((), ())), precision=HIGHEST, preferred_element_type=F32)


def factor_lead(lead_ref, low_ref, inv_ref, work, size):
    eye = (
        lax.broadcasted_iota(I32, (size, size), 0) == lax.broadcasted_iota(I32, (size, size), 1)
    ).astype(F32)
    work[:, :size] = lead_ref[:size]
    work[:, size:] = eye
    factor_block(work, size)
    l0, i0 = triangular(work, size)
    l10 = mm_t(lead_ref[size : 2 * size], i0)
    work[:, :size] = lead_ref[2 * size :] - mm_t(l10, l10)
    work[:, size:] = eye
    factor_block(work, size)
    l1, i1 = triangular(work, size)
    low_ref[0] = jnp.concatenate([l0, jnp.zeros_like(l0)], axis=1)
    low_ref[1] = jnp.concatenate([l10, l1], axis=1)
    inv_ref[:size, :size] = i0
    inv_ref[:size, size:] = jnp.zeros_like(i0)
    inv_ref[size:, :size] = -mm(i1, mm(l10, i0))
    inv_ref[size:, size:] = i1


LEAD = ((0, 0), (1, 0), (1, 1))


def exchange_kernel(
    grid, size, blocks, spots,
    rows_inv, row_slot, cols_inv, lead_row, lead_col, child_hbm, flat_hbm,
    recv_two, low_ref, inv_ref, fcol_ref,
    child, send_one, recv_one, turned, send_two, wide, chunk, part, sum_one, sum_two, got_one, got_two, lead, work,
    child_sem, chunk_sem, local_sem, one_send, one_recv, two_send, two_recv,
    la_send, la_recv, lb_send, lb_recv, lc_send, lc_recv,
):
    f, r, c = lax.axis_index("front"), lax.axis_index("row"), lax.axis_index("col")
    other = 1 - f
    piece = len(LEAD) * size // grid
    half = grid // 2
    row_steps, col_steps = codes(half, 1), codes(half, 2)
    row_peers = [(0, d) for d in row_steps] + [(1, d) for d in row_steps] + [(1, (0, 0))]
    row_at = lambda p, d: (lax.rem(f + p, 2), member(r, d, half), c)
    col_at = lambda d: (f, r, member(c, d, half))
    code_of = lambda d: 2 * d[0] + d[1]

    def remote(src, dst, send_sem, recv_sem, peer):
        return pltpu.make_async_remote_copy(
            src_ref=src, dst_ref=dst, send_sem=send_sem, recv_sem=recv_sem, device_id=peer, device_id_type=MESH
        )

    def line(n, slot):
        rows = pl.ds(n * size * spots, size * spots)
        return pltpu.make_async_copy(flat_hbm.at[rows], chunk.at[slot], chunk_sem.at[slot])

    loads = [pltpu.make_async_copy(child_hbm.at[p], child.at[p], child_sem.at[p]) for p in range(2)]
    for load in loads:
        load.start()
    line(0, 0).start()
    meet([row_at(p, d) for p, d in row_peers] + [col_at(d) for d in col_steps])
    for load in loads:
        load.wait()
    line(0, 0).wait()

    corner = chunk[0, pl.ds(0, size, stride=spots), :]
    lane = lax.broadcasted_iota(I32, (size, blocks, size), 1)
    for p in range(2):
        for n, (a, b) in enumerate(LEAD):
            qa, qb = lead_row[2 * p + a], lead_col[2 * p + b]
            block = child[p, jnp.maximum(qa, 0)].astype(F32)
            block = jnp.sum(jnp.where(lane == qb, block, 0.0), axis=1)
            block = jnp.where((qa >= 0) & (qb >= 0), block, 0.0)
            mine = (f == p) & (r == a) & (c == b)
            part[p, pl.ds(n * size, size)] = block + jnp.where(mine, corner, 0.0)
    round_a = []
    for n, (p, d) in enumerate(row_peers):
        peer = row_at(p, d)
        copy = remote(
            part.at[peer[0], pl.ds(peer[1] * piece, piece)],
            got_one.at[f, r], la_send.at[n], la_recv.at[p, code_of(d)], peer,
        )
        copy.start()
        round_a.append(copy)

    round_one = []
    for p in range(2):
        for n, (q, d) in enumerate(row_peers):
            if q != p:
                continue
            peer = row_at(p, d)
            for s in range(2):
                slot = 2 * peer[1] + s
                send_one[peer[0], slot] = child[peer[0], rows_inv[peer[0] * 2 * grid + slot]]
            copy = remote(
                send_one.at[peer[0], pl.ds(2 * peer[1], 2)],
                recv_one.at[f, pl.ds(2 * r, 2)], one_send.at[n], one_recv.at[p, code_of(d)], peer,
            )
            copy.start()
            round_one.append(copy)

    def turn(source, k, slot):
        wide[...] = source.astype(F32).reshape(size * blocks, size)
        for j in range(blocks):
            turned[k, slot, j] = wide[pl.ds(j, size, stride=blocks), :].astype(BF16)

    def turn_own(s, carry):
        slot = 2 * r + s
        turn(child[f, rows_inv[f * 2 * grid + slot]], f, slot)
        return carry

    lax.fori_loop(0, 2, turn_own, 0)

    for copy in round_a:
        copy.wait_recv()
    got_one[f, r] = part[f, pl.ds(pl.multiple_of(r * piece, 8), piece)]
    total = got_one[0, 0]
    for k in range(2):
        for n in range(grid):
            if k + n > 0:
                total = total + got_one[k, n]
    sum_one[...] = total
    got_two[c] = total
    round_b = []
    for n, d in enumerate(col_steps):
        copy = remote(sum_one, got_two.at[c], lb_send.at[n], lb_recv.at[code_of(d)], col_at(d))
        copy.start()
        round_b.append(copy)

    def finish_child(p):
        k = f if p == 0 else other
        for n, (q, d) in enumerate(row_peers):
            if q != p:
                continue
            round_one[n].wait_recv()
            source = member(r, d, half, -1)

            def turn_one(s, carry):
                turn(recv_one[k, 2 * source + s], k, 2 * source + s)
                return carry

            lax.fori_loop(0, 2, turn_one, 0)

        def gather(j, carry):
            row = row_slot[k * blocks + j]
            for slot in range(2 * grid):
                send_two[k, slot // 2, j, slot % 2] = turned[k, row, cols_inv[k * 2 * grid + slot]]
            return carry

        lax.fori_loop(0, blocks, gather, 0)
        sent = []
        for n, d in enumerate(col_steps):
            peer = col_at(d)
            copy = remote(
                send_two.at[k, peer[2]], recv_two.at[c, k], two_send.at[p, n], two_recv.at[k, code_of(d)], peer
            )
            copy.start()
            sent.append(copy)
        local = pltpu.make_async_copy(send_two.at[k, c], recv_two.at[c, k], local_sem.at[p])
        local.start()
        return sent, local

    sent_a, local_a = finish_child(0)

    for copy in round_b:
        copy.wait_recv()
    total = got_two[0]
    for n in range(1, grid):
        total = total + got_two[n]
    sum_two[...] = total
    lead[pl.ds(pl.multiple_of(r * piece, 8), piece)] = total
    round_c = []
    for n, d in enumerate(row_steps):
        copy = remote(
            sum_two, lead.at[pl.ds(pl.multiple_of(r * piece, 8), piece)], lc_send.at[n], lc_recv.at[code_of(d)], row_at(0, d)
        )
        copy.start()
        round_c.append(copy)

    sent_b, local_b = finish_child(1)

    for n in range(spots):
        line(n, n % 2).start()
        if n > 0:
            line(n - 1, (n - 1) % 2).wait()
            fcol_ref[n - 1] = chunk[(n - 1) % 2, pl.ds(0, size, stride=spots), :]
    line(spots - 1, (spots - 1) % 2).wait()
    fcol_ref[spots - 1] = chunk[(spots - 1) % 2, pl.ds(0, size, stride=spots), :]

    for n, d in enumerate(row_steps):
        source = pl.ds(pl.multiple_of(member(r, d, half, -1) * piece, 8), piece)
        remote(sum_two, lead.at[source], lc_send.at[n], lc_recv.at[code_of(d)], row_at(0, d)).wait_recv()
    factor_lead(lead, low_ref, inv_ref, work, size)

    for copy in round_a + round_b + round_c + round_one:
        copy.wait_send()
    for sent, local, k in ((sent_a, local_a, f), (sent_b, local_b, other)):
        local.wait()
        for n in range(len(sent)):
            sent[n].wait_send()
            sent[n].wait_recv()


def exchange(child, flat, rows_inv, row_slot, cols_inv, lead_row, lead_col, grid, spots):
    _, blocks, size, _, _ = child.shape
    piece = len(LEAD) * size // grid
    dma = pltpu.SemaphoreType.DMA
    smem = pl.BlockSpec(memory_space=SMEM)
    hbm = pl.BlockSpec(memory_space=HBM)
    vmem = pl.BlockSpec(memory_space=VMEM)
    return pl.pallas_call(
        functools.partial(exchange_kernel, grid, size, blocks, spots),
        out_shape=[
            jax.ShapeDtypeStruct((grid, 2, blocks, 2, size, size), BF16),
            jax.ShapeDtypeStruct((2, size, 2 * size), F32),
            jax.ShapeDtypeStruct((2 * size, 2 * size), F32),
            jax.ShapeDtypeStruct((spots, size, size), F32),
        ],
        in_specs=[smem] * 5 + [hbm] * 2,
        out_specs=[hbm, vmem, vmem, vmem],
        scratch_shapes=[
            pltpu.VMEM(child.shape, BF16),
            pltpu.VMEM((2, 2 * grid, size, blocks, size), BF16),
            pltpu.VMEM((2, 2 * grid, size, blocks, size), BF16),
            pltpu.VMEM((2, 2 * grid, blocks, size, size), BF16),
            pltpu.VMEM((2, grid, blocks, 2, size, size), BF16),
            pltpu.VMEM((size * blocks, size), F32),
            pltpu.VMEM((2, size * spots, size), F32),
            pltpu.VMEM((2, len(LEAD) * size, size), F32),
            pltpu.VMEM((piece, size), F32),
            pltpu.VMEM((piece, size), F32),
            pltpu.VMEM((2, grid, piece, size), F32),
            pltpu.VMEM((grid, piece, size), F32),
            pltpu.VMEM((len(LEAD) * size, size), F32),
            pltpu.VMEM((size, 2 * size), F32),
            dma((2,)),
            dma((2,)),
            dma((2,)),
            dma((2 * grid,)),
            dma((2, grid)),
            dma((2, grid)),
            dma((2, grid)),
            dma((2 * grid,)),
            dma((2, grid)),
            dma((grid,)),
            dma((grid,)),
            dma((grid,)),
            dma((grid,)),
        ],
        compiler_params=pltpu.CompilerParams(
            collective_id=1, has_side_effects=True, vmem_limit_bytes=60 * 2**20
        ),
        cost_estimate=pl.CostEstimate(flops=400_000_000, bytes_accessed=8 * child.size, transcendentals=0),
        name="exchange",
    )(rows_inv.reshape(-1), row_slot.reshape(-1), cols_inv.reshape(-1), lead_row.reshape(-1), lead_col.reshape(-1), child, flat)


def added(base, parts):
    for ref, index, valid in parts:
        base = base + jnp.where(valid, ref(jnp.maximum(index, 0)).astype(F32), 0.0)
    return base


def panel_kernel(spots, row_ref, col_ref, fcol_ref, frow_ref, c0, c1, r0, r1, rows_out, cols_out):
    size = fcol_ref.shape[-1]
    cols = (c0, c1)
    rows = (r0, r1)
    for l in range(spots):
        parts = []
        for k in range(2):
            index = row_ref[k * spots + l]
            valid = (index >= 0) & (col_ref[k * spots] >= 0)
            parts.append((lambda i, k=k: cols[k][0, 0, i, 0], index, valid))
        rows_out[l] = added(fcol_ref[l], parts)
        parts = []
        for k in range(2):
            index = col_ref[k * spots + l]
            valid = (index >= 0) & (row_ref[k * spots] >= 0)
            parts.append((lambda i, k=k: rows[k][i // 2, 0, 0, i % 2], index, valid))
        cols_out[l] = added(frow_ref[pl.ds(l, size, stride=spots), :], parts).T


def panels(received, fcol, flat, row_pos, col_pos):
    grid, _, blocks, _, size, _ = received.shape
    spots = fcol.shape[0]

    def by_col(k):
        def index(_, row, col):
            i = jnp.maximum(col[k * spots], 0)
            return (i // 2, k, 0, i % 2, 0, 0)

        return pl.BlockSpec((1, 1, blocks, 1, size, size), index)

    def by_row(k):
        return pl.BlockSpec(
            (grid, 1, 1, 2, size, size),
            lambda _, row, col: (0, k, jnp.maximum(row[k * spots], 0), 0, 0, 0),
        )

    shape = jax.ShapeDtypeStruct((spots, size, size), F32)
    whole = pl.BlockSpec((spots, size, size), lambda *_: (0, 0, 0))
    return pl.pallas_call(
        functools.partial(panel_kernel, spots),
        grid_spec=pltpu.PrefetchScalarGridSpec(
            num_scalar_prefetch=2,
            grid=(1,),
            in_specs=[
                whole,
                pl.BlockSpec((size * spots, size), lambda *_: (0, 0)),
                by_col(0),
                by_col(1),
                by_row(0),
                by_row(1),
            ],
            out_specs=[whole, whole],
        ),
        out_shape=[shape, shape],
        cost_estimate=pl.CostEstimate(flops=2_000_000, bytes_accessed=6_000_000, transcendentals=0),
        name="panels",
    )(row_pos.reshape(-1), col_pos.reshape(-1), fcol, flat, received, received, received, received)


def spread_kernel(grid, spots, rows_ref, cols_ref, rows_out, cols_out, one_send, one_recv, two_send, two_recv):
    f, r, c = lax.axis_index("front"), lax.axis_index("row"), lax.axis_index("col")
    half = grid // 2
    part = spots // half
    row_peer = lambda i: (f, r, i)
    col_peer = lambda i: (f, i, c)
    groups = ((rows_ref, rows_out, c, row_peer), (cols_ref, cols_out, r, col_peer))
    meet([peer(lax.rem(me + d, grid)) for _, _, me, peer in groups for d in range(1, grid)])

    def first(g, s, n):
        source, out, me, peer = groups[g]
        to = lax.rem(s + n, grid)
        piece = pl.ds((to // 2) * part, part)
        return pltpu.make_async_remote_copy(
            src_ref=source.at[piece],
            dst_ref=out.at[s, piece],
            send_sem=one_send.at[g, n],
            recv_sem=one_recv.at[g, s],
            device_id=peer(to),
            device_id_type=MESH,
        )

    def second(g, s, n, source):
        _, out, me, peer = groups[g]
        piece = pl.ds((me // 2) * part, part)
        return pltpu.make_async_remote_copy(
            src_ref=source.at[piece],
            dst_ref=out.at[s, piece],
            send_sem=two_send.at[g, s, n],
            recv_sem=two_recv.at[g, s, n],
            device_id=peer(lax.rem(me + 2 * n, grid)),
            device_id_type=MESH,
        )

    for g in range(2):
        for s in range(2):

            @pl.when(groups[g][2] == s)
            def _():
                for n in hop_order(grid):
                    first(g, s, n).start()

    for g in range(2):
        source, out, me, _ = groups[g]
        for s in range(2):

            @pl.when(me == s)
            def _():
                out[s, pl.ds(0, part)] = source[pl.ds(0, part)]
                for n in range(1, half):
                    second(g, s, n, source).start()

    for g in range(2):
        _, out, me, _ = groups[g]
        for s in range(2):

            @pl.when(me != s)
            def _():
                piece = pl.ds((me // 2) * part, part)
                pltpu.make_async_remote_copy(
                    src_ref=out.at[s, piece],
                    dst_ref=out.at[s, piece],
                    send_sem=one_send.at[g, 0],
                    recv_sem=one_recv.at[g, s],
                    device_id=groups[g][3](s),
                    device_id_type=MESH,
                ).wait_recv()
                for n in range(1, half):
                    second(g, s, n, out.at[s]).start()

    for g in range(2):
        source, out, me, _ = groups[g]
        for s in range(2):

            @pl.when(me == s)
            def _():
                for n in hop_order(grid):
                    first(g, s, n).wait_send()

            for n in range(1, half):
                second(g, s, n, out.at[s]).wait_send()
                piece = pl.ds(lax.rem(me // 2 + half - n, half) * part, part)
                pltpu.make_async_remote_copy(
                    src_ref=out.at[s, piece],
                    dst_ref=out.at[s, piece],
                    send_sem=two_send.at[g, s, n],
                    recv_sem=two_recv.at[g, s, n],
                    device_id=groups[g][3](lax.rem(me + 2 * n, grid)),
                    device_id_type=MESH,
                ).wait_recv()


def spread(rows, cols, grid):
    spots, size, _ = rows.shape
    half = grid // 2
    shape = jax.ShapeDtypeStruct((2, spots, size, size), F32)
    return pl.pallas_call(
        functools.partial(spread_kernel, grid, spots),
        out_shape=[shape, shape],
        in_specs=[pl.BlockSpec(memory_space=VMEM)] * 2,
        out_specs=[pl.BlockSpec(memory_space=VMEM)] * 2,
        scratch_shapes=[
            pltpu.SemaphoreType.DMA((2, grid)),
            pltpu.SemaphoreType.DMA((2, 2)),
            pltpu.SemaphoreType.DMA((2, 2, half)),
            pltpu.SemaphoreType.DMA((2, 2, half)),
        ],
        compiler_params=pltpu.CompilerParams(collective_id=3, has_side_effects=True),
        cost_estimate=pl.CostEstimate(flops=40_000_000, bytes_accessed=8 * rows.size, transcendentals=0),
        name="spread",
    )(rows, cols)


def split(value):
    high = value.astype(BF16)
    return high, (value - high.astype(F32)).astype(BF16)


def update_kernel(
    spots, row_ref, col_ref, where_ref, front_ref, r0, r1, rows_ref, cols_ref, low_ref, inv_ref, out_ref,
    v_rows, rows_high, rows_low, cols_high, cols_low,
):
    l = pl.program_id(0)
    size = front_ref.shape[-1]
    my_row, my_col = where_ref[1], where_ref[2]
    received = (r0, r1)

    @pl.when(l == 0)
    def _():
        for i in range(spots):
            here = pl.ds(i * size, size)
            v = mm_t(jnp.concatenate([rows_ref[0, i], rows_ref[1, i]], axis=1), inv_ref[...])
            if i == 0:
                low = jnp.where(my_row == 0, low_ref[0], low_ref[1])
                v = jnp.where(my_row < 2, low, v)
            v_rows[here, :] = v
            rows_high[here, :], rows_low[here, :] = split(v)
            w = mm_t(jnp.concatenate([cols_ref[0, i], cols_ref[1, i]], axis=1), inv_ref[...])
            cols_high[here, :], cols_low[here, :] = split(w)

    here = pl.ds(pl.multiple_of(l * size, size), size)
    high, low = rows_high[here, :], rows_low[here, :]
    top = (l == 0) & (my_row < 2)
    for j in range(spots):
        there = pl.ds(j * size, size)

        def dot(a, b):
            return lax.dot_general(a, b, (((1,), (1,)), ((), ())), preferred_element_type=F32)

        ch, cl = cols_high[there, :], cols_low[there, :]
        product = dot(high, ch) + (dot(high, cl) + dot(low, ch))
        parts = []
        for k in range(2):
            index = col_ref[k * spots + j]
            valid = (index >= 0) & (row_ref[k * spots + l] >= 0)
            parts.append((lambda i, k=k: received[k][i // 2, 0, 0, i % 2], index, valid))
        value = added(front_ref[pl.ds(j, size, stride=spots), :], parts) - product
        value = jnp.where(top, 0.0, value)
        if j == 0:
            v = v_rows[here, :]
            value = jnp.where(my_col == 0, v[:, :size], jnp.where(my_col == 1, v[:, size:], value))
        out_ref[pl.ds(j, size, stride=spots), :] = value


def update(flat, received, rows, cols, low, inverse, row_pos, col_pos, where):
    grid, _, blocks, _, size, _ = received.shape
    spots = rows.shape[1]

    def by_row(k):
        return pl.BlockSpec(
            (grid, 1, 1, 2, size, size),
            lambda l, row, *_: (0, k, jnp.maximum(row[k * spots + l], 0), 0, 0, 0),
        )

    def whole(value):
        zeros = (0,) * value.ndim
        return pl.BlockSpec(value.shape, lambda *_: zeros, pipeline_mode=pl.Buffered(1))

    line = pl.BlockSpec((size * spots, size), lambda l, *_: (l, 0))
    order = spots * size
    return pl.pallas_call(
        functools.partial(update_kernel, spots),
        grid_spec=pltpu.PrefetchScalarGridSpec(
            num_scalar_prefetch=3,
            grid=(spots,),
            in_specs=[line, by_row(0), by_row(1), whole(rows), whole(cols), whole(low), whole(inverse)],
            out_specs=line,
            scratch_shapes=[pltpu.VMEM((order, 2 * size), F32)] + [pltpu.VMEM((order, 2 * size), BF16)] * 4,
        ),
        out_shape=jax.ShapeDtypeStruct(flat.shape, F32),
        compiler_params=pltpu.CompilerParams(dimension_semantics=("arbitrary",)),
        cost_estimate=pl.CostEstimate(flops=4_000_000_000, bytes_accessed=12 * flat.size, transcendentals=0),
        name="update",
    )(row_pos.reshape(-1), col_pos.reshape(-1), where, flat, received, received, rows, cols, low, inverse)


def per_device(grid, orig_front, child_updates, index_maps):
    front, row, col = (lax.axis_index(name) for name in ("front", "row", "col"))
    local = orig_front[0, :, 0, :, :, 0, :]
    spots, size, _, _ = local.shape
    flat = local.reshape(spots * size * spots, size)
    child = child_updates[0, :, :, 0, :, :, 0, :]
    rows_inv, lead_row, lead_col, row_slot, cols_inv, row_pos, col_pos = tables(
        index_maps, front, row, col, grid, spots
    )
    where = jnp.stack([front, row, col]).astype(I32)
    received, low, inverse, fcol = exchange(
        child, flat, rows_inv, row_slot, cols_inv, lead_row, lead_col, grid, spots
    )
    rows, cols = panels(received, fcol, flat, row_pos, col_pos)
    rows, cols = spread(rows, cols, grid)
    out = update(flat, received, rows, cols, low, inverse, row_pos, col_pos, where)
    return out.reshape(1, spots, 1, size, spots, 1, size)


def solution(mesh):
    placed = (
        P("front", None, "row", None, None, "col", None),
        P("front", None, None, "row", None, None, "col", None),
        P(),
    )
    return jax.shard_map(
        functools.partial(per_device, mesh.shape["row"]),
        mesh=mesh,
        in_specs=placed,
        out_specs=P("front", None, "row", None, None, "col", None),
        check_vma=False,
    )
```

```python
import functools

import jax
import jax.numpy as jnp
from jax import lax
from jax.experimental import pallas as pl
from jax.experimental.pallas import tpu as pltpu
from jax.sharding import PartitionSpec as P

F32 = jnp.float32
BF16 = jnp.bfloat16
I32 = jnp.int32
MESH = pl.DeviceIdType.MESH
HIGHEST = lax.Precision.HIGHEST
HBM = pltpu.MemorySpace.HBM
VMEM = pltpu.MemorySpace.VMEM
SMEM = pltpu.MemorySpace.SMEM


def tables(maps, front, row, col, grid, parent_blocks):
    blocks = maps.shape[-1] // grid
    by_source = maps.reshape(2, 2, blocks, grid)
    target = by_source % grid
    place = by_source // grid
    ids = jnp.arange(blocks, dtype=I32)
    before = ids[None, :] < ids[:, None]
    same = target[:, :, :, None, :] == target[:, :, None, :, :]
    order = jnp.sum((same & before[None, None, :, :, None]).astype(I32), axis=3)
    send_slot = target * 2 + order
    recv_slot = jnp.arange(grid, dtype=I32) * 2 + order
    mine = lax.dynamic_index_in_dim(by_source, front, 1, keepdims=False)
    row_send = lax.dynamic_index_in_dim(
        lax.dynamic_index_in_dim(send_slot, front, 1, keepdims=False), row, 2, keepdims=False
    )
    held_rows = lax.dynamic_index_in_dim(mine, row, 2, keepdims=False)
    held_cols = lax.dynamic_index_in_dim(mine, col, 2, keepdims=False)
    lead = jnp.arange(2, dtype=I32)
    lead_row = jnp.sum(
        (held_rows[:, None, :] == lead[None, :, None]).astype(I32) * (ids + 1), axis=-1
    ) - 1
    lead_col = jnp.sum(
        (held_cols[:, None, :] == lead[None, :, None]).astype(I32) * (ids + 1), axis=-1
    ) - 1
    own = lambda value: lax.dynamic_index_in_dim(value, front, 0, keepdims=False)
    own_target, own_place, own_recv = own(target), own(place), own(recv_slot)
    col_send = lax.dynamic_index_in_dim(own(send_slot), col, 2, keepdims=False)
    flat = lambda value: value.reshape(2, blocks * grid)
    row_hit = flat(own_target == row).astype(I32)
    col_hit = flat(own_target == col).astype(I32)
    count = jnp.arange(blocks * grid, dtype=I32)
    rank = jnp.sum(row_hit[:, None, :] * (count[None, :] < count[:, None]).astype(I32), axis=-1)
    row_slot = jnp.sum(
        row_hit[:, None, :] * (rank[:, None, :] == ids[None, :, None]).astype(I32) * flat(own_recv)[:, None, :],
        axis=-1,
    )
    spots = jnp.arange(parent_blocks, dtype=I32)
    at = (flat(own_place)[:, None, :] == spots[None, :, None]).astype(I32)
    row_pos = jnp.sum(row_hit[:, None, :] * at * (rank + 1)[:, None, :], axis=-1) - 1
    col_pos = jnp.sum(col_hit[:, None, :] * at * (flat(own_recv) + 1)[:, None, :], axis=-1) - 1
    slots = jnp.arange(2 * grid, dtype=I32)
    inverse = lambda sent: jnp.sum((sent[:, None, :] == slots[None, :, None]).astype(I32) * ids, axis=-1)
    return inverse(row_send), lead_row, lead_col, row_slot, inverse(col_send), row_pos, col_pos


def meet(peers):
    barrier = pltpu.get_barrier_semaphore()
    for peer in peers:
        pl.semaphore_signal(barrier, inc=1, device_id=peer, device_id_type=MESH)
    pl.semaphore_wait(barrier, len(peers))


def hop_order(grid):
    return [d for pair in zip(range(1, grid), range(grid - 1, 0, -1)) for d in pair][: grid - 1]


def codes(half, flip_cost):
    pairs = [(n, flip) for n in range(half) for flip in range(2) if n + flip > 0]
    return sorted(pairs, key=lambda pair: -(min(pair[0], half - pair[0]) + flip_cost * pair[1]))


def member(me, code, half, sign=1):
    ring = lax.rem(me // 2 + (half + sign * code[0]), half)
    return 2 * ring + lax.rem(me + code[1], 2)


def factor_block(work, size):
    lanes = lax.broadcasted_iota(I32, (size, size), 1)
    rows = lax.broadcasted_iota(I32, (size, 1), 0)

    def step(j, carry):
        pivot_row = work[pl.ds(j, 1), :]
        left = work[:, :size]
        column = jnp.sum(jnp.where(lanes == j, left, 0.0), axis=1, keepdims=True)
        pivot = jnp.sum(jnp.where(lanes[:1] == j, pivot_row[:, :size], 0.0), axis=1, keepdims=True)
        scale = jnp.where(rows > j, column / pivot, 0.0)
        work[...] = work[...] - scale * pivot_row
        return carry

    lax.fori_loop(0, size, step, 0)


def triangular(work, size):
    eye = lax.broadcasted_iota(I32, (size, size), 0) == lax.broadcasted_iota(I32, (size, size), 1)
    upper = lax.broadcasted_iota(I32, (size, size), 0) <= lax.broadcasted_iota(I32, (size, size), 1)
    u = work[:, :size]
    root = lax.rsqrt(jnp.sum(jnp.where(eye, u, 0.0), axis=1, keepdims=True))
    lower = jnp.where(upper, u * root, 0.0).T
    inverse = work[:, size:] * root
    return lower, inverse


def mm(a, b):
    return jnp.dot(a, b, precision=HIGHEST, preferred_element_type=F32)


def mm_t(a, b):
    return lax.dot_general(a, b, (((1,), (1,)), ((), ())), precision=HIGHEST, preferred_element_type=F32)


def factor_lead(lead_ref, low_ref, inv_ref, work, size):
    eye = (
        lax.broadcasted_iota(I32, (size, size), 0) == lax.broadcasted_iota(I32, (size, size), 1)
    ).astype(F32)
    work[:, :size] = lead_ref[:size]
    work[:, size:] = eye
    factor_block(work, size)
    l0, i0 = triangular(work, size)
    l10 = mm_t(lead_ref[size : 2 * size], i0)
    work[:, :size] = lead_ref[2 * size :] - mm_t(l10, l10)
    work[:, size:] = eye
    factor_block(work, size)
    l1, i1 = triangular(work, size)
    low_ref[0] = jnp.concatenate([l0, jnp.zeros_like(l0)], axis=1)
    low_ref[1] = jnp.concatenate([l10, l1], axis=1)
    inv_ref[:size, :size] = i0
    inv_ref[:size, size:] = jnp.zeros_like(i0)
    inv_ref[size:, :size] = -mm(i1, mm(l10, i0))
    inv_ref[size:, size:] = i1


LEAD = ((0, 0), (1, 0), (1, 1))


def exchange_kernel(
    grid, size, blocks, spots,
    rows_inv, row_slot, cols_inv, lead_row, lead_col, child_hbm, flat_hbm,
    recv_two, low_ref, inv_ref, fcol_ref,
    child, send_one, recv_one, turned, send_two, wide, chunk, part, sum_one, sum_two, got_one, got_two, lead, work,
    child_sem, chunk_sem, local_sem, one_send, one_recv, two_send, two_recv,
    la_send, la_recv, lb_send, lb_recv, lc_send, lc_recv,
):
    f, r, c = lax.axis_index("front"), lax.axis_index("row"), lax.axis_index("col")
    other = 1 - f
    piece = len(LEAD) * size // grid
    half = grid // 2
    row_steps, col_steps = codes(half, 1), codes(half, 2)
    row_peers = [(0, d) for d in row_steps] + [(1, d) for d in row_steps] + [(1, (0, 0))]
    row_at = lambda p, d: (lax.rem(f + p, 2), member(r, d, half), c)
    col_at = lambda d: (f, r, member(c, d, half))
    code_of = lambda d: 2 * d[0] + d[1]

    def remote(src, dst, send_sem, recv_sem, peer):
        return pltpu.make_async_remote_copy(
            src_ref=src, dst_ref=dst, send_sem=send_sem, recv_sem=recv_sem, device_id=peer, device_id_type=MESH
        )

    def line(n, slot):
        rows = pl.ds(n * size * spots, size * spots)
        return pltpu.make_async_copy(flat_hbm.at[rows], chunk.at[slot], chunk_sem.at[slot])

    loads = [pltpu.make_async_copy(child_hbm.at[p], child.at[p], child_sem.at[p]) for p in range(2)]
    for load in loads:
        load.start()
    line(0, 0).start()
    meet([row_at(p, d) for p, d in row_peers] + [col_at(d) for d in col_steps])
    for load in loads:
        load.wait()
    line(0, 0).wait()

    corner = chunk[0, pl.ds(0, size, stride=spots), :]
    lane = lax.broadcasted_iota(I32, (size, blocks, size), 1)
    for p in range(2):
        for n, (a, b) in enumerate(LEAD):
            qa, qb = lead_row[2 * p + a], lead_col[2 * p + b]
            block = child[p, jnp.maximum(qa, 0)].astype(F32)
            block = jnp.sum(jnp.where(lane == qb, block, 0.0), axis=1)
            block = jnp.where((qa >= 0) & (qb >= 0), block, 0.0)
            mine = (f == p) & (r == a) & (c == b)
            part[p, pl.ds(n * size, size)] = block + jnp.where(mine, corner, 0.0)
    round_a = []
    for n, (p, d) in enumerate(row_peers):
        peer = row_at(p, d)
        copy = remote(
            part.at[peer[0], pl.ds(peer[1] * piece, piece)],
            got_one.at[f, r], la_send.at[n], la_recv.at[p, code_of(d)], peer,
        )
        copy.start()
        round_a.append(copy)

    round_one = []
    for p in range(2):
        for n, (q, d) in enumerate(row_peers):
            if q != p:
                continue
            peer = row_at(p, d)
            for s in range(2):
                slot = 2 * peer[1] + s
                send_one[peer[0], slot] = child[peer[0], rows_inv[peer[0] * 2 * grid + slot]]
            copy = remote(
                send_one.at[peer[0], pl.ds(2 * peer[1], 2)],
                recv_one.at[f, pl.ds(2 * r, 2)], one_send.at[n], one_recv.at[p, code_of(d)], peer,
            )
            copy.start()
            round_one.append(copy)

    def turn(source, k, slot):
        wide[...] = source.astype(F32).reshape(size * blocks, size)
        for j in range(blocks):
            turned[k, slot, j] = wide[pl.ds(j, size, stride=blocks), :].astype(BF16)

    def turn_own(s, carry):
        slot = 2 * r + s
        turn(child[f, rows_inv[f * 2 * grid + slot]], f, slot)
        return carry

    lax.fori_loop(0, 2, turn_own, 0)

    for copy in round_a:
        copy.wait_recv()
    got_one[f, r] = part[f, pl.ds(pl.multiple_of(r * piece, 8), piece)]
    total = got_one[0, 0]
    for k in range(2):
        for n in range(grid):
            if k + n > 0:
                total = total + got_one[k, n]
    sum_one[...] = total
    got_two[c] = total
    round_b = []
    for n, d in enumerate(col_steps):
        copy = remote(sum_one, got_two.at[c], lb_send.at[n], lb_recv.at[code_of(d)], col_at(d))
        copy.start()
        round_b.append(copy)

    def finish_child(p):
        k = f if p == 0 else other
        for n, (q, d) in enumerate(row_peers):
            if q != p:
                continue
            round_one[n].wait_recv()
            source = member(r, d, half, -1)

            def turn_one(s, carry):
                turn(recv_one[k, 2 * source + s], k, 2 * source + s)
                return carry

            lax.fori_loop(0, 2, turn_one, 0)

        def gather(j, carry):
            row = row_slot[k * blocks + j]
            for slot in range(2 * grid):
                send_two[k, slot // 2, j, slot % 2] = turned[k, row, cols_inv[k * 2 * grid + slot]]
            return carry

        lax.fori_loop(0, blocks, gather, 0)
        sent = []
        for n, d in enumerate(col_steps):
            peer = col_at(d)
            copy = remote(
                send_two.at[k, peer[2]], recv_two.at[c, k], two_send.at[p, n], two_recv.at[k, code_of(d)], peer
            )
            copy.start()
            sent.append(copy)
        local = pltpu.make_async_copy(send_two.at[k, c], recv_two.at[c, k], local_sem.at[p])
        local.start()
        return sent, local

    sent_a, local_a = finish_child(0)

    for copy in round_b:
        copy.wait_recv()
    total = got_two[0]
    for n in range(1, grid):
        total = total + got_two[n]
    sum_two[...] = total
    lead[pl.ds(pl.multiple_of(r * piece, 8), piece)] = total
    round_c = []
    for n, d in enumerate(row_steps):
        copy = remote(
            sum_two, lead.at[pl.ds(pl.multiple_of(r * piece, 8), piece)], lc_send.at[n], lc_recv.at[code_of(d)], row_at(0, d)
        )
        copy.start()
        round_c.append(copy)

    sent_b, local_b = finish_child(1)

    for n in range(spots):
        line(n, n % 2).start()
        if n > 0:
            line(n - 1, (n - 1) % 2).wait()
            fcol_ref[n - 1] = chunk[(n - 1) % 2, pl.ds(0, size, stride=spots), :]
    line(spots - 1, (spots - 1) % 2).wait()
    fcol_ref[spots - 1] = chunk[(spots - 1) % 2, pl.ds(0, size, stride=spots), :]

    for n, d in enumerate(row_steps):
        source = pl.ds(pl.multiple_of(member(r, d, half, -1) * piece, 8), piece)
        remote(sum_two, lead.at[source], lc_send.at[n], lc_recv.at[code_of(d)], row_at(0, d)).wait_recv()
    factor_lead(lead, low_ref, inv_ref, work, size)

    for copy in round_a + round_b + round_c + round_one:
        copy.wait_send()
    for sent, local, k in ((sent_a, local_a, f), (sent_b, local_b, other)):
        local.wait()
        for n in range(len(sent)):
            sent[n].wait_send()
            sent[n].wait_recv()


def exchange(child, flat, rows_inv, row_slot, cols_inv, lead_row, lead_col, grid, spots):
    _, blocks, size, _, _ = child.shape
    piece = len(LEAD) * size // grid
    dma = pltpu.SemaphoreType.DMA
    smem = pl.BlockSpec(memory_space=SMEM)
    hbm = pl.BlockSpec(memory_space=HBM)
    vmem = pl.BlockSpec(memory_space=VMEM)
    return pl.pallas_call(
        functools.partial(exchange_kernel, grid, size, blocks, spots),
        out_shape=[
            jax.ShapeDtypeStruct((grid, 2, blocks, 2, size, size), BF16),
            jax.ShapeDtypeStruct((2, size, 2 * size), F32),
            jax.ShapeDtypeStruct((2 * size, 2 * size), F32),
            jax.ShapeDtypeStruct((spots, size, size), F32),
        ],
        in_specs=[smem] * 5 + [hbm] * 2,
        out_specs=[hbm, vmem, vmem, vmem],
        scratch_shapes=[
            pltpu.VMEM(child.shape, BF16),
            pltpu.VMEM((2, 2 * grid, size, blocks, size), BF16),
            pltpu.VMEM((2, 2 * grid, size, blocks, size), BF16),
            pltpu.VMEM((2, 2 * grid, blocks, size, size), BF16),
            pltpu.VMEM((2, grid, blocks, 2, size, size), BF16),
            pltpu.VMEM((size * blocks, size), F32),
            pltpu.VMEM((2, size * spots, size), F32),
            pltpu.VMEM((2, len(LEAD) * size, size), F32),
            pltpu.VMEM((piece, size), F32),
            pltpu.VMEM((piece, size), F32),
            pltpu.VMEM((2, grid, piece, size), F32),
            pltpu.VMEM((grid, piece, size), F32),
            pltpu.VMEM((len(LEAD) * size, size), F32),
            pltpu.VMEM((size, 2 * size), F32),
            dma((2,)),
            dma((2,)),
            dma((2,)),
            dma((2 * grid,)),
            dma((2, grid)),
            dma((2, grid)),
            dma((2, grid)),
            dma((2 * grid,)),
            dma((2, grid)),
            dma((grid,)),
            dma((grid,)),
            dma((grid,)),
            dma((grid,)),
        ],
        compiler_params=pltpu.CompilerParams(
            collective_id=1, has_side_effects=True, vmem_limit_bytes=60 * 2**20
        ),
        cost_estimate=pl.CostEstimate(flops=400_000_000, bytes_accessed=8 * child.size, transcendentals=0),
        name="exchange",
    )(rows_inv.reshape(-1), row_slot.reshape(-1), cols_inv.reshape(-1), lead_row.reshape(-1), lead_col.reshape(-1), child, flat)


def added(base, parts):
    for block, valid in parts:
        base = base + jnp.where(valid, block.astype(F32), 0.0)
    return base


def split(value):
    high = value.astype(BF16)
    return high, (value - high.astype(F32)).astype(BF16)


def spread_kernel(
    grid, spots, size, row_ref, col_ref, child_hbm, flat_hbm, fcol_ref, low_ref, inv_ref,
    whole_hbm, v_rows, rows_high, rows_low, cols_high, cols_low,
    child, whole, rows_own, cols_own, rows_all, cols_all,
    child_sem, in_sem, out_sem, one_send, one_recv, two_send, two_recv,
):
    f, r, c = lax.axis_index("front"), lax.axis_index("row"), lax.axis_index("col")
    half = grid // 2
    part = spots // half
    row_peer = lambda i: (f, r, i)
    col_peer = lambda i: (f, i, c)
    groups = ((rows_own, rows_all, c, row_peer), (cols_own, cols_all, r, col_peer))
    order = hop_order(grid)

    def line(l):
        return pl.ds(pl.multiple_of(l * size * spots, size * spots), size * spots)

    def line_in(l):
        return pltpu.make_async_copy(flat_hbm.at[line(l)], whole.at[line(l)], in_sem.at[l])

    def line_out(l):
        return pltpu.make_async_copy(whole.at[line(l)], whole_hbm.at[line(l)], out_sem.at[l])

    line_in(0).start()
    for n in range(grid):
        pltpu.make_async_copy(child_hbm.at[n], child.at[n], child_sem.at[n]).start()
    for l in range(1, spots):
        line_in(l).start()
    meet([peer(lax.rem(me + d, grid)) for _, _, me, peer in groups for d in range(1, grid)])

    def from_child(l, j):
        parts = []
        for k in range(2):
            row, col = row_ref[k * spots + l], col_ref[k * spots + j]
            valid = (row >= 0) & (col >= 0)
            row, col = jnp.maximum(row, 0), jnp.maximum(col, 0)
            parts.append((child[col // 2, k, row, col % 2], valid))
        return parts

    line_in(0).wait()
    for n in range(grid):
        pltpu.make_async_copy(child_hbm.at[n], child.at[n], child_sem.at[n]).wait()

    @pl.when(c < 2)
    def _():
        def one(l, carry):
            rows_own[l] = added(fcol_ref[l], from_child(l, 0))
            return carry

        lax.fori_loop(0, spots, one, 0)

    @pl.when(r < 2)
    def _():
        for j in range(spots):
            cols_own[j] = added(whole[pl.ds(j, size, stride=spots), :], from_child(0, j)).T

    def first(g, s, n):
        source, out, me, peer = groups[g]
        to = lax.rem(s + n, grid)
        piece = pl.ds((to // 2) * part, part)
        return pltpu.make_async_remote_copy(
            src_ref=source.at[piece],
            dst_ref=out.at[s, piece],
            send_sem=one_send.at[g, n],
            recv_sem=one_recv.at[g, s],
            device_id=peer(to),
            device_id_type=MESH,
        )

    def second(g, s, n, source):
        _, out, me, peer = groups[g]
        piece = pl.ds((me // 2) * part, part)
        return pltpu.make_async_remote_copy(
            src_ref=source.at[piece],
            dst_ref=out.at[s, piece],
            send_sem=two_send.at[g, s, n],
            recv_sem=two_recv.at[g, s, n],
            device_id=peer(lax.rem(me + 2 * n, grid)),
            device_id_type=MESH,
        )

    for g in range(2):
        for s in range(2):

            @pl.when(groups[g][2] == s)
            def _():
                for n in order:
                    first(g, s, n).start()

    for g in range(2):
        source, out, me, _ = groups[g]
        for s in range(2):

            @pl.when(me == s)
            def _():
                out[s, pl.ds(0, part)] = source[pl.ds(0, part)]
                for n in range(1, half):
                    second(g, s, n, source).start()

    def assemble(l, carry):
        @pl.when(l > 0)
        def _():
            line_in(l).wait()

        for j in range(spots):
            here = pl.ds(l * size * spots + j, size, stride=spots)
            whole[here, :] = added(whole[here, :], from_child(l, j))
        line_out(l).start()
        return carry

    lax.fori_loop(0, spots, assemble, 0)

    for g in range(2):
        _, out, me, _ = groups[g]
        for s in range(2):

            @pl.when(me != s)
            def _():
                piece = pl.ds((me // 2) * part, part)
                pltpu.make_async_remote_copy(
                    src_ref=out.at[s, piece],
                    dst_ref=out.at[s, piece],
                    send_sem=one_send.at[g, 0],
                    recv_sem=one_recv.at[g, s],
                    device_id=groups[g][3](s),
                    device_id_type=MESH,
                ).wait_recv()
                for n in range(1, half):
                    second(g, s, n, out.at[s]).start()

    def solve(g, quarter):
        out = groups[g][1]

        def one(i, carry):
            l = quarter * part + i
            here = pl.ds(pl.multiple_of(l * size, size), size)
            v = mm_t(jnp.concatenate([out[0, l], out[1, l]], axis=1), inv_ref[...])
            if g == 0:
                low = jnp.where(r == 0, low_ref[0], low_ref[1])
                v = jnp.where((r < 2) & (l == 0), low, v)
                v_rows[here, :] = v
                rows_high[here, :], rows_low[here, :] = split(v)
            else:
                cols_high[here, :], cols_low[here, :] = split(v)
            return carry

        lax.fori_loop(0, part, one, 0)

    for g in range(2):
        solve(g, groups[g][2] // 2)

    for n in range(1, half):
        for g in range(2):
            source, out, me, _ = groups[g]
            quarter = lax.rem(me // 2 + half - n, half)
            piece = pl.ds(quarter * part, part)
            for s in range(2):
                pltpu.make_async_remote_copy(
                    src_ref=out.at[s, piece],
                    dst_ref=out.at[s, piece],
                    send_sem=two_send.at[g, s, n],
                    recv_sem=two_recv.at[g, s, n],
                    device_id=groups[g][3](lax.rem(me + 2 * n, grid)),
                    device_id_type=MESH,
                ).wait_recv()
            solve(g, quarter)

    for g in range(2):
        _, out, me, _ = groups[g]
        for s in range(2):

            @pl.when(me == s)
            def _():
                for n in order:
                    first(g, s, n).wait_send()

            for n in range(1, half):
                second(g, s, n, out.at[s]).wait_send()
    for l in range(spots):
        line_out(l).wait()


def spread(received, flat, fcol, low, inverse, row_pos, col_pos, grid):
    spots, size, _ = fcol.shape
    half = grid // 2
    order = spots * size
    dma = pltpu.SemaphoreType.DMA
    smem = pl.BlockSpec(memory_space=SMEM)
    hbm = pl.BlockSpec(memory_space=HBM)
    vmem = pl.BlockSpec(memory_space=VMEM)
    return pl.pallas_call(
        functools.partial(spread_kernel, grid, spots, size),
        out_shape=[jax.ShapeDtypeStruct(flat.shape, F32), jax.ShapeDtypeStruct((order, 2 * size), F32)]
        + [jax.ShapeDtypeStruct((order, 2 * size), BF16)] * 4,
        in_specs=[smem] * 2 + [hbm] * 2 + [vmem] * 3,
        out_specs=[hbm] + [vmem] * 5,
        scratch_shapes=[
            pltpu.VMEM(received.shape, BF16),
            pltpu.VMEM(flat.shape, F32),
            pltpu.VMEM((spots, size, size), F32),
            pltpu.VMEM((spots, size, size), F32),
            pltpu.VMEM((2, spots, size, size), F32),
            pltpu.VMEM((2, spots, size, size), F32),
            dma((grid,)),
            dma((spots,)),
            dma((spots,)),
            dma((2, grid)),
            dma((2, 2)),
            dma((2, 2, half)),
            dma((2, 2, half)),
        ],
        compiler_params=pltpu.CompilerParams(
            collective_id=3, has_side_effects=True, vmem_limit_bytes=48 * 2**20
        ),
        cost_estimate=pl.CostEstimate(flops=40_000_000, bytes_accessed=8 * flat.size, transcendentals=0),
        name="spread",
    )(row_pos.reshape(-1), col_pos.reshape(-1), received, flat, fcol, low, inverse)


def update_kernel(spots, size, where_ref, whole_ref, v_rows, rows_high, rows_low, cols_high, cols_low, out_ref):
    step = pl.program_id(0)
    my_row, my_col = where_ref[1], where_ref[2]
    count = whole_ref.shape[0] // (size * spots)
    wide = 2 if spots % 2 == 0 else 1

    def dot(a, b):
        return lax.dot_general(a, b, (((1,), (1,)), ((), ())), preferred_element_type=F32)

    high, low = rows_high[...], rows_low[...]
    for j in range(0, spots, wide):
        there = pl.ds(j * size, wide * size)
        ch, cl = cols_high[there, :], cols_low[there, :]
        product = dot(high, ch) + (dot(high, cl) + dot(low, ch))
        for i in range(count):
            top = (step == 0) & (my_row < 2) & (i == 0)
            for w in range(wide):
                here = pl.ds(i * size * spots + j + w, size, stride=spots)
                value = whole_ref[here, :] - product[i * size : (i + 1) * size, w * size : (w + 1) * size]
                value = jnp.where(top, 0.0, value)
                if j + w == 0:
                    v = v_rows[pl.ds(i * size, size), :]
                    value = jnp.where(my_col == 0, v[:, :size], jnp.where(my_col == 1, v[:, size:], value))
                out_ref[here, :] = value


def update(whole, v_rows, rows_high, rows_low, cols_high, cols_low, where, spots):
    size = whole.shape[-1]
    count = 2 if spots % 2 == 0 else 1
    line = pl.BlockSpec((count * size * spots, size), lambda l, *_: (l, 0))
    rows = pl.BlockSpec((count * size, 2 * size), lambda l, *_: (l, 0))
    cols = pl.BlockSpec((spots * size, 2 * size), lambda l, *_: (0, 0), pipeline_mode=pl.Buffered(1))
    return pl.pallas_call(
        functools.partial(update_kernel, spots, size),
        grid_spec=pltpu.PrefetchScalarGridSpec(
            num_scalar_prefetch=1,
            grid=(spots // count,),
            in_specs=[line, rows, rows, rows, cols, cols],
            out_specs=line,
        ),
        out_shape=jax.ShapeDtypeStruct(whole.shape, F32),
        compiler_params=pltpu.CompilerParams(dimension_semantics=("arbitrary",)),
        cost_estimate=pl.CostEstimate(flops=4_000_000_000, bytes_accessed=8 * whole.size, transcendentals=0),
        name="update",
    )(where, whole, v_rows, rows_high, rows_low, cols_high, cols_low)


def per_device(grid, orig_front, child_updates, index_maps):
    front, row, col = (lax.axis_index(name) for name in ("front", "row", "col"))
    local = orig_front[0, :, 0, :, :, 0, :]
    spots, size, _, _ = local.shape
    flat = local.reshape(spots * size * spots, size)
    child = child_updates[0, :, :, 0, :, :, 0, :]
    rows_inv, lead_row, lead_col, row_slot, cols_inv, row_pos, col_pos = tables(
        index_maps, front, row, col, grid, spots
    )
    where = jnp.stack([front, row, col]).astype(I32)
    received, low, inverse, fcol = exchange(
        child, flat, rows_inv, row_slot, cols_inv, lead_row, lead_col, grid, spots
    )
    whole, *factors = spread(received, flat, fcol, low, inverse, row_pos, col_pos, grid)
    out = update(whole, *factors, where, spots)
    return out.reshape(1, spots, 1, size, spots, 1, size)


def solution(mesh):
    placed = (
        P("front", None, "row", None, None, "col", None),
        P("front", None, None, "row", None, None, "col", None),
        P(),
    )
    return jax.shard_map(
        functools.partial(per_device, mesh.shape["row"]),
        mesh=mesh,
        in_specs=placed,
        out_specs=P("front", None, "row", None, None, "col", None),
        check_vma=False,
    )
```

```python
import functools

import jax
import jax.numpy as jnp
from jax import lax
from jax.experimental import pallas as pl
from jax.experimental.pallas import tpu as pltpu
from jax.sharding import PartitionSpec as P

F32 = jnp.float32
BF16 = jnp.bfloat16
I32 = jnp.int32
MESH = pl.DeviceIdType.MESH
HIGHEST = lax.Precision.HIGHEST
HBM = pltpu.MemorySpace.HBM
VMEM = pltpu.MemorySpace.VMEM
SMEM = pltpu.MemorySpace.SMEM


def tables(maps, front, row, col, grid, parent_blocks):
    blocks = maps.shape[-1] // grid
    by_source = maps.reshape(2, 2, blocks, grid)
    target = by_source % grid
    place = by_source // grid
    ids = jnp.arange(blocks, dtype=I32)
    before = ids[None, :] < ids[:, None]
    same = target[:, :, :, None, :] == target[:, :, None, :, :]
    order = jnp.sum((same & before[None, None, :, :, None]).astype(I32), axis=3)
    send_slot = target * 2 + order
    recv_slot = jnp.arange(grid, dtype=I32) * 2 + order
    mine = lax.dynamic_index_in_dim(by_source, front, 1, keepdims=False)
    row_send = lax.dynamic_index_in_dim(
        lax.dynamic_index_in_dim(send_slot, front, 1, keepdims=False), row, 2, keepdims=False
    )
    held_rows = lax.dynamic_index_in_dim(mine, row, 2, keepdims=False)
    held_cols = lax.dynamic_index_in_dim(mine, col, 2, keepdims=False)
    lead = jnp.arange(2, dtype=I32)
    lead_row = jnp.sum(
        (held_rows[:, None, :] == lead[None, :, None]).astype(I32) * (ids + 1), axis=-1
    ) - 1
    lead_col = jnp.sum(
        (held_cols[:, None, :] == lead[None, :, None]).astype(I32) * (ids + 1), axis=-1
    ) - 1
    own = lambda value: lax.dynamic_index_in_dim(value, front, 0, keepdims=False)
    own_target, own_place, own_recv = own(target), own(place), own(recv_slot)
    col_send = lax.dynamic_index_in_dim(own(send_slot), col, 2, keepdims=False)
    flat = lambda value: value.reshape(2, blocks * grid)
    row_hit = flat(own_target == row).astype(I32)
    col_hit = flat(own_target == col).astype(I32)
    count = jnp.arange(blocks * grid, dtype=I32)
    rank = jnp.sum(row_hit[:, None, :] * (count[None, :] < count[:, None]).astype(I32), axis=-1)
    row_slot = jnp.sum(
        row_hit[:, None, :] * (rank[:, None, :] == ids[None, :, None]).astype(I32) * flat(own_recv)[:, None, :],
        axis=-1,
    )
    spots = jnp.arange(parent_blocks, dtype=I32)
    at = (flat(own_place)[:, None, :] == spots[None, :, None]).astype(I32)
    row_pos = jnp.sum(row_hit[:, None, :] * at * (rank + 1)[:, None, :], axis=-1) - 1
    col_pos = jnp.sum(col_hit[:, None, :] * at * (flat(own_recv) + 1)[:, None, :], axis=-1) - 1
    slots = jnp.arange(2 * grid, dtype=I32)
    inverse = lambda sent: jnp.sum((sent[:, None, :] == slots[None, :, None]).astype(I32) * ids, axis=-1)
    return inverse(row_send), lead_row, lead_col, row_slot, inverse(col_send), row_pos, col_pos


def meet(peers):
    barrier = pltpu.get_barrier_semaphore()
    for peer in peers:
        pl.semaphore_signal(barrier, inc=1, device_id=peer, device_id_type=MESH)
    pl.semaphore_wait(barrier, len(peers))


def hop_order(grid):
    return [d for pair in zip(range(1, grid), range(grid - 1, 0, -1)) for d in pair][: grid - 1]


def codes(half, flip_cost):
    pairs = [(n, flip) for n in range(half) for flip in range(2) if n + flip > 0]
    return sorted(pairs, key=lambda pair: -(min(pair[0], half - pair[0]) + flip_cost * pair[1]))


def member(me, code, half, sign=1):
    ring = lax.rem(me // 2 + (half + sign * code[0]), half)
    return 2 * ring + lax.rem(me + code[1], 2)


def factor_block(work, size):
    lanes = lax.broadcasted_iota(I32, (size, size), 1)
    rows = lax.broadcasted_iota(I32, (size, 1), 0)

    def step(j, carry):
        pivot_row = work[pl.ds(j, 1), :]
        left = work[:, :size]
        column = jnp.sum(jnp.where(lanes == j, left, 0.0), axis=1, keepdims=True)
        pivot = jnp.sum(jnp.where(lanes[:1] == j, pivot_row[:, :size], 0.0), axis=1, keepdims=True)
        scale = jnp.where(rows > j, column / pivot, 0.0)
        work[...] = work[...] - scale * pivot_row
        return carry

    lax.fori_loop(0, size, step, 0)


def triangular(work, size):
    eye = lax.broadcasted_iota(I32, (size, size), 0) == lax.broadcasted_iota(I32, (size, size), 1)
    upper = lax.broadcasted_iota(I32, (size, size), 0) <= lax.broadcasted_iota(I32, (size, size), 1)
    u = work[:, :size]
    root = lax.rsqrt(jnp.sum(jnp.where(eye, u, 0.0), axis=1, keepdims=True))
    lower = jnp.where(upper, u * root, 0.0).T
    inverse = work[:, size:] * root
    return lower, inverse


def mm(a, b):
    return jnp.dot(a, b, precision=HIGHEST, preferred_element_type=F32)


def mm_t(a, b):
    return lax.dot_general(a, b, (((1,), (1,)), ((), ())), precision=HIGHEST, preferred_element_type=F32)


def factor_lead(lead_ref, low_ref, inv_ref, work, size):
    eye = (
        lax.broadcasted_iota(I32, (size, size), 0) == lax.broadcasted_iota(I32, (size, size), 1)
    ).astype(F32)
    work[:, :size] = lead_ref[:size]
    work[:, size:] = eye
    factor_block(work, size)
    l0, i0 = triangular(work, size)
    l10 = mm_t(lead_ref[size : 2 * size], i0)
    work[:, :size] = lead_ref[2 * size :] - mm_t(l10, l10)
    work[:, size:] = eye
    factor_block(work, size)
    l1, i1 = triangular(work, size)
    low_ref[0] = jnp.concatenate([l0, jnp.zeros_like(l0)], axis=1)
    low_ref[1] = jnp.concatenate([l10, l1], axis=1)
    inv_ref[:size, :size] = i0
    inv_ref[:size, size:] = jnp.zeros_like(i0)
    inv_ref[size:, :size] = -mm(i1, mm(l10, i0))
    inv_ref[size:, size:] = i1


LEAD = ((0, 0), (1, 0), (1, 1))


def exchange_kernel(
    grid, size, blocks, spots,
    rows_inv, row_slot, cols_inv, lead_row, lead_col, child_hbm, flat_hbm,
    recv_two, low_out, inv_out, fcol_out,
    low_ref, inv_ref, fcol_ref, child, send_one, recv_one, turned, send_two, wide, chunk, part, sum_one, sum_two, got_one, got_two, lead, work,
    child_sem, chunk_sem, local_sem, out_sem, one_send, one_recv, two_send, two_recv,
    la_send, la_recv, lb_send, lb_recv, lc_send, lc_recv,
):
    f, r, c = lax.axis_index("front"), lax.axis_index("row"), lax.axis_index("col")
    other = 1 - f
    piece = len(LEAD) * size // grid
    half = grid // 2
    row_steps, col_steps = codes(half, 1), codes(half, 2)
    row_peers = [(0, d) for d in row_steps] + [(1, d) for d in row_steps] + [(1, (0, 0))]
    row_at = lambda p, d: (lax.rem(f + p, 2), member(r, d, half), c)
    col_at = lambda d: (f, r, member(c, d, half))
    code_of = lambda d: 2 * d[0] + d[1]

    def remote(src, dst, send_sem, recv_sem, peer):
        return pltpu.make_async_remote_copy(
            src_ref=src, dst_ref=dst, send_sem=send_sem, recv_sem=recv_sem, device_id=peer, device_id_type=MESH
        )

    def line(n, slot):
        rows = pl.ds(n * size * spots, size * spots)
        return pltpu.make_async_copy(flat_hbm.at[rows], chunk.at[slot], chunk_sem.at[slot])

    loads = [pltpu.make_async_copy(child_hbm.at[p], child.at[p], child_sem.at[p]) for p in range(2)]
    for load in loads:
        load.start()
    line(0, 0).start()
    meet([row_at(p, d) for p, d in row_peers] + [col_at(d) for d in col_steps])
    for load in loads:
        load.wait()
    line(0, 0).wait()

    corner = chunk[0, pl.ds(0, size, stride=spots), :]
    lane = lax.broadcasted_iota(I32, (size, blocks, size), 1)
    for p in range(2):
        for n, (a, b) in enumerate(LEAD):
            qa, qb = lead_row[2 * p + a], lead_col[2 * p + b]
            block = child[p, jnp.maximum(qa, 0)].astype(F32)
            block = jnp.sum(jnp.where(lane == qb, block, 0.0), axis=1)
            block = jnp.where((qa >= 0) & (qb >= 0), block, 0.0)
            mine = (f == p) & (r == a) & (c == b)
            part[p, pl.ds(n * size, size)] = block + jnp.where(mine, corner, 0.0)
    round_a = []
    for n, (p, d) in enumerate(row_peers):
        peer = row_at(p, d)
        copy = remote(
            part.at[peer[0], pl.ds(peer[1] * piece, piece)],
            got_one.at[f, r], la_send.at[n], la_recv.at[p, code_of(d)], peer,
        )
        copy.start()
        round_a.append(copy)

    for p in range(2):
        for q, d in row_peers:
            if q == p:
                front, row, _ = row_at(p, d)
                for s in range(2):
                    slot = 2 * row + s
                    send_one[front, slot] = child[front, rows_inv[front * 2 * grid + slot]]

    for copy in round_a:
        copy.wait_recv()
    got_one[f, r] = part[f, pl.ds(pl.multiple_of(r * piece, 8), piece)]
    total = got_one[0, 0]
    for k in range(2):
        for n in range(grid):
            if k + n > 0:
                total = total + got_one[k, n]
    sum_one[...] = total
    got_two[c] = total
    round_b = []
    for n, d in enumerate(col_steps):
        copy = remote(sum_one, got_two.at[c], lb_send.at[n], lb_recv.at[code_of(d)], col_at(d))
        copy.start()
        round_b.append(copy)

    def turn(source, k, slot):
        wide[...] = source.astype(F32).reshape(size * blocks, size)
        for j in range(blocks):
            turned[k, slot, j] = wide[pl.ds(j, size, stride=blocks), :].astype(BF16)

    def turn_own(s, carry):
        slot = 2 * r + s
        turn(child[f, rows_inv[f * 2 * grid + slot]], f, slot)
        return carry

    lax.fori_loop(0, 2, turn_own, 0)

    for copy in round_b:
        copy.wait_recv()
    total = got_two[0]
    for n in range(1, grid):
        total = total + got_two[n]
    sum_two[...] = total
    lead[pl.ds(pl.multiple_of(r * piece, 8), piece)] = total
    round_c = []
    for n, d in enumerate(row_steps):
        copy = remote(
            sum_two, lead.at[pl.ds(pl.multiple_of(r * piece, 8), piece)], lc_send.at[n], lc_recv.at[code_of(d)], row_at(0, d)
        )
        copy.start()
        round_c.append(copy)

    round_one = []
    for n, (p, d) in enumerate(row_peers):
        peer = row_at(p, d)
        copy = remote(
            send_one.at[peer[0], pl.ds(2 * peer[1], 2)],
            recv_one.at[f, pl.ds(2 * r, 2)], one_send.at[n], one_recv.at[p, code_of(d)], peer,
        )
        copy.start()
        round_one.append(copy)

    for n, d in enumerate(row_steps):
        source = pl.ds(pl.multiple_of(member(r, d, half, -1) * piece, 8), piece)
        remote(sum_two, lead.at[source], lc_send.at[n], lc_recv.at[code_of(d)], row_at(0, d)).wait_recv()
    factor_lead(lead, low_ref, inv_ref, work, size)
    outs = [
        pltpu.make_async_copy(low_ref, low_out, out_sem.at[0]),
        pltpu.make_async_copy(inv_ref, inv_out, out_sem.at[1]),
    ]

    def finish_child(p):
        k = f if p == 0 else other
        for n, (q, d) in enumerate(row_peers):
            if q != p:
                continue
            round_one[n].wait_recv()
            source = member(r, d, half, -1)

            def turn_one(s, carry):
                turn(recv_one[k, 2 * source + s], k, 2 * source + s)
                return carry

            lax.fori_loop(0, 2, turn_one, 0)

        def gather(j, carry):
            row = row_slot[k * blocks + j]
            for slot in range(2 * grid):
                send_two[k, slot // 2, j, slot % 2] = turned[k, row, cols_inv[k * 2 * grid + slot]]
            return carry

        lax.fori_loop(0, blocks, gather, 0)
        sent = []
        for n, d in enumerate(col_steps):
            peer = col_at(d)
            copy = remote(
                send_two.at[k, peer[2]], recv_two.at[c, k], two_send.at[p, n], two_recv.at[k, code_of(d)], peer
            )
            copy.start()
            sent.append(copy)
        local = pltpu.make_async_copy(send_two.at[k, c], recv_two.at[c, k], local_sem.at[p])
        local.start()
        return sent, local

    sent_a, local_a = finish_child(0)
    sent_b, local_b = finish_child(1)

    for n in range(spots):
        line(n, n % 2).start()
        if n > 0:
            line(n - 1, (n - 1) % 2).wait()
            fcol_ref[n - 1] = chunk[(n - 1) % 2, pl.ds(0, size, stride=spots), :]
    line(spots - 1, (spots - 1) % 2).wait()
    fcol_ref[spots - 1] = chunk[(spots - 1) % 2, pl.ds(0, size, stride=spots), :]
    outs.append(pltpu.make_async_copy(fcol_ref, fcol_out, out_sem.at[2]))
    for copy in outs:
        copy.start()

    for copy in outs:
        copy.wait()
    for copy in round_a + round_b + round_c + round_one:
        copy.wait_send()
    for sent, local, k in ((sent_a, local_a, f), (sent_b, local_b, other)):
        local.wait()
        for n in range(len(sent)):
            sent[n].wait_send()
            sent[n].wait_recv()


def exchange(child, flat, rows_inv, row_slot, cols_inv, lead_row, lead_col, grid, spots):
    _, blocks, size, _, _ = child.shape
    piece = len(LEAD) * size // grid
    dma = pltpu.SemaphoreType.DMA
    smem = pl.BlockSpec(memory_space=SMEM)
    hbm = pl.BlockSpec(memory_space=HBM)
    return pl.pallas_call(
        functools.partial(exchange_kernel, grid, size, blocks, spots),
        out_shape=[
            jax.ShapeDtypeStruct((grid, 2, blocks, 2, size, size), BF16),
            jax.ShapeDtypeStruct((2, size, 2 * size), F32),
            jax.ShapeDtypeStruct((2 * size, 2 * size), F32),
            jax.ShapeDtypeStruct((spots, size, size), F32),
        ],
        in_specs=[smem] * 5 + [hbm] * 2,
        out_specs=[hbm] * 4,
        scratch_shapes=[
            pltpu.VMEM((2, size, 2 * size), F32),
            pltpu.VMEM((2 * size, 2 * size), F32),
            pltpu.VMEM((spots, size, size), F32),
            pltpu.VMEM(child.shape, BF16),
            pltpu.VMEM((2, 2 * grid, size, blocks, size), BF16),
            pltpu.VMEM((2, 2 * grid, size, blocks, size), BF16),
            pltpu.VMEM((2, 2 * grid, blocks, size, size), BF16),
            pltpu.VMEM((2, grid, blocks, 2, size, size), BF16),
            pltpu.VMEM((size * blocks, size), F32),
            pltpu.VMEM((2, size * spots, size), F32),
            pltpu.VMEM((2, len(LEAD) * size, size), F32),
            pltpu.VMEM((piece, size), F32),
            pltpu.VMEM((piece, size), F32),
            pltpu.VMEM((2, grid, piece, size), F32),
            pltpu.VMEM((grid, piece, size), F32),
            pltpu.VMEM((len(LEAD) * size, size), F32),
            pltpu.VMEM((size, 2 * size), F32),
            dma((2,)),
            dma((2,)),
            dma((2,)),
            dma((3,)),
            dma((2 * grid,)),
            dma((2, grid)),
            dma((2, grid)),
            dma((2, grid)),
            dma((2 * grid,)),
            dma((2, grid)),
            dma((grid,)),
            dma((grid,)),
            dma((grid,)),
            dma((grid,)),
        ],
        compiler_params=pltpu.CompilerParams(
            collective_id=1, has_side_effects=True, vmem_limit_bytes=60 * 2**20
        ),
        cost_estimate=pl.CostEstimate(flops=400_000_000, bytes_accessed=8 * child.size, transcendentals=0),
        name="exchange",
    )(rows_inv.reshape(-1), row_slot.reshape(-1), cols_inv.reshape(-1), lead_row.reshape(-1), lead_col.reshape(-1), child, flat)


def added(base, parts):
    for block, valid in parts:
        base = base + jnp.where(valid, block.astype(F32), 0.0)
    return base


def split(value):
    high = value.astype(BF16)
    return high, (value - high.astype(F32)).astype(BF16)


def spread_kernel(
    grid, spots, size, row_ref, col_ref, child_hbm, flat_hbm, fcol_hbm, low_hbm, inv_hbm,
    whole_hbm, v_rows_out, rows_high_out, rows_low_out, cols_high_out, cols_low_out,
    fcol_ref, low_ref, inv_ref, v_rows, rows_high, rows_low, cols_high, cols_low, child, whole, rows_own, cols_own, rows_all, cols_all,
    child_sem, in_sem, out_sem, small_sem, v_sem, one_send, one_recv, two_send, two_recv,
):
    f, r, c = lax.axis_index("front"), lax.axis_index("row"), lax.axis_index("col")
    half = grid // 2
    part = spots // half
    row_peer = lambda i: (f, r, i)
    col_peer = lambda i: (f, i, c)
    groups = ((rows_own, rows_all, c, row_peer), (cols_own, cols_all, r, col_peer))
    order = hop_order(grid)

    def line(l):
        return pl.ds(pl.multiple_of(l * size * spots, size * spots), size * spots)

    def line_in(l):
        return pltpu.make_async_copy(flat_hbm.at[line(l)], whole.at[line(l)], in_sem.at[l])

    def line_out(l):
        return pltpu.make_async_copy(whole.at[line(l)], whole_hbm.at[line(l)], out_sem.at[l])

    line_in(0).start()
    for n in range(grid):
        pltpu.make_async_copy(child_hbm.at[n], child.at[n], child_sem.at[n]).start()
    small = [
        pltpu.make_async_copy(src, dst, small_sem.at[n])
        for n, (src, dst) in enumerate(((fcol_hbm, fcol_ref), (low_hbm, low_ref), (inv_hbm, inv_ref)))
    ]
    for copy in small:
        copy.start()
    for l in range(1, spots):
        line_in(l).start()
    meet([peer(lax.rem(me + d, grid)) for _, _, me, peer in groups for d in range(1, grid)])

    def from_child(l, j):
        parts = []
        for k in range(2):
            row, col = row_ref[k * spots + l], col_ref[k * spots + j]
            valid = (row >= 0) & (col >= 0)
            row, col = jnp.maximum(row, 0), jnp.maximum(col, 0)
            parts.append((child[col // 2, k, row, col % 2], valid))
        return parts

    line_in(0).wait()
    for copy in small:
        copy.wait()
    for n in range(grid):
        pltpu.make_async_copy(child_hbm.at[n], child.at[n], child_sem.at[n]).wait()

    @pl.when(c < 2)
    def _():
        def one(l, carry):
            rows_own[l] = added(fcol_ref[l], from_child(l, 0))
            return carry

        lax.fori_loop(0, spots, one, 0)

    @pl.when(r < 2)
    def _():
        for j in range(spots):
            cols_own[j] = added(whole[pl.ds(j, size, stride=spots), :], from_child(0, j)).T

    def first(g, s, n):
        source, out, me, peer = groups[g]
        to = lax.rem(s + n, grid)
        piece = pl.ds((to // 2) * part, part)
        return pltpu.make_async_remote_copy(
            src_ref=source.at[piece],
            dst_ref=out.at[s, piece],
            send_sem=one_send.at[g, n],
            recv_sem=one_recv.at[g, s],
            device_id=peer(to),
            device_id_type=MESH,
        )

    def second(g, s, n, source):
        _, out, me, peer = groups[g]
        piece = pl.ds((me // 2) * part, part)
        return pltpu.make_async_remote_copy(
            src_ref=source.at[piece],
            dst_ref=out.at[s, piece],
            send_sem=two_send.at[g, s, n],
            recv_sem=two_recv.at[g, s, n],
            device_id=peer(lax.rem(me + 2 * n, grid)),
            device_id_type=MESH,
        )

    for g in range(2):
        for s in range(2):

            @pl.when(groups[g][2] == s)
            def _():
                for n in order:
                    first(g, s, n).start()

    for g in range(2):
        source, out, me, _ = groups[g]
        for s in range(2):

            @pl.when(me == s)
            def _():
                out[s, pl.ds(0, part)] = source[pl.ds(0, part)]
                for n in range(1, half):
                    second(g, s, n, source).start()

    def assemble(l, carry):
        @pl.when(l > 0)
        def _():
            line_in(l).wait()

        for j in range(spots):
            here = pl.ds(l * size * spots + j, size, stride=spots)
            whole[here, :] = added(whole[here, :], from_child(l, j))
        line_out(l).start()
        return carry

    lax.fori_loop(0, spots, assemble, 0)

    for g in range(2):
        _, out, me, _ = groups[g]
        for s in range(2):

            @pl.when(me != s)
            def _():
                piece = pl.ds((me // 2) * part, part)
                pltpu.make_async_remote_copy(
                    src_ref=out.at[s, piece],
                    dst_ref=out.at[s, piece],
                    send_sem=one_send.at[g, 0],
                    recv_sem=one_recv.at[g, s],
                    device_id=groups[g][3](s),
                    device_id_type=MESH,
                ).wait_recv()
                for n in range(1, half):
                    second(g, s, n, out.at[s]).start()

    def solve(g, quarter, n):
        out = groups[g][1]

        def one(i, carry):
            l = quarter * part + i
            here = pl.ds(pl.multiple_of(l * size, size), size)
            v = mm_t(jnp.concatenate([out[0, l], out[1, l]], axis=1), inv_ref[...])
            if g == 0:
                low = jnp.where(r == 0, low_ref[0], low_ref[1])
                v = jnp.where((r < 2) & (l == 0), low, v)
                v_rows[here, :] = v
                rows_high[here, :], rows_low[here, :] = split(v)
            else:
                cols_high[here, :], cols_low[here, :] = split(v)
            return carry

        lax.fori_loop(0, part, one, 0)
        here = pl.ds(pl.multiple_of(quarter * part * size, size), part * size)
        for i, (src, dst) in enumerate(factors[g]):
            copy = pltpu.make_async_copy(src.at[here], dst.at[here], v_sem.at[g, n, i])
            copy.start()
            leaving.append(copy)

    factors = (
        ((rows_high, rows_high_out), (rows_low, rows_low_out), (v_rows, v_rows_out)),
        ((cols_high, cols_high_out), (cols_low, cols_low_out)),
    )
    leaving = []
    for g in range(2):
        solve(g, groups[g][2] // 2, 0)

    for n in range(1, half):
        for g in range(2):
            source, out, me, _ = groups[g]
            quarter = lax.rem(me // 2 + half - n, half)
            piece = pl.ds(quarter * part, part)
            for s in range(2):
                pltpu.make_async_remote_copy(
                    src_ref=out.at[s, piece],
                    dst_ref=out.at[s, piece],
                    send_sem=two_send.at[g, s, n],
                    recv_sem=two_recv.at[g, s, n],
                    device_id=groups[g][3](lax.rem(me + 2 * n, grid)),
                    device_id_type=MESH,
                ).wait_recv()
            solve(g, quarter, n)

    for g in range(2):
        _, out, me, _ = groups[g]
        for s in range(2):

            @pl.when(me == s)
            def _():
                for n in order:
                    first(g, s, n).wait_send()

            for n in range(1, half):
                second(g, s, n, out.at[s]).wait_send()
    for l in range(spots):
        line_out(l).wait()
    for copy in leaving:
        copy.wait()


def spread(received, flat, fcol, low, inverse, row_pos, col_pos, grid):
    spots, size, _ = fcol.shape
    half = grid // 2
    order = spots * size
    dma = pltpu.SemaphoreType.DMA
    smem = pl.BlockSpec(memory_space=SMEM)
    hbm = pl.BlockSpec(memory_space=HBM)
    return pl.pallas_call(
        functools.partial(spread_kernel, grid, spots, size),
        out_shape=[jax.ShapeDtypeStruct(flat.shape, F32), jax.ShapeDtypeStruct((order, 2 * size), F32)]
        + [jax.ShapeDtypeStruct((order, 2 * size), BF16)] * 4,
        in_specs=[smem] * 2 + [hbm] * 5,
        out_specs=[hbm] * 6,
        scratch_shapes=[
            pltpu.VMEM(fcol.shape, F32),
            pltpu.VMEM(low.shape, F32),
            pltpu.VMEM(inverse.shape, F32),
            pltpu.VMEM((order, 2 * size), F32),
        ]
        + [pltpu.VMEM((order, 2 * size), BF16)] * 4
        + [
            pltpu.VMEM(received.shape, BF16),
            pltpu.VMEM(flat.shape, F32),
            pltpu.VMEM((spots, size, size), F32),
            pltpu.VMEM((spots, size, size), F32),
            pltpu.VMEM((2, spots, size, size), F32),
            pltpu.VMEM((2, spots, size, size), F32),
            dma((grid,)),
            dma((spots,)),
            dma((spots,)),
            dma((3,)),
            dma((2, half, 3)),
            dma((2, grid)),
            dma((2, 2)),
            dma((2, 2, half)),
            dma((2, 2, half)),
        ],
        compiler_params=pltpu.CompilerParams(
            collective_id=3, has_side_effects=True, vmem_limit_bytes=60 * 2**20
        ),
        cost_estimate=pl.CostEstimate(flops=40_000_000, bytes_accessed=8 * flat.size, transcendentals=0),
        name="spread",
    )(row_pos.reshape(-1), col_pos.reshape(-1), received, flat, fcol, low, inverse)


def update_kernel(spots, size, where_ref, whole_ref, v_rows, rows_high, rows_low, cols_high, cols_low, out_ref):
    step = pl.program_id(0)
    my_row, my_col = where_ref[1], where_ref[2]
    count = whole_ref.shape[0] // (size * spots)
    wide = 2 if spots % 2 == 0 else 1

    def dot(a, b):
        return lax.dot_general(a, b, (((1,), (1,)), ((), ())), preferred_element_type=F32)

    high, low = rows_high[...], rows_low[...]
    for j in range(0, spots, wide):
        there = pl.ds(j * size, wide * size)
        ch, cl = cols_high[there, :], cols_low[there, :]
        product = dot(high, ch) + (dot(high, cl) + dot(low, ch))
        for i in range(count):
            top = (step == 0) & (my_row < 2) & (i == 0)
            for w in range(wide):
                here = pl.ds(i * size * spots + j + w, size, stride=spots)
                value = whole_ref[here, :] - product[i * size : (i + 1) * size, w * size : (w + 1) * size]
                value = jnp.where(top, 0.0, value)
                if j + w == 0:
                    v = v_rows[pl.ds(i * size, size), :]
                    value = jnp.where(my_col == 0, v[:, :size], jnp.where(my_col == 1, v[:, size:], value))
                out_ref[here, :] = value


def update(whole, v_rows, rows_high, rows_low, cols_high, cols_low, where, spots):
    size = whole.shape[-1]
    count = 2 if spots % 2 == 0 else 1
    line = pl.BlockSpec((count * size * spots, size), lambda l, *_: (l, 0))
    rows = pl.BlockSpec((count * size, 2 * size), lambda l, *_: (l, 0))
    cols = pl.BlockSpec((spots * size, 2 * size), lambda l, *_: (0, 0), pipeline_mode=pl.Buffered(1))
    return pl.pallas_call(
        functools.partial(update_kernel, spots, size),
        grid_spec=pltpu.PrefetchScalarGridSpec(
            num_scalar_prefetch=1,
            grid=(spots // count,),
            in_specs=[line, rows, rows, rows, cols, cols],
            out_specs=line,
        ),
        out_shape=jax.ShapeDtypeStruct(whole.shape, F32),
        compiler_params=pltpu.CompilerParams(dimension_semantics=("arbitrary",), vmem_limit_bytes=60 * 2**20),
        cost_estimate=pl.CostEstimate(flops=4_000_000_000, bytes_accessed=8 * whole.size, transcendentals=0),
        name="update",
    )(where, whole, v_rows, rows_high, rows_low, cols_high, cols_low)


def per_device(grid, orig_front, child_updates, index_maps):
    front, row, col = (lax.axis_index(name) for name in ("front", "row", "col"))
    local = orig_front[0, :, 0, :, :, 0, :]
    spots, size, _, _ = local.shape
    flat = local.reshape(spots * size * spots, size)
    child = child_updates[0, :, :, 0, :, :, 0, :]
    rows_inv, lead_row, lead_col, row_slot, cols_inv, row_pos, col_pos = tables(
        index_maps, front, row, col, grid, spots
    )
    where = jnp.stack([front, row, col]).astype(I32)
    received, low, inverse, fcol = exchange(
        child, flat, rows_inv, row_slot, cols_inv, lead_row, lead_col, grid, spots
    )
    whole, *factors = spread(received, flat, fcol, low, inverse, row_pos, col_pos, grid)
    out = update(whole, *factors, where, spots)
    return out.reshape(1, spots, 1, size, spots, 1, size)


def solution(mesh):
    placed = (
        P("front", None, "row", None, None, "col", None),
        P("front", None, None, "row", None, None, "col", None),
        P(),
    )
    return jax.shard_map(
        functools.partial(per_device, mesh.shape["row"]),
        mesh=mesh,
        in_specs=placed,
        out_specs=P("front", None, "row", None, None, "col", None),
        check_vma=False,
    )
```

```python
import functools

import jax
import jax.numpy as jnp
from jax import lax
from jax.experimental import pallas as pl
from jax.experimental.pallas import tpu as pltpu
from jax.sharding import PartitionSpec as P

F32 = jnp.float32
BF16 = jnp.bfloat16
I32 = jnp.int32
MESH = pl.DeviceIdType.MESH
HIGHEST = lax.Precision.HIGHEST
HBM = pltpu.MemorySpace.HBM
VMEM = pltpu.MemorySpace.VMEM
SMEM = pltpu.MemorySpace.SMEM


def table_kernel(grid, blocks, spots, maps, rows_inv, lead_row, lead_col, row_slot, cols_inv, row_pos, col_pos):
    front, row, col = lax.axis_index("front"), lax.axis_index("row"), lax.axis_index("col")
    total = blocks * grid
    fills = ((rows_inv, 0), (row_slot, 0), (cols_inv, 0), (lead_row, -1), (lead_col, -1), (row_pos, -1), (col_pos, -1))
    for ref, fill in fills:

        def clear(i, carry, ref=ref, fill=fill):
            ref[i] = fill
            return carry

        lax.fori_loop(0, ref.shape[0], clear, 0)

    def order_of(values, q):
        order = jnp.int32(0)
        for before in range(q):
            order = order + jnp.where(values[before] == values[q], 1, 0)
        return order

    def held(p, base, place, spare, inverse, lead):
        blocks_at = [maps[base + q * grid + place] for q in range(blocks)]
        target = [lax.rem(value, grid) for value in blocks_at]
        for q in range(blocks):
            if inverse is not None:
                inverse[p * 2 * grid + 2 * target[q] + order_of(target, q)] = q
            if lead is not None:
                lead[jnp.where(blocks_at[q] < 2, 2 * p + blocks_at[q], spare)] = q

    def one_pair(p, carry):
        mine = (2 * p + front) * total
        own = (2 * front + p) * total
        held(p, mine, row, 4, rows_inv, lead_row)
        held(p, mine, col, 4, None, lead_col)
        held(p, own, col, 4, cols_inv, None)

        def one_source(r, rank):
            row_order, col_order = jnp.int32(0), jnp.int32(0)
            for q in range(blocks):
                value = maps[own + q * grid + r]
                target, place = lax.rem(value, grid), lax.div(value, grid)
                hit = target == row
                row_slot[jnp.where(hit, p * blocks + rank, 2 * blocks)] = 2 * r + row_order
                row_pos[jnp.where(hit, p * spots + place, 2 * spots)] = rank
                row_order = row_order + jnp.where(hit, 1, 0)
                rank = rank + jnp.where(hit, 1, 0)
                hit = target == col
                col_pos[jnp.where(hit, p * spots + place, 2 * spots)] = 2 * r + col_order
                col_order = col_order + jnp.where(hit, 1, 0)
            return rank

        lax.fori_loop(0, grid, one_source, jnp.int32(0))
        return carry

    lax.fori_loop(0, 2, one_pair, 0)


def tables(maps, grid, spots):
    blocks = maps.shape[-1] // grid
    sizes = (4 * grid, 5, 5, 2 * blocks + 1, 4 * grid, 2 * spots + 1, 2 * spots + 1)
    smem = pl.BlockSpec(memory_space=SMEM)
    return pl.pallas_call(
        functools.partial(table_kernel, grid, blocks, spots),
        out_shape=[jax.ShapeDtypeStruct((size,), I32) for size in sizes],
        in_specs=[smem],
        out_specs=[smem] * len(sizes),
        cost_estimate=pl.CostEstimate(flops=10_000, bytes_accessed=4096, transcendentals=0),
        name="tables",
    )(maps.reshape(-1))


def meet(peers):
    barrier = pltpu.get_barrier_semaphore()
    for peer in peers:
        pl.semaphore_signal(barrier, inc=1, device_id=peer, device_id_type=MESH)
    pl.semaphore_wait(barrier, len(peers))


def codes(half, flip_cost):
    pairs = [(n, flip) for n in range(half) for flip in range(2) if n + flip > 0]
    return sorted(pairs, key=lambda pair: -(min(pair[0], half - pair[0]) + flip_cost * pair[1]))


def member(me, code, half, sign=1):
    ring = lax.rem(me // 2 + (half + sign * code[0]), half)
    return 2 * ring + lax.rem(me + code[1], 2)


def factor_block(work, size):
    lanes = lax.broadcasted_iota(I32, (size, size), 1)
    rows = lax.broadcasted_iota(I32, (size, 1), 0)

    def step(j, carry):
        pivot_row = work[pl.ds(j, 1), :]
        left = work[:, :size]
        column = jnp.sum(jnp.where(lanes == j, left, 0.0), axis=1, keepdims=True)
        pivot = jnp.sum(jnp.where(lanes[:1] == j, pivot_row[:, :size], 0.0), axis=1, keepdims=True)
        scale = jnp.where(rows > j, column / pivot, 0.0)
        work[...] = work[...] - scale * pivot_row
        return carry

    lax.fori_loop(0, size, step, 0)


def triangular(work, size):
    eye = lax.broadcasted_iota(I32, (size, size), 0) == lax.broadcasted_iota(I32, (size, size), 1)
    upper = lax.broadcasted_iota(I32, (size, size), 0) <= lax.broadcasted_iota(I32, (size, size), 1)
    u = work[:, :size]
    root = lax.rsqrt(jnp.sum(jnp.where(eye, u, 0.0), axis=1, keepdims=True))
    lower = jnp.where(upper, u * root, 0.0).T
    inverse = work[:, size:] * root
    return lower, inverse


def mm(a, b):
    return jnp.dot(a, b, precision=HIGHEST, preferred_element_type=F32)


def mm_t(a, b):
    return lax.dot_general(a, b, (((1,), (1,)), ((), ())), precision=HIGHEST, preferred_element_type=F32)


def factor_lead(lead_ref, low_ref, inv_ref, work, size):
    eye = (
        lax.broadcasted_iota(I32, (size, size), 0) == lax.broadcasted_iota(I32, (size, size), 1)
    ).astype(F32)
    work[:, :size] = lead_ref[:size]
    work[:, size:] = eye
    factor_block(work, size)
    l0, i0 = triangular(work, size)
    l10 = mm_t(lead_ref[size : 2 * size], i0)
    work[:, :size] = lead_ref[2 * size :] - mm_t(l10, l10)
    work[:, size:] = eye
    factor_block(work, size)
    l1, i1 = triangular(work, size)
    low_ref[0] = jnp.concatenate([l0, jnp.zeros_like(l0)], axis=1)
    low_ref[1] = jnp.concatenate([l10, l1], axis=1)
    inv_ref[:size, :size] = i0
    inv_ref[:size, size:] = jnp.zeros_like(i0)
    inv_ref[size:, :size] = -mm(i1, mm(l10, i0))
    inv_ref[size:, size:] = i1


LEAD = ((0, 0), (1, 0), (1, 1))


def exchange_kernel(
    grid, size, blocks, spots,
    rows_inv, row_slot, cols_inv, lead_row, lead_col, child_hbm, flat_hbm,
    recv_two, low_out, inv_out, fcol_out,
    low_ref, inv_ref, fcol_ref, child, send_one, recv_one, turned, send_two, wide, chunk, part, sum_one, sum_two, got_one, got_two, lead, work,
    child_sem, chunk_sem, local_sem, out_sem, one_send, one_recv, two_send, two_recv,
    la_send, la_recv, lb_send, lb_recv, lc_send, lc_recv,
):
    f, r, c = lax.axis_index("front"), lax.axis_index("row"), lax.axis_index("col")
    other = 1 - f
    piece = len(LEAD) * size // grid
    half = grid // 2
    row_steps, col_steps = codes(half, 1), codes(half, 2)
    row_peers = [(0, d) for d in row_steps] + [(1, d) for d in row_steps] + [(1, (0, 0))]
    row_at = lambda p, d: (lax.rem(f + p, 2), member(r, d, half), c)
    col_at = lambda d: (f, r, member(c, d, half))
    code_of = lambda d: 2 * d[0] + d[1]

    def remote(src, dst, send_sem, recv_sem, peer):
        return pltpu.make_async_remote_copy(
            src_ref=src, dst_ref=dst, send_sem=send_sem, recv_sem=recv_sem, device_id=peer, device_id_type=MESH
        )

    def line(n, slot):
        rows = pl.ds(n * size * spots, size * spots)
        return pltpu.make_async_copy(flat_hbm.at[rows], chunk.at[slot], chunk_sem.at[slot])

    loads = [pltpu.make_async_copy(child_hbm.at[p], child.at[p], child_sem.at[p]) for p in range(2)]
    for load in loads:
        load.start()
    line(0, 0).start()
    meet([row_at(p, d) for p, d in row_peers] + [col_at(d) for d in col_steps])
    for load in loads:
        load.wait()
    line(0, 0).wait()

    corner = chunk[0, pl.ds(0, size, stride=spots), :]
    lane = lax.broadcasted_iota(I32, (size, blocks, size), 1)
    for p in range(2):
        for n, (a, b) in enumerate(LEAD):
            qa, qb = lead_row[2 * p + a], lead_col[2 * p + b]
            block = child[p, jnp.maximum(qa, 0)].astype(F32)
            block = jnp.sum(jnp.where(lane == qb, block, 0.0), axis=1)
            block = jnp.where((qa >= 0) & (qb >= 0), block, 0.0)
            mine = (f == p) & (r == a) & (c == b)
            part[p, pl.ds(n * size, size)] = block + jnp.where(mine, corner, 0.0)
    round_a = []
    for n, (p, d) in enumerate(row_peers):
        peer = row_at(p, d)
        copy = remote(
            part.at[peer[0], pl.ds(peer[1] * piece, piece)],
            got_one.at[f, r], la_send.at[n], la_recv.at[p, code_of(d)], peer,
        )
        copy.start()
        round_a.append(copy)

    for p in range(2):
        for q, d in row_peers:
            if q == p:
                front, row, _ = row_at(p, d)
                for s in range(2):
                    slot = 2 * row + s
                    send_one[front, slot] = child[front, rows_inv[front * 2 * grid + slot]]

    for copy in round_a:
        copy.wait_recv()
    got_one[f, r] = part[f, pl.ds(pl.multiple_of(r * piece, 8), piece)]
    total = got_one[0, 0]
    for k in range(2):
        for n in range(grid):
            if k + n > 0:
                total = total + got_one[k, n]
    sum_one[...] = total
    got_two[c] = total
    round_b = []
    for n, d in enumerate(col_steps):
        copy = remote(sum_one, got_two.at[c], lb_send.at[n], lb_recv.at[code_of(d)], col_at(d))
        copy.start()
        round_b.append(copy)

    def turn(source, k, slot):
        wide[...] = source.astype(F32).reshape(size * blocks, size)
        for j in range(blocks):
            turned[k, slot, j] = wide[pl.ds(j, size, stride=blocks), :].astype(BF16)

    def turn_own(s, carry):
        slot = 2 * r + s
        turn(child[f, rows_inv[f * 2 * grid + slot]], f, slot)
        return carry

    lax.fori_loop(0, 2, turn_own, 0)

    for copy in round_b:
        copy.wait_recv()
    total = got_two[0]
    for n in range(1, grid):
        total = total + got_two[n]
    sum_two[...] = total
    lead[pl.ds(pl.multiple_of(r * piece, 8), piece)] = total
    round_c = []
    for n, d in enumerate(row_steps):
        copy = remote(
            sum_two, lead.at[pl.ds(pl.multiple_of(r * piece, 8), piece)], lc_send.at[n], lc_recv.at[code_of(d)], row_at(0, d)
        )
        copy.start()
        round_c.append(copy)

    round_one = []
    for n, (p, d) in enumerate(row_peers):
        peer = row_at(p, d)
        copy = remote(
            send_one.at[peer[0], pl.ds(2 * peer[1], 2)],
            recv_one.at[f, pl.ds(2 * r, 2)], one_send.at[n], one_recv.at[p, code_of(d)], peer,
        )
        copy.start()
        round_one.append(copy)

    for n, d in enumerate(row_steps):
        source = pl.ds(pl.multiple_of(member(r, d, half, -1) * piece, 8), piece)
        remote(sum_two, lead.at[source], lc_send.at[n], lc_recv.at[code_of(d)], row_at(0, d)).wait_recv()
    factor_lead(lead, low_ref, inv_ref, work, size)
    outs = [
        pltpu.make_async_copy(low_ref, low_out, out_sem.at[0]),
        pltpu.make_async_copy(inv_ref, inv_out, out_sem.at[1]),
    ]

    def finish_child(p):
        k = f if p == 0 else other
        for n, (q, d) in enumerate(row_peers):
            if q != p:
                continue
            round_one[n].wait_recv()
            source = member(r, d, half, -1)

            def turn_one(s, carry):
                turn(recv_one[k, 2 * source + s], k, 2 * source + s)
                return carry

            lax.fori_loop(0, 2, turn_one, 0)

        def gather(j, carry):
            row = row_slot[k * blocks + j]
            for slot in range(2 * grid):
                send_two[k, slot // 2, j, slot % 2] = turned[k, row, cols_inv[k * 2 * grid + slot]]
            return carry

        lax.fori_loop(0, blocks, gather, 0)
        sent = []
        for n, d in enumerate(col_steps):
            peer = col_at(d)
            copy = remote(
                send_two.at[k, peer[2]], recv_two.at[c, k], two_send.at[p, n], two_recv.at[k, code_of(d)], peer
            )
            copy.start()
            sent.append(copy)
        local = pltpu.make_async_copy(send_two.at[k, c], recv_two.at[c, k], local_sem.at[p])
        local.start()
        return sent, local

    sent_a, local_a = finish_child(0)
    sent_b, local_b = finish_child(1)

    for n in range(spots):
        line(n, n % 2).start()
        if n > 0:
            line(n - 1, (n - 1) % 2).wait()
            fcol_ref[n - 1] = chunk[(n - 1) % 2, pl.ds(0, size, stride=spots), :]
    line(spots - 1, (spots - 1) % 2).wait()
    fcol_ref[spots - 1] = chunk[(spots - 1) % 2, pl.ds(0, size, stride=spots), :]
    outs.append(pltpu.make_async_copy(fcol_ref, fcol_out, out_sem.at[2]))
    for copy in outs:
        copy.start()

    for copy in outs:
        copy.wait()
    for copy in round_a + round_b + round_c + round_one:
        copy.wait_send()
    for sent, local, k in ((sent_a, local_a, f), (sent_b, local_b, other)):
        local.wait()
        for n in range(len(sent)):
            sent[n].wait_send()
            sent[n].wait_recv()


def exchange(child, flat, rows_inv, row_slot, cols_inv, lead_row, lead_col, grid, spots):
    _, blocks, size, _, _ = child.shape
    piece = len(LEAD) * size // grid
    dma = pltpu.SemaphoreType.DMA
    smem = pl.BlockSpec(memory_space=SMEM)
    hbm = pl.BlockSpec(memory_space=HBM)
    return pl.pallas_call(
        functools.partial(exchange_kernel, grid, size, blocks, spots),
        out_shape=[
            jax.ShapeDtypeStruct((grid, 2, blocks, 2, size, size), BF16),
            jax.ShapeDtypeStruct((2, size, 2 * size), F32),
            jax.ShapeDtypeStruct((2 * size, 2 * size), F32),
            jax.ShapeDtypeStruct((spots, size, size), F32),
        ],
        in_specs=[smem] * 5 + [hbm] * 2,
        out_specs=[hbm] * 4,
        scratch_shapes=[
            pltpu.VMEM((2, size, 2 * size), F32),
            pltpu.VMEM((2 * size, 2 * size), F32),
            pltpu.VMEM((spots, size, size), F32),
            pltpu.VMEM(child.shape, BF16),
            pltpu.VMEM((2, 2 * grid, size, blocks, size), BF16),
            pltpu.VMEM((2, 2 * grid, size, blocks, size), BF16),
            pltpu.VMEM((2, 2 * grid, blocks, size, size), BF16),
            pltpu.VMEM((2, grid, blocks, 2, size, size), BF16),
            pltpu.VMEM((size * blocks, size), F32),
            pltpu.VMEM((2, size * spots, size), F32),
            pltpu.VMEM((2, len(LEAD) * size, size), F32),
            pltpu.VMEM((piece, size), F32),
            pltpu.VMEM((piece, size), F32),
            pltpu.VMEM((2, grid, piece, size), F32),
            pltpu.VMEM((grid, piece, size), F32),
            pltpu.VMEM((len(LEAD) * size, size), F32),
            pltpu.VMEM((size, 2 * size), F32),
            dma((2,)),
            dma((2,)),
            dma((2,)),
            dma((3,)),
            dma((2 * grid,)),
            dma((2, grid)),
            dma((2, grid)),
            dma((2, grid)),
            dma((2 * grid,)),
            dma((2, grid)),
            dma((grid,)),
            dma((grid,)),
            dma((grid,)),
            dma((grid,)),
        ],
        compiler_params=pltpu.CompilerParams(
            collective_id=1, has_side_effects=True, vmem_limit_bytes=60 * 2**20
        ),
        cost_estimate=pl.CostEstimate(flops=400_000_000, bytes_accessed=8 * child.size, transcendentals=0),
        name="exchange",
    )(rows_inv.reshape(-1), row_slot.reshape(-1), cols_inv.reshape(-1), lead_row.reshape(-1), lead_col.reshape(-1), child, flat)


def added(base, parts):
    for block, valid in parts:
        base = base + jnp.where(valid, block.astype(F32), 0.0)
    return base


def split(value):
    high = value.astype(BF16)
    return high, (value - high.astype(F32)).astype(BF16)


def spread_kernel(
    grid, spots, size, row_ref, col_ref, child_hbm, flat_hbm, fcol_hbm, low_hbm, inv_hbm,
    whole_hbm, v_rows_out, rows_high_out, rows_low_out, cols_high_out, cols_low_out,
    fcol_ref, low_ref, inv_ref, v_rows, rows_high, rows_low, cols_high, cols_low, child, whole, rows_own, cols_own, rows_all, cols_all,
    child_sem, in_sem, out_sem, small_sem, v_sem, one_send, one_recv, flip_send, flip_recv, two_send, two_recv,
):
    f, r, c = lax.axis_index("front"), lax.axis_index("row"), lax.axis_index("col")
    half = grid // 2
    part = spots // half
    row_peer = lambda i: (f, r, i)
    col_peer = lambda i: (f, i, c)
    groups = ((rows_own, rows_all, c, row_peer), (cols_own, cols_all, r, col_peer))

    def line(l):
        return pl.ds(pl.multiple_of(l * size * spots, size * spots), size * spots)

    def line_in(l):
        return pltpu.make_async_copy(flat_hbm.at[line(l)], whole.at[line(l)], in_sem.at[l])

    def line_out(l):
        return pltpu.make_async_copy(whole.at[line(l)], whole_hbm.at[line(l)], out_sem.at[l])

    line_in(0).start()
    for n in range(grid):
        pltpu.make_async_copy(child_hbm.at[n], child.at[n], child_sem.at[n]).start()
    small = [
        pltpu.make_async_copy(src, dst, small_sem.at[n])
        for n, (src, dst) in enumerate(((fcol_hbm, fcol_ref), (low_hbm, low_ref), (inv_hbm, inv_ref)))
    ]
    for copy in small:
        copy.start()
    for l in range(1, spots):
        line_in(l).start()
    meet([peer(lax.rem(me + d, grid)) for _, _, me, peer in groups for d in range(1, grid)])

    def from_child(l, j):
        parts = []
        for k in range(2):
            row, col = row_ref[k * spots + l], col_ref[k * spots + j]
            valid = (row >= 0) & (col >= 0)
            row, col = jnp.maximum(row, 0), jnp.maximum(col, 0)
            parts.append((child[col // 2, k, row, col % 2], valid))
        return parts

    line_in(0).wait()
    for copy in small:
        copy.wait()
    for n in range(grid):
        pltpu.make_async_copy(child_hbm.at[n], child.at[n], child_sem.at[n]).wait()

    @pl.when(c < 2)
    def _():
        def one(l, carry):
            rows_own[l] = added(fcol_ref[l], from_child(l, 0))
            return carry

        lax.fori_loop(0, spots, one, 0)

    @pl.when(r < 2)
    def _():
        for j in range(spots):
            cols_own[j] = added(whole[pl.ds(j, size, stride=spots), :], from_child(0, j)).T

    def remote(src, dst, send_sem, recv_sem, peer):
        return pltpu.make_async_remote_copy(
            src_ref=src, dst_ref=dst, send_sem=send_sem, recv_sem=recv_sem, device_id=peer, device_id_type=MESH
        )

    def first(g, n):
        source, out, me, peer = groups[g]
        piece = pl.ds(n * part, part)
        to = peer(2 * n + lax.rem(me, 2))
        return remote(source.at[piece], out.at[lax.rem(me, 2), piece], one_send.at[g, n], one_recv.at[g], to)

    def piece_of(g):
        return pl.ds((groups[g][2] // 2) * part, part)

    def panel_of(g, t):
        return lax.rem(groups[g][2] + t, 2)

    def across(g, source):
        _, out, me, peer = groups[g]
        to = peer(2 * (me // 2) + lax.rem(me + 1, 2))
        piece = piece_of(g)
        return remote(source.at[piece], out.at[panel_of(g, 0), piece], flip_send.at[g], flip_recv.at[g], to)

    def along(g, t, n, source):
        _, out, me, peer = groups[g]
        piece = piece_of(g)
        to = peer(lax.rem(me + 2 * n, grid))
        return remote(source.at[piece], out.at[panel_of(g, t), piece], two_send.at[g, t, n], two_recv.at[g, t, n], to)

    def assemble(l, carry):
        @pl.when(l > 0)
        def _():
            line_in(l).wait()

        for j in range(spots):
            here = pl.ds(l * size * spots + j, size, stride=spots)
            whole[here, :] = added(whole[here, :], from_child(l, j))
        line_out(l).start()
        return carry

    cuts = [spots * n // 3 for n in range(4)]

    for g in range(2):

        @pl.when(groups[g][2] < 2)
        def _():
            source, out, me, _ = groups[g]
            for n in range(1, half):
                first(g, n).start()
            across(g, source).start()
            for n in range(1, half):
                along(g, 0, n, source).start()
            out[me, pl.ds(0, part)] = source[pl.ds(0, part)]

    lax.fori_loop(cuts[0], cuts[1], assemble, 0)

    for g in range(2):

        @pl.when(groups[g][2] >= 2)
        def _():
            here = groups[g][1].at[panel_of(g, 0)]
            remote(
                here.at[piece_of(g)], here.at[piece_of(g)], one_send.at[g, 0], one_recv.at[g],
                groups[g][3](lax.rem(groups[g][2], 2)),
            ).wait_recv()
            across(g, here).start()
            for n in range(1, half):
                along(g, 0, n, here).start()

    lax.fori_loop(cuts[1], cuts[2], assemble, 0)

    for g in range(2):
        here = groups[g][1].at[panel_of(g, 1)]
        me = groups[g][2]
        remote(
            here.at[piece_of(g)], here.at[piece_of(g)], flip_send.at[g], flip_recv.at[g],
            groups[g][3](2 * (me // 2) + lax.rem(me + 1, 2)),
        ).wait_recv()
        for n in range(1, half):
            along(g, 1, n, here).start()

    lax.fori_loop(cuts[2], cuts[3], assemble, 0)

    def solve(g, quarter, n):
        out = groups[g][1]

        def one(i, carry):
            l = quarter * part + i
            here = pl.ds(pl.multiple_of(l * size, size), size)
            v = mm_t(jnp.concatenate([out[0, l], out[1, l]], axis=1), inv_ref[...])
            if g == 0:
                low = jnp.where(r == 0, low_ref[0], low_ref[1])
                v = jnp.where((r < 2) & (l == 0), low, v)
                v_rows[here, :] = v
                rows_high[here, :], rows_low[here, :] = split(v)
            else:
                cols_high[here, :], cols_low[here, :] = split(v)
            return carry

        lax.fori_loop(0, part, one, 0)
        here = pl.ds(pl.multiple_of(quarter * part * size, size), part * size)
        for i, (src, dst) in enumerate(factors[g]):
            copy = pltpu.make_async_copy(src.at[here], dst.at[here], v_sem.at[g, n, i])
            copy.start()
            leaving.append(copy)

    factors = (
        ((rows_high, rows_high_out), (rows_low, rows_low_out), (v_rows, v_rows_out)),
        ((cols_high, cols_high_out), (cols_low, cols_low_out)),
    )
    leaving = []
    for g in range(2):
        solve(g, groups[g][2] // 2, 0)

    for n in range(1, half):
        for g in range(2):
            source, out, me, _ = groups[g]
            quarter = lax.rem(me // 2 + half - n, half)
            piece = pl.ds(quarter * part, part)
            for t in range(2):
                here = out.at[panel_of(g, t), piece]
                to = groups[g][3](lax.rem(me + 2 * n, grid))
                remote(here, here, two_send.at[g, t, n], two_recv.at[g, t, n], to).wait_recv()
            solve(g, quarter, n)

    for g in range(2):
        here = groups[g][1].at[0]

        @pl.when(groups[g][2] < 2)
        def _():
            for n in range(1, half):
                first(g, n).wait_send()

        across(g, here).wait_send()
        for t in range(2):
            for n in range(1, half):
                along(g, t, n, here).wait_send()
    for l in range(spots):
        line_out(l).wait()
    for copy in leaving:
        copy.wait()


def spread(received, flat, fcol, low, inverse, row_pos, col_pos, grid):
    spots, size, _ = fcol.shape
    half = grid // 2
    order = spots * size
    dma = pltpu.SemaphoreType.DMA
    smem = pl.BlockSpec(memory_space=SMEM)
    hbm = pl.BlockSpec(memory_space=HBM)
    return pl.pallas_call(
        functools.partial(spread_kernel, grid, spots, size),
        out_shape=[jax.ShapeDtypeStruct(flat.shape, F32), jax.ShapeDtypeStruct((order, 2 * size), F32)]
        + [jax.ShapeDtypeStruct((order, 2 * size), BF16)] * 4,
        in_specs=[smem] * 2 + [hbm] * 5,
        out_specs=[hbm] * 6,
        scratch_shapes=[
            pltpu.VMEM(fcol.shape, F32),
            pltpu.VMEM(low.shape, F32),
            pltpu.VMEM(inverse.shape, F32),
            pltpu.VMEM((order, 2 * size), F32),
        ]
        + [pltpu.VMEM((order, 2 * size), BF16)] * 4
        + [
            pltpu.VMEM(received.shape, BF16),
            pltpu.VMEM(flat.shape, F32),
            pltpu.VMEM((spots, size, size), F32),
            pltpu.VMEM((spots, size, size), F32),
            pltpu.VMEM((2, spots, size, size), F32),
            pltpu.VMEM((2, spots, size, size), F32),
            dma((grid,)),
            dma((spots,)),
            dma((spots,)),
            dma((3,)),
            dma((2, half, 3)),
            dma((2, half)),
            dma((2,)),
            dma((2,)),
            dma((2,)),
            dma((2, 2, half)),
            dma((2, 2, half)),
        ],
        compiler_params=pltpu.CompilerParams(
            collective_id=3, has_side_effects=True, vmem_limit_bytes=60 * 2**20
        ),
        cost_estimate=pl.CostEstimate(flops=40_000_000, bytes_accessed=8 * flat.size, transcendentals=0),
        name="spread",
    )(row_pos.reshape(-1), col_pos.reshape(-1), received, flat, fcol, low, inverse)


def update_kernel(spots, size, where_ref, whole_ref, v_rows, rows_high, rows_low, cols_high, cols_low, out_ref):
    step = pl.program_id(0)
    my_row, my_col = where_ref[1], where_ref[2]
    count = whole_ref.shape[0] // (size * spots)
    wide = 2 if spots % 2 == 0 else 1

    def dot(a, b):
        return lax.dot_general(a, b, (((1,), (1,)), ((), ())), preferred_element_type=F32)

    high, low = rows_high[...], rows_low[...]
    for j in range(0, spots, wide):
        there = pl.ds(j * size, wide * size)
        ch, cl = cols_high[there, :], cols_low[there, :]
        product = dot(high, ch) + (dot(high, cl) + dot(low, ch))
        for i in range(count):
            top = (step == 0) & (my_row < 2) & (i == 0)
            for w in range(wide):
                here = pl.ds(i * size * spots + j + w, size, stride=spots)
                value = whole_ref[here, :] - product[i * size : (i + 1) * size, w * size : (w + 1) * size]
                value = jnp.where(top, 0.0, value)
                if j + w == 0:
                    v = v_rows[pl.ds(i * size, size), :]
                    value = jnp.where(my_col == 0, v[:, :size], jnp.where(my_col == 1, v[:, size:], value))
                out_ref[here, :] = value


def update(whole, v_rows, rows_high, rows_low, cols_high, cols_low, where, spots):
    size = whole.shape[-1]
    count = 2 if spots % 2 == 0 else 1
    line = pl.BlockSpec((count * size * spots, size), lambda l, *_: (l, 0))
    rows = pl.BlockSpec((count * size, 2 * size), lambda l, *_: (l, 0))
    cols = pl.BlockSpec((spots * size, 2 * size), lambda l, *_: (0, 0), pipeline_mode=pl.Buffered(1))
    return pl.pallas_call(
        functools.partial(update_kernel, spots, size),
        grid_spec=pltpu.PrefetchScalarGridSpec(
            num_scalar_prefetch=1,
            grid=(spots // count,),
            in_specs=[line, rows, rows, rows, cols, cols],
            out_specs=line,
        ),
        out_shape=jax.ShapeDtypeStruct(whole.shape, F32),
        compiler_params=pltpu.CompilerParams(dimension_semantics=("arbitrary",), vmem_limit_bytes=60 * 2**20),
        cost_estimate=pl.CostEstimate(flops=4_000_000_000, bytes_accessed=8 * whole.size, transcendentals=0),
        name="update",
    )(where, whole, v_rows, rows_high, rows_low, cols_high, cols_low)


def per_device(grid, orig_front, child_updates, index_maps):
    front, row, col = (lax.axis_index(name) for name in ("front", "row", "col"))
    local = orig_front[0, :, 0, :, :, 0, :]
    spots, size, _, _ = local.shape
    flat = local.reshape(spots * size * spots, size)
    child = child_updates[0, :, :, 0, :, :, 0, :]
    rows_inv, lead_row, lead_col, row_slot, cols_inv, row_pos, col_pos = tables(index_maps, grid, spots)
    where = jnp.stack([front, row, col]).astype(I32)
    received, low, inverse, fcol = exchange(
        child, flat, rows_inv, row_slot, cols_inv, lead_row, lead_col, grid, spots
    )
    whole, *factors = spread(received, flat, fcol, low, inverse, row_pos, col_pos, grid)
    out = update(whole, *factors, where, spots)
    return out.reshape(1, spots, 1, size, spots, 1, size)


def solution(mesh):
    placed = (
        P("front", None, "row", None, None, "col", None),
        P("front", None, None, "row", None, None, "col", None),
        P(),
    )
    return jax.shard_map(
        functools.partial(per_device, mesh.shape["row"]),
        mesh=mesh,
        in_specs=placed,
        out_specs=P("front", None, "row", None, None, "col", None),
        check_vma=False,
    )
```

```python
import functools

import jax
import jax.numpy as jnp
from jax import lax
from jax.experimental import pallas as pl
from jax.experimental.pallas import tpu as pltpu
from jax.sharding import PartitionSpec as P

F32 = jnp.float32
BF16 = jnp.bfloat16
I32 = jnp.int32
MESH = pl.DeviceIdType.MESH
HIGHEST = lax.Precision.HIGHEST
HBM = pltpu.MemorySpace.HBM
VMEM = pltpu.MemorySpace.VMEM
SMEM = pltpu.MemorySpace.SMEM


def table_kernel(grid, blocks, spots, maps, rows_inv, lead_row, lead_col, row_slot, cols_inv, row_pos, col_pos):
    front, row, col = lax.axis_index("front"), lax.axis_index("row"), lax.axis_index("col")
    fills = ((rows_inv, 0), (row_slot, 0), (cols_inv, 0), (lead_row, -1), (lead_col, -1), (row_pos, -1), (col_pos, -1))
    for ref, fill in fills:

        def clear(i, carry, ref=ref, fill=fill):
            ref[i] = fill
            return carry

        lax.fori_loop(0, ref.shape[0], clear, 0)

    def order_of(values, q):
        order = jnp.int32(0)
        for before in range(q):
            order = order + jnp.where(values[before] == values[q], 1, 0)
        return order

    def held(p, base, place, spare, inverse, lead):
        blocks_at = [maps[base[0], base[1], q * grid + place] for q in range(blocks)]
        target = [lax.rem(value, grid) for value in blocks_at]
        for q in range(blocks):
            if inverse is not None:
                inverse[p * 2 * grid + 2 * target[q] + order_of(target, q)] = q
            if lead is not None:
                lead[jnp.where(blocks_at[q] < 2, 2 * p + blocks_at[q], spare)] = q

    def one_pair(p, carry):
        mine, own = (p, front), (front, p)
        held(p, mine, row, 4, rows_inv, lead_row)
        held(p, mine, col, 4, None, lead_col)
        held(p, own, col, 4, cols_inv, None)

        def one_source(r, rank):
            row_order, col_order = jnp.int32(0), jnp.int32(0)
            for q in range(blocks):
                value = maps[front, p, q * grid + r]
                target, place = lax.rem(value, grid), lax.div(value, grid)
                hit = target == row
                row_slot[jnp.where(hit, p * blocks + rank, 2 * blocks)] = 2 * r + row_order
                row_pos[jnp.where(hit, p * spots + place, 2 * spots)] = rank
                row_order = row_order + jnp.where(hit, 1, 0)
                rank = rank + jnp.where(hit, 1, 0)
                hit = target == col
                col_pos[jnp.where(hit, p * spots + place, 2 * spots)] = 2 * r + col_order
                col_order = col_order + jnp.where(hit, 1, 0)
            return rank

        lax.fori_loop(0, grid, one_source, jnp.int32(0))
        return carry

    lax.fori_loop(0, 2, one_pair, 0)


def tables(maps, grid, spots):
    blocks = maps.shape[-1] // grid
    sizes = (4 * grid, 5, 5, 2 * blocks + 1, 4 * grid, 2 * spots + 1, 2 * spots + 1)
    smem = pl.BlockSpec(memory_space=SMEM)
    return pl.pallas_call(
        functools.partial(table_kernel, grid, blocks, spots),
        out_shape=[jax.ShapeDtypeStruct((size,), I32) for size in sizes],
        in_specs=[smem],
        out_specs=[smem] * len(sizes),
        cost_estimate=pl.CostEstimate(flops=10_000, bytes_accessed=4096, transcendentals=0),
        name="tables",
    )(maps)


def meet(peers):
    barrier = pltpu.get_barrier_semaphore()
    for peer in peers:
        pl.semaphore_signal(barrier, inc=1, device_id=peer, device_id_type=MESH)
    pl.semaphore_wait(barrier, len(peers))


def codes(half, flip_cost):
    pairs = [(n, flip) for n in range(half) for flip in range(2) if n + flip > 0]
    return sorted(pairs, key=lambda pair: -(min(pair[0], half - pair[0]) + flip_cost * pair[1]))


def member(me, code, half, sign=1):
    ring = lax.rem(me // 2 + (half + sign * code[0]), half)
    return 2 * ring + lax.rem(me + code[1], 2)


def factor_block(work, size):
    lanes = lax.broadcasted_iota(I32, (size, size), 1)
    rows = lax.broadcasted_iota(I32, (size, 1), 0)

    def step(j, carry):
        pivot_row = work[pl.ds(j, 1), :]
        left = work[:, :size]
        column = jnp.sum(jnp.where(lanes == j, left, 0.0), axis=1, keepdims=True)
        pivot = jnp.sum(jnp.where(lanes[:1] == j, pivot_row[:, :size], 0.0), axis=1, keepdims=True)
        scale = jnp.where(rows > j, column / pivot, 0.0)
        work[...] = work[...] - scale * pivot_row
        return carry

    lax.fori_loop(0, size, step, 0)


def triangular(work, size):
    eye = lax.broadcasted_iota(I32, (size, size), 0) == lax.broadcasted_iota(I32, (size, size), 1)
    upper = lax.broadcasted_iota(I32, (size, size), 0) <= lax.broadcasted_iota(I32, (size, size), 1)
    u = work[:, :size]
    root = lax.rsqrt(jnp.sum(jnp.where(eye, u, 0.0), axis=1, keepdims=True))
    lower = jnp.where(upper, u * root, 0.0).T
    inverse = work[:, size:] * root
    return lower, inverse


def mm(a, b):
    return jnp.dot(a, b, precision=HIGHEST, preferred_element_type=F32)


def mm_t(a, b):
    return lax.dot_general(a, b, (((1,), (1,)), ((), ())), precision=HIGHEST, preferred_element_type=F32)


def factor_lead(lead_ref, low_ref, inv_ref, work, size):
    eye = (
        lax.broadcasted_iota(I32, (size, size), 0) == lax.broadcasted_iota(I32, (size, size), 1)
    ).astype(F32)
    work[:, :size] = lead_ref[:size]
    work[:, size:] = eye
    factor_block(work, size)
    l0, i0 = triangular(work, size)
    l10 = mm_t(lead_ref[size : 2 * size], i0)
    work[:, :size] = lead_ref[2 * size :] - mm_t(l10, l10)
    work[:, size:] = eye
    factor_block(work, size)
    l1, i1 = triangular(work, size)
    low_ref[0] = jnp.concatenate([l0, jnp.zeros_like(l0)], axis=1)
    low_ref[1] = jnp.concatenate([l10, l1], axis=1)
    inv_ref[:size, :size] = i0
    inv_ref[:size, size:] = jnp.zeros_like(i0)
    inv_ref[size:, :size] = -mm(i1, mm(l10, i0))
    inv_ref[size:, size:] = i1


LEAD = ((0, 0), (1, 0), (1, 1))


def exchange_kernel(
    grid, size, blocks, spots,
    rows_inv, row_slot, cols_inv, lead_row, lead_col, child_hbm, flat_hbm,
    recv_two, low_out, inv_out, fcol_out,
    low_ref, inv_ref, fcol_ref, child, send_one, recv_one, turned, send_two, wide, chunk, part, sum_one, sum_two, got_one, got_two, lead, work,
    child_sem, chunk_sem, local_sem, out_sem, one_send, one_recv, two_send, two_recv,
    la_send, la_recv, lb_send, lb_recv, lc_send, lc_recv,
):
    f, r, c = lax.axis_index("front"), lax.axis_index("row"), lax.axis_index("col")
    other = 1 - f
    piece = len(LEAD) * size // grid
    half = grid // 2
    row_steps, col_steps = codes(half, 1), codes(half, 2)
    row_peers = [(0, d) for d in row_steps] + [(1, d) for d in row_steps] + [(1, (0, 0))]
    row_at = lambda p, d: (lax.rem(f + p, 2), member(r, d, half), c)
    col_at = lambda d: (f, r, member(c, d, half))
    code_of = lambda d: 2 * d[0] + d[1]

    def remote(src, dst, send_sem, recv_sem, peer):
        return pltpu.make_async_remote_copy(
            src_ref=src, dst_ref=dst, send_sem=send_sem, recv_sem=recv_sem, device_id=peer, device_id_type=MESH
        )

    def line(n, slot):
        rows = pl.ds(n * size * spots, size * spots)
        return pltpu.make_async_copy(flat_hbm.at[rows], chunk.at[slot], chunk_sem.at[slot])

    loads = [pltpu.make_async_copy(child_hbm.at[p], child.at[p], child_sem.at[p]) for p in range(2)]
    for load in loads:
        load.start()
    line(0, 0).start()
    meet([row_at(p, d) for p, d in row_peers] + [col_at(d) for d in col_steps])
    for load in loads:
        load.wait()
    line(0, 0).wait()

    corner = chunk[0, pl.ds(0, size, stride=spots), :]
    lane = lax.broadcasted_iota(I32, (size, blocks, size), 1)
    for p in range(2):
        for n, (a, b) in enumerate(LEAD):
            qa, qb = lead_row[2 * p + a], lead_col[2 * p + b]
            block = child[p, jnp.maximum(qa, 0)].astype(F32)
            block = jnp.sum(jnp.where(lane == qb, block, 0.0), axis=1)
            block = jnp.where((qa >= 0) & (qb >= 0), block, 0.0)
            mine = (f == p) & (r == a) & (c == b)
            part[p, pl.ds(n * size, size)] = block + jnp.where(mine, corner, 0.0)
    round_a = []
    for n, (p, d) in enumerate(row_peers):
        peer = row_at(p, d)
        copy = remote(
            part.at[peer[0], pl.ds(peer[1] * piece, piece)],
            got_one.at[f, r], la_send.at[n], la_recv.at[p, code_of(d)], peer,
        )
        copy.start()
        round_a.append(copy)

    for p in range(2):
        for q, d in row_peers:
            if q == p:
                front, row, _ = row_at(p, d)
                for s in range(2):
                    slot = 2 * row + s
                    send_one[front, slot] = child[front, rows_inv[front * 2 * grid + slot]]

    for copy in round_a:
        copy.wait_recv()
    got_one[f, r] = part[f, pl.ds(pl.multiple_of(r * piece, 8), piece)]
    total = got_one[0, 0]
    for k in range(2):
        for n in range(grid):
            if k + n > 0:
                total = total + got_one[k, n]
    sum_one[...] = total
    got_two[c] = total
    round_b = []
    for n, d in enumerate(col_steps):
        copy = remote(sum_one, got_two.at[c], lb_send.at[n], lb_recv.at[code_of(d)], col_at(d))
        copy.start()
        round_b.append(copy)

    def turn(source, k, slot):
        wide[...] = source.astype(F32).reshape(size * blocks, size)
        for j in range(blocks):
            turned[k, slot, j] = wide[pl.ds(j, size, stride=blocks), :].astype(BF16)

    def turn_own(s, carry):
        slot = 2 * r + s
        turn(child[f, rows_inv[f * 2 * grid + slot]], f, slot)
        return carry

    lax.fori_loop(0, 2, turn_own, 0)

    for copy in round_b:
        copy.wait_recv()
    total = got_two[0]
    for n in range(1, grid):
        total = total + got_two[n]
    sum_two[...] = total
    lead[pl.ds(pl.multiple_of(r * piece, 8), piece)] = total
    round_c = []
    for n, d in enumerate(row_steps):
        copy = remote(
            sum_two, lead.at[pl.ds(pl.multiple_of(r * piece, 8), piece)], lc_send.at[n], lc_recv.at[code_of(d)], row_at(0, d)
        )
        copy.start()
        round_c.append(copy)

    round_one = []
    for n, (p, d) in enumerate(row_peers):
        peer = row_at(p, d)
        copy = remote(
            send_one.at[peer[0], pl.ds(2 * peer[1], 2)],
            recv_one.at[f, pl.ds(2 * r, 2)], one_send.at[n], one_recv.at[p, code_of(d)], peer,
        )
        copy.start()
        round_one.append(copy)

    for n, d in enumerate(row_steps):
        source = pl.ds(pl.multiple_of(member(r, d, half, -1) * piece, 8), piece)
        remote(sum_two, lead.at[source], lc_send.at[n], lc_recv.at[code_of(d)], row_at(0, d)).wait_recv()
    factor_lead(lead, low_ref, inv_ref, work, size)
    outs = [
        pltpu.make_async_copy(low_ref, low_out, out_sem.at[0]),
        pltpu.make_async_copy(inv_ref, inv_out, out_sem.at[1]),
    ]

    def finish_child(p):
        k = f if p == 0 else other
        for n, (q, d) in enumerate(row_peers):
            if q != p:
                continue
            round_one[n].wait_recv()
            source = member(r, d, half, -1)

            def turn_one(s, carry):
                turn(recv_one[k, 2 * source + s], k, 2 * source + s)
                return carry

            lax.fori_loop(0, 2, turn_one, 0)

        def gather(j, carry):
            row = row_slot[k * blocks + j]
            for slot in range(2 * grid):
                send_two[k, slot // 2, j, slot % 2] = turned[k, row, cols_inv[k * 2 * grid + slot]]
            return carry

        lax.fori_loop(0, blocks, gather, 0)
        sent = []
        for n, d in enumerate(col_steps):
            peer = col_at(d)
            copy = remote(
                send_two.at[k, peer[2]], recv_two.at[c, k], two_send.at[p, n], two_recv.at[k, code_of(d)], peer
            )
            copy.start()
            sent.append(copy)
        local = pltpu.make_async_copy(send_two.at[k, c], recv_two.at[c, k], local_sem.at[p])
        local.start()
        return sent, local

    sent_a, local_a = finish_child(0)
    sent_b, local_b = finish_child(1)

    for n in range(spots):
        line(n, n % 2).start()
        if n > 0:
            line(n - 1, (n - 1) % 2).wait()
            fcol_ref[n - 1] = chunk[(n - 1) % 2, pl.ds(0, size, stride=spots), :]
    line(spots - 1, (spots - 1) % 2).wait()
    fcol_ref[spots - 1] = chunk[(spots - 1) % 2, pl.ds(0, size, stride=spots), :]
    outs.append(pltpu.make_async_copy(fcol_ref, fcol_out, out_sem.at[2]))
    for copy in outs:
        copy.start()

    for copy in outs:
        copy.wait()
    for copy in round_a + round_b + round_c + round_one:
        copy.wait_send()
    for sent, local, k in ((sent_a, local_a, f), (sent_b, local_b, other)):
        local.wait()
        for n in range(len(sent)):
            sent[n].wait_send()
            sent[n].wait_recv()


def exchange(child, flat, rows_inv, row_slot, cols_inv, lead_row, lead_col, grid, spots):
    _, blocks, size, _, _ = child.shape
    piece = len(LEAD) * size // grid
    dma = pltpu.SemaphoreType.DMA
    smem = pl.BlockSpec(memory_space=SMEM)
    hbm = pl.BlockSpec(memory_space=HBM)
    return pl.pallas_call(
        functools.partial(exchange_kernel, grid, size, blocks, spots),
        out_shape=[
            jax.ShapeDtypeStruct((grid, 2, blocks, 2, size, size), BF16),
            jax.ShapeDtypeStruct((2, size, 2 * size), F32),
            jax.ShapeDtypeStruct((2 * size, 2 * size), F32),
            jax.ShapeDtypeStruct((spots, size, size), F32),
        ],
        in_specs=[smem] * 5 + [hbm] * 2,
        out_specs=[hbm] * 4,
        scratch_shapes=[
            pltpu.VMEM((2, size, 2 * size), F32),
            pltpu.VMEM((2 * size, 2 * size), F32),
            pltpu.VMEM((spots, size, size), F32),
            pltpu.VMEM(child.shape, BF16),
            pltpu.VMEM((2, 2 * grid, size, blocks, size), BF16),
            pltpu.VMEM((2, 2 * grid, size, blocks, size), BF16),
            pltpu.VMEM((2, 2 * grid, blocks, size, size), BF16),
            pltpu.VMEM((2, grid, blocks, 2, size, size), BF16),
            pltpu.VMEM((size * blocks, size), F32),
            pltpu.VMEM((2, size * spots, size), F32),
            pltpu.VMEM((2, len(LEAD) * size, size), F32),
            pltpu.VMEM((piece, size), F32),
            pltpu.VMEM((piece, size), F32),
            pltpu.VMEM((2, grid, piece, size), F32),
            pltpu.VMEM((grid, piece, size), F32),
            pltpu.VMEM((len(LEAD) * size, size), F32),
            pltpu.VMEM((size, 2 * size), F32),
            dma((2,)),
            dma((2,)),
            dma((2,)),
            dma((3,)),
            dma((2 * grid,)),
            dma((2, grid)),
            dma((2, grid)),
            dma((2, grid)),
            dma((2 * grid,)),
            dma((2, grid)),
            dma((grid,)),
            dma((grid,)),
            dma((grid,)),
            dma((grid,)),
        ],
        compiler_params=pltpu.CompilerParams(
            collective_id=1, has_side_effects=True, vmem_limit_bytes=60 * 2**20
        ),
        cost_estimate=pl.CostEstimate(flops=400_000_000, bytes_accessed=8 * child.size, transcendentals=0),
        name="exchange",
    )(rows_inv.reshape(-1), row_slot.reshape(-1), cols_inv.reshape(-1), lead_row.reshape(-1), lead_col.reshape(-1), child, flat)


def added(base, parts):
    for block, valid in parts:
        base = base + jnp.where(valid, block.astype(F32), 0.0)
    return base


def split(value):
    high = value.astype(BF16)
    return high, (value - high.astype(F32)).astype(BF16)


def spread_kernel(
    grid, spots, size, row_ref, col_ref, child_hbm, flat_hbm, fcol_hbm, low_hbm, inv_hbm,
    whole_hbm, v_rows_out, rows_high_out, rows_low_out, cols_high_out, cols_low_out,
    fcol_ref, low_ref, inv_ref, v_rows, rows_high, rows_low, cols_high, cols_low, child, whole, rows_own, cols_own, rows_all, cols_all,
    child_sem, in_sem, out_sem, small_sem, v_sem, one_send, one_recv, flip_send, flip_recv, two_send, two_recv,
):
    f, r, c = lax.axis_index("front"), lax.axis_index("row"), lax.axis_index("col")
    half = grid // 2
    part = spots // half
    row_peer = lambda i: (f, r, i)
    col_peer = lambda i: (f, i, c)
    groups = ((rows_own, rows_all, c, row_peer), (cols_own, cols_all, r, col_peer))

    def line(l):
        return pl.ds(pl.multiple_of(l * size * spots, size * spots), size * spots)

    def line_in(l):
        return pltpu.make_async_copy(flat_hbm.at[line(l)], whole.at[line(l)], in_sem.at[l])

    def line_out(l):
        return pltpu.make_async_copy(whole.at[line(l)], whole_hbm.at[line(l)], out_sem.at[l])

    line_in(0).start()
    for n in range(grid):
        pltpu.make_async_copy(child_hbm.at[n], child.at[n], child_sem.at[n]).start()
    small = [
        pltpu.make_async_copy(src, dst, small_sem.at[n])
        for n, (src, dst) in enumerate(((fcol_hbm, fcol_ref), (low_hbm, low_ref), (inv_hbm, inv_ref)))
    ]
    for copy in small:
        copy.start()
    for l in range(1, spots):
        line_in(l).start()
    meet([peer(lax.rem(me + d, grid)) for _, _, me, peer in groups for d in range(1, grid)])

    def from_child(l, j):
        parts = []
        for k in range(2):
            row, col = row_ref[k * spots + l], col_ref[k * spots + j]
            valid = (row >= 0) & (col >= 0)
            row, col = jnp.maximum(row, 0), jnp.maximum(col, 0)
            parts.append((child[col // 2, k, row, col % 2], valid))
        return parts

    line_in(0).wait()
    for copy in small:
        copy.wait()
    for n in range(grid):
        pltpu.make_async_copy(child_hbm.at[n], child.at[n], child_sem.at[n]).wait()

    @pl.when(c < 2)
    def _():
        def one(l, carry):
            rows_own[l] = added(fcol_ref[l], from_child(l, 0))
            return carry

        lax.fori_loop(0, spots, one, 0)

    @pl.when(r < 2)
    def _():
        for j in range(spots):
            cols_own[j] = added(whole[pl.ds(j, size, stride=spots), :], from_child(0, j)).T

    def remote(src, dst, send_sem, recv_sem, peer):
        return pltpu.make_async_remote_copy(
            src_ref=src, dst_ref=dst, send_sem=send_sem, recv_sem=recv_sem, device_id=peer, device_id_type=MESH
        )

    def first(g, n):
        source, out, me, peer = groups[g]
        piece = pl.ds(n * part, part)
        to = peer(2 * n + lax.rem(me, 2))
        return remote(source.at[piece], out.at[lax.rem(me, 2), piece], one_send.at[g, n], one_recv.at[g], to)

    def piece_of(g):
        return pl.ds((groups[g][2] // 2) * part, part)

    def panel_of(g, t):
        return lax.rem(groups[g][2] + t, 2)

    def across(g, source):
        _, out, me, peer = groups[g]
        to = peer(2 * (me // 2) + lax.rem(me + 1, 2))
        piece = piece_of(g)
        return remote(source.at[piece], out.at[panel_of(g, 0), piece], flip_send.at[g], flip_recv.at[g], to)

    def along(g, t, n, source):
        _, out, me, peer = groups[g]
        piece = piece_of(g)
        to = peer(lax.rem(me + 2 * n, grid))
        return remote(source.at[piece], out.at[panel_of(g, t), piece], two_send.at[g, t, n], two_recv.at[g, t, n], to)

    def assemble(l, carry):
        @pl.when(l > 0)
        def _():
            line_in(l).wait()

        for j in range(spots):
            here = pl.ds(l * size * spots + j, size, stride=spots)
            whole[here, :] = added(whole[here, :], from_child(l, j))
        line_out(l).start()
        return carry

    cuts = [spots * n // 3 for n in range(4)]

    for g in range(2):

        @pl.when(groups[g][2] < 2)
        def _():
            source, out, me, _ = groups[g]
            for n in range(1, half):
                first(g, n).start()
            across(g, source).start()
            for n in range(1, half):
                along(g, 0, n, source).start()
            out[me, pl.ds(0, part)] = source[pl.ds(0, part)]

    lax.fori_loop(cuts[0], cuts[1], assemble, 0)

    for g in range(2):

        @pl.when(groups[g][2] >= 2)
        def _():
            here = groups[g][1].at[panel_of(g, 0)]
            remote(
                here.at[piece_of(g)], here.at[piece_of(g)], one_send.at[g, 0], one_recv.at[g],
                groups[g][3](lax.rem(groups[g][2], 2)),
            ).wait_recv()
            across(g, here).start()
            for n in range(1, half):
                along(g, 0, n, here).start()

    lax.fori_loop(cuts[1], cuts[2], assemble, 0)

    for g in range(2):
        here = groups[g][1].at[panel_of(g, 1)]
        me = groups[g][2]
        remote(
            here.at[piece_of(g)], here.at[piece_of(g)], flip_send.at[g], flip_recv.at[g],
            groups[g][3](2 * (me // 2) + lax.rem(me + 1, 2)),
        ).wait_recv()
        for n in range(1, half):
            along(g, 1, n, here).start()

    lax.fori_loop(cuts[2], cuts[3], assemble, 0)

    def solve(g, quarter, n):
        out = groups[g][1]

        def one(i, carry):
            l = quarter * part + i
            here = pl.ds(pl.multiple_of(l * size, size), size)
            v = mm_t(jnp.concatenate([out[0, l], out[1, l]], axis=1), inv_ref[...])
            if g == 0:
                low = jnp.where(r == 0, low_ref[0], low_ref[1])
                v = jnp.where((r < 2) & (l == 0), low, v)
                v_rows[here, :] = v
                rows_high[here, :], rows_low[here, :] = split(v)
            else:
                cols_high[here, :], cols_low[here, :] = split(v)
            return carry

        lax.fori_loop(0, part, one, 0)
        here = pl.ds(pl.multiple_of(quarter * part * size, size), part * size)
        for i, (src, dst) in enumerate(factors[g]):
            copy = pltpu.make_async_copy(src.at[here], dst.at[here], v_sem.at[g, n, i])
            copy.start()
            leaving.append(copy)

    factors = (
        ((rows_high, rows_high_out), (rows_low, rows_low_out), (v_rows, v_rows_out)),
        ((cols_high, cols_high_out), (cols_low, cols_low_out)),
    )
    leaving = []
    for g in range(2):
        solve(g, groups[g][2] // 2, 0)

    for n in range(1, half):
        for g in range(2):
            source, out, me, _ = groups[g]
            quarter = lax.rem(me // 2 + half - n, half)
            piece = pl.ds(quarter * part, part)
            for t in range(2):
                here = out.at[panel_of(g, t), piece]
                to = groups[g][3](lax.rem(me + 2 * n, grid))
                remote(here, here, two_send.at[g, t, n], two_recv.at[g, t, n], to).wait_recv()
            solve(g, quarter, n)

    for g in range(2):
        here = groups[g][1].at[0]

        @pl.when(groups[g][2] < 2)
        def _():
            for n in range(1, half):
                first(g, n).wait_send()

        across(g, here).wait_send()
        for t in range(2):
            for n in range(1, half):
                along(g, t, n, here).wait_send()
    for l in range(spots):
        line_out(l).wait()
    for copy in leaving:
        copy.wait()


def spread(received, flat, fcol, low, inverse, row_pos, col_pos, grid):
    spots, size, _ = fcol.shape
    half = grid // 2
    order = spots * size
    dma = pltpu.SemaphoreType.DMA
    smem = pl.BlockSpec(memory_space=SMEM)
    hbm = pl.BlockSpec(memory_space=HBM)
    return pl.pallas_call(
        functools.partial(spread_kernel, grid, spots, size),
        out_shape=[jax.ShapeDtypeStruct(flat.shape, F32), jax.ShapeDtypeStruct((order, 2 * size), F32)]
        + [jax.ShapeDtypeStruct((order, 2 * size), BF16)] * 4,
        in_specs=[smem] * 2 + [hbm] * 5,
        out_specs=[hbm] * 6,
        scratch_shapes=[
            pltpu.VMEM(fcol.shape, F32),
            pltpu.VMEM(low.shape, F32),
            pltpu.VMEM(inverse.shape, F32),
            pltpu.VMEM((order, 2 * size), F32),
        ]
        + [pltpu.VMEM((order, 2 * size), BF16)] * 4
        + [
            pltpu.VMEM(received.shape, BF16),
            pltpu.VMEM(flat.shape, F32),
            pltpu.VMEM((spots, size, size), F32),
            pltpu.VMEM((spots, size, size), F32),
            pltpu.VMEM((2, spots, size, size), F32),
            pltpu.VMEM((2, spots, size, size), F32),
            dma((grid,)),
            dma((spots,)),
            dma((spots,)),
            dma((3,)),
            dma((2, half, 3)),
            dma((2, half)),
            dma((2,)),
            dma((2,)),
            dma((2,)),
            dma((2, 2, half)),
            dma((2, 2, half)),
        ],
        compiler_params=pltpu.CompilerParams(
            collective_id=3, has_side_effects=True, vmem_limit_bytes=60 * 2**20
        ),
        cost_estimate=pl.CostEstimate(flops=40_000_000, bytes_accessed=8 * flat.size, transcendentals=0),
        name="spread",
    )(row_pos.reshape(-1), col_pos.reshape(-1), received, flat, fcol, low, inverse)


def update_kernel(spots, size, where_ref, whole_ref, v_rows, rows_high, rows_low, cols_high, cols_low, out_ref):
    step = pl.program_id(0)
    my_row, my_col = where_ref[1], where_ref[2]
    count = whole_ref.shape[0] // (size * spots)
    wide = 2 if spots % 2 == 0 else 1

    def dot(a, b):
        return lax.dot_general(a, b, (((1,), (1,)), ((), ())), preferred_element_type=F32)

    left = jnp.concatenate([rows_high[...], rows_high[...], rows_low[...]], axis=1)
    for j in range(0, spots, wide):
        there = pl.ds(j * size, wide * size)
        ch, cl = cols_high[there, :], cols_low[there, :]
        product = dot(left, jnp.concatenate([ch, cl, ch], axis=1))
        for i in range(count):
            top = (step == 0) & (my_row < 2) & (i == 0)
            for w in range(wide):
                here = pl.ds(i * size * spots + j + w, size, stride=spots)
                value = whole_ref[here, :] - product[i * size : (i + 1) * size, w * size : (w + 1) * size]
                value = jnp.where(top, 0.0, value)
                if j + w == 0:
                    v = v_rows[pl.ds(i * size, size), :]
                    value = jnp.where(my_col == 0, v[:, :size], jnp.where(my_col == 1, v[:, size:], value))
                out_ref[here, :] = value


def update(whole, v_rows, rows_high, rows_low, cols_high, cols_low, where, spots):
    size = whole.shape[-1]
    count = 2 if spots % 2 == 0 else 1
    line = pl.BlockSpec((count * size * spots, size), lambda l, *_: (l, 0))
    rows = pl.BlockSpec((count * size, 2 * size), lambda l, *_: (l, 0))
    cols = pl.BlockSpec((spots * size, 2 * size), lambda l, *_: (0, 0), pipeline_mode=pl.Buffered(1))
    return pl.pallas_call(
        functools.partial(update_kernel, spots, size),
        grid_spec=pltpu.PrefetchScalarGridSpec(
            num_scalar_prefetch=1,
            grid=(spots // count,),
            in_specs=[line, rows, rows, rows, cols, cols],
            out_specs=line,
        ),
        out_shape=jax.ShapeDtypeStruct(whole.shape, F32),
        compiler_params=pltpu.CompilerParams(dimension_semantics=("arbitrary",), vmem_limit_bytes=60 * 2**20),
        cost_estimate=pl.CostEstimate(flops=4_000_000_000, bytes_accessed=8 * whole.size, transcendentals=0),
        name="update",
    )(where, whole, v_rows, rows_high, rows_low, cols_high, cols_low)


def per_device(grid, orig_front, child_updates, index_maps):
    front, row, col = (lax.axis_index(name) for name in ("front", "row", "col"))
    local = orig_front[0, :, 0, :, :, 0, :]
    spots, size, _, _ = local.shape
    flat = local.reshape(spots * size * spots, size)
    child = child_updates[0, :, :, 0, :, :, 0, :]
    rows_inv, lead_row, lead_col, row_slot, cols_inv, row_pos, col_pos = tables(index_maps, grid, spots)
    where = jnp.stack([front, row, col]).astype(I32)
    received, low, inverse, fcol = exchange(
        child, flat, rows_inv, row_slot, cols_inv, lead_row, lead_col, grid, spots
    )
    whole, *factors = spread(received, flat, fcol, low, inverse, row_pos, col_pos, grid)
    out = update(whole, *factors, where, spots)
    return out.reshape(1, spots, 1, size, spots, 1, size)


def solution(mesh):
    placed = (
        P("front", None, "row", None, None, "col", None),
        P("front", None, None, "row", None, None, "col", None),
        P(),
    )
    return jax.shard_map(
        functools.partial(per_device, mesh.shape["row"]),
        mesh=mesh,
        in_specs=placed,
        out_specs=P("front", None, "row", None, None, "col", None),
        check_vma=False,
    )
```
